32 devices in a mesh: row: 8 (over y, x, core), col: 4 (over z).
Axes of the slice: x: 2, y: 2, z: 4, core: 2. Of those that a mesh axis runs over, the one named last changes fastest.
Arguments:
- left_factors: float32 [128, 256, 32], P(None, ('row', 'col')), may hold values from -12 to 12
- right_factors: float32 [128, 128, 32], P(None, ('col', 'row')), may hold values from -12 to 12
- weight: float32 [1024, 128], replicated, may hold values from -0.1875 to 0.1875
- bias: float32 [128], replicated, may hold values from -2 to 2
- cotangent: float32 [256, 128, 128], P('row', 'col'), may hold values from -6 to 6
Outputs:
- pair_out: float32 [256, 128, 128], P('row', 'col')
- left_grad: float32 [128, 256, 32], P(None, ('row', 'col'))
- right_grad: float32 [128, 128, 32], P(None, ('col', 'row'))
- weight_grad: float32 [1024, 128], replicated
- bias_grad: float32 [128], replicated
The draws below stay inside these ranges and needn't reach their ends.
All inputs are finite; a program needn't handle non-finite values.
Results may differ from the reference program's by a relative error of at most 0.0001.
Values sent between devices are 32-bit elements; how exact they have to be, the bound alone decides.
A program may use at most 64 MiB of HBM per device.

```python
import jax
import jax.numpy as jnp
from jax import lax

S = 128
C = 32
CZ = 128
NI = 256
NJ = 128


def block_scale(rng, extent, cuts, low, high):
    def one(dim, blocks):
        steps = jax.random.uniform(jax.random.fold_in(jax.random.fold_in(rng, 6), dim), (blocks,), jnp.float32, low / len(cuts), high / len(cuts))
        return jnp.repeat(jnp.exp(steps), extent[dim] // blocks).reshape((-1,) + (1,) * (len(extent) - dim - 1))

    level = one(*cuts[0])
    for cut in cuts[1:]:
        level = level * one(*cut)
    return level


def noise(rng, shape, deviation, limit, shards=(), dtype=jnp.bfloat16):
    loudness = block_scale(rng, shape, shards, -0.22, 0.18) if shards else 1.0
    drawn = jax.random.normal(rng, shape, jnp.float32) * deviation * loudness
    return jnp.minimum(jnp.maximum(drawn, -limit), limit).astype(dtype)


def setup_inputs(seed: int = 0) -> dict:
    arg_keys = jax.random.split(jax.random.key(seed), 6)
    return {
        "left_factors": noise(arg_keys[0], (S, NI, C), 2.0, 12.0, ((1, 32),), jnp.float32),
        "right_factors": noise(arg_keys[1], (S, NJ, C), 2.0, 12.0, ((1, 32),), jnp.float32),
        "weight": noise(arg_keys[2], (C * C, CZ), (C * C) ** -0.5, 0.1875, (), jnp.float32),
        "bias": noise(arg_keys[3], (CZ,), 0.3, 2.0, (), jnp.float32),
        "cotangent": noise(arg_keys[4], (NI, NJ, CZ), 1.0, 6.0, ((0, 8), (1, 4)), jnp.float32),
    }


def reference(left_factors, right_factors, weight, bias, cotangent):
    high = lax.Precision.HIGHEST
    step_rows = 16
    blocks = NI // step_rows
    left_blocks = left_factors.reshape(S, blocks, step_rows, C).transpose(1, 0, 2, 3)
    cot_blocks = cotangent.reshape(blocks, step_rows, NJ, CZ)

    def visit(carry, item):
        weight_sum, right_sum = carry
        left_block, cot_block = item
        outer = jnp.einsum("sic,sjd->ijcd", left_block, right_factors, precision=high) / S
        flat = outer.reshape(step_rows, NJ, C * C)
        pair_block = jnp.einsum("ijk,ke->ije", flat, weight, precision=high) + bias
        grad_flat = jnp.einsum("ije,ke->ijk", cot_block, weight, precision=high)
        weight_sum = weight_sum + jnp.einsum("ijk,ije->ke", flat, cot_block, precision=high)
        grad_outer = grad_flat.reshape(step_rows, NJ, C, C)
        left_block_grad = jnp.einsum("ijcd,sjd->sic", grad_outer, right_factors, precision=high) / S
        right_sum = right_sum + jnp.einsum("ijcd,sic->sjd", grad_outer, left_block, precision=high) / S
        return (weight_sum, right_sum), (pair_block, left_block_grad)

    start = (jnp.zeros((C * C, CZ), jnp.float32), jnp.zeros((S, NJ, C), jnp.float32))
    (weight_sum, right_grad), (pair_blocks, left_parts) = lax.scan(visit, start, (left_blocks, cot_blocks))
    pair_out = pair_blocks.reshape(NI, NJ, CZ)
    left_grad = left_parts.transpose(1, 0, 2, 3).reshape(S, NI, C)
    weight_grad = weight_sum / NI
    bias_grad = jnp.sum(cotangent, axis=(0, 1)) / NI
    return pair_out, left_grad, right_grad, weight_grad, bias_grad
```

```python
import functools

import jax
import jax.numpy as jnp
from jax import lax
from jax.experimental import pallas as pl
from jax.experimental.pallas import tpu as pltpu
from jax.sharding import PartitionSpec as P

F32 = jnp.float32
BF16 = jnp.bfloat16
MESH = pl.DeviceIdType.MESH
VMEM = pl.BlockSpec(memory_space=pltpu.VMEM)
HBM = pl.BlockSpec(memory_space=pltpu.HBM)
STEP = 8


def in_hbm(x):
    return pltpu.with_memory_space_constraint(x, pltpu.HBM)


def split(x):
    high = x.astype(BF16)
    return high, (x - high.astype(F32)).astype(BF16)


def dot(a, b):
    return lax.dot_general(a, b, (((1,), (0,)), ((), ())), preferred_element_type=F32)


def dot_wide(a_high, a_low, b_both):
    half = b_both.shape[1] // 2
    wide = dot(a_high, b_both)
    return wide[:, 0:half] + (wide[:, half:] + dot(a_low, b_both[:, 0:half]))


def dot_tall(a_both, b_high, b_low):
    half = a_both.shape[0] // 2
    tall = dot(a_both, b_high)
    return tall[0:half] + (tall[half:] + dot(a_both[0:half], b_low))


def total(parts):
    return functools.reduce(lambda a, b: a + b, parts)


def swap_groups(pieces):
    lane = lax.broadcasted_iota(jnp.int32, pieces[0].shape, 1)
    low = lane < 64
    even = (lane & 32) == 0

    def far(a, b):
        moved = pltpu.roll(jnp.where(low, b, a), 64, 1)
        return jnp.where(low, a, moved), jnp.where(low, moved, b)

    def near(a, b):
        return (
            jnp.where(even, a, pltpu.roll(b, 32, 1)),
            jnp.where(even, pltpu.roll(a, 96, 1), b),
        )

    p0, p2 = far(pieces[0], pieces[2])
    p1, p3 = far(pieces[1], pieces[3])
    p0, p1 = near(p0, p1)
    p2, p3 = near(p2, p3)
    return p0, p1, p2, p3


def tile_kernel(
    nrow, ncol, width, l_ref, r_ref, w_ref, b_ref, cot_ref,
    pair_ref, lg_ref, rg_ref, wg_ref, bg_ref,
    lo, ro, lp, lbuf, vbuf, rpa, rp, rbuf,
    wp, cbuf, xs, xbuf, zs, zbuf, bsrc, brow, bmid, bcol,
    w_v, b_v, cot_v, tmp, scr_a, scr_b, acc,
    c2, ct2, w_c, wt2, wt_l, h_h, h_l, rt_c, r2, t_h, t_l, l_c, l_l, lt_c,
    loc, gls, glr, grs, grr, gps, ls, lr, rs, rr, brs, brr, bcs, bcr,
    vr, ks, kr, xss, xsr, zss, zsr, azs, azr, axs, axr, acs, acr,
):
    row, col = lax.axis_index("row"), lax.axis_index("col")
    chip, core = row // 2, lax.rem(row, 2)
    mate = row + 1 - 2 * core
    chips = nrow // 2
    lw, samples = l_ref.shape
    rw = r_ref.shape[0]
    tile_rows, tile_cols = ncol * lw // width, nrow * rw // width
    channels, pair_width = w_ref.shape
    rights = tile_cols * width
    scale = 1.0 / samples
    per = 128 // width
    share = channels // (nrow * ncol)
    lanes_step = STEP * width
    gcols = max(1, lanes_step // lw)
    groups = ncol // gcols
    glanes = gcols * lw
    grows = glanes // width * tile_cols
    own_group = col // gcols
    piece = lw // 2
    lower, upper = col, ncol - 1 - col
    both = jnp.minimum(lower, upper)
    longer = jnp.where(lower > upper, -1, 1)
    inner = jnp.logical_and(col > 0, col < ncol - 1)

    def along(k):
        paired = k <= 2 * both
        distance = jnp.where(paired, (k + 1) // 2, k - both)
        side = jnp.where(jnp.logical_and(paired, lax.rem(k, 2) == 0), -longer, longer)
        return col + side * distance

    def group_at(k):
        return along(k) if gcols == 1 else lax.rem(own_group + k, groups)

    def via_end(source, target):
        return jnp.logical_or(
            jnp.logical_and(source == 0, target >= 3),
            jnp.logical_and(source == ncol - 1, target <= ncol - 4),
        )

    def via_here(target):
        return jnp.logical_or(
            jnp.logical_and(col == 1, target >= 3),
            jnp.logical_and(col == ncol - 2, target <= ncol - 4),
        )

    def in_row(peer):
        return {"row": peer, "col": col}

    def in_col(peer):
        return {"row": row, "col": peer}

    def block(ref, index, size):
        return ref.at[pl.ds(pl.multiple_of(index * size, size), size)]

    def each(count, here, act):
        @pl.loop(1, count)
        def _(k):
            act(lax.rem(here + k, count))

    def each_chip(act):
        each(chips, chip, act)

    def send(src, dst, send_sem, recv_sem, device):
        return pltpu.make_async_remote_copy(
            src_ref=src, dst_ref=dst, send_sem=send_sem, recv_sem=recv_sem,
            device_id=device, device_id_type=MESH,
        )

    def part(ref, index, s):
        return ref.at[pl.ds(pl.multiple_of(index * lw + s * piece, piece), piece)]

    def left_own(s, side):
        return send(
            l_ref.at[pl.ds(s * piece, piece)], part(lo, col, s), gls.at[col, s, (side + 1) // 2], glr.at[col, s],
            in_col(col + side),
        )

    def left_on(q, s):
        return send(
            part(lo, q, s), part(lo, q, s), gls.at[q, s, 0], glr.at[q, s],
            in_col(col + jnp.where(q < col, 1, -1)),
        )

    def right_gather(peer, slot):
        return send(r_ref, block(ro, slot, rw), grs.at[peer], grr.at[slot], in_row(peer))

    def right_pass(slot, there):
        return send(block(ro, slot, rw), block(ro, slot, rw), gps.at[slot // 2], grr.at[there], in_row(mate))

    def left_term(peer, slot):
        return send(block(lp, peer, lw), lbuf.at[slot], ls.at[peer], lr.at[slot], in_col(peer))

    def left_via(peer):
        return send(
            block(lp, peer, lw), vbuf.at[peer], ls.at[peer], vr.at[peer], in_col(jnp.where(col == 0, 1, ncol - 2))
        )

    def right_term(peer, slot):
        return send(block(rp, peer, rw), rbuf.at[slot], rs.at[peer], rr.at[slot], in_row(peer))

    def bias_row(peer, slot):
        return send(bsrc, brow.at[slot], brs.at[peer], brr.at[slot], in_row(peer))

    def bias_col(peer, slot):
        return send(bmid, bcol.at[slot], bcs.at[peer], bcr.at[slot], in_col(peer))

    def core_term(q):
        return send(wp.at[1 - core, q], cbuf.at[q], ks.at[q], kr.at[q], in_row(mate))

    def chip_term(q, peer, slot):
        return send(xs.at[q, peer], xbuf.at[q, slot], xss.at[q, peer], xsr.at[q, slot], in_row(2 * peer + core))

    def col_term(peer, slot):
        return send(zs.at[peer], zbuf.at[slot], zss.at[peer], zsr.at[slot], in_col(peer))

    def col_whole(peer, slot):
        piece = wg_ref.at[core, slot, chip]
        return send(piece, piece, azs.at[peer], azr.at[slot], in_col(peer))

    def chip_whole(q, peer, slot):
        piece = wg_ref.at[core, q, slot]
        return send(piece, piece, axs.at[q, peer], axr.at[q, slot], in_row(2 * peer + core))

    def core_whole(half, q):
        piece = wg_ref.at[half, q]
        return send(piece, piece, acs.at[q], acr.at[q], in_row(mate))

    own_left = pl.ds(pl.multiple_of(col * lw, lw), lw)
    own_right = pl.ds(pl.multiple_of(row * rw, rw), rw)
    loads = [
        pltpu.make_async_copy(src, dst, loc.at[k])
        for k, (src, dst) in enumerate([
            (w_ref, w_v), (cot_ref, cot_v), (r_ref, ro.at[own_right]), (l_ref, lo.at[own_left]), (b_ref, b_v),
        ])
    ]
    barrier = pltpu.get_barrier_semaphore()
    each(ncol, col, lambda p: pl.semaphore_signal(
        barrier, inc=1, device_id=in_col(p), device_id_type=MESH))
    each(nrow, row, lambda p: pl.semaphore_signal(
        barrier, inc=1, device_id=in_row(p), device_id_type=MESH))
    for load in loads:
        load.start()
    pl.semaphore_wait(barrier, nrow + ncol - 2)

    def ends(act):
        for s in range(2):
            @pl.when(col < ncol - 1)
            def _():
                act(left_own(s, 1))

            @pl.when(col > 0)
            def _():
                act(left_own(s, -1))

    ends(lambda copy: copy.start())
    each_chip(lambda m: right_gather(2 * m + core, row).start())
    right_gather(mate, row).start()

    loads[0].wait()
    loads[1].wait()
    for d in range(width):
        tmp[d * width : (d + 1) * width, :] = w_v[pl.ds(d, width, stride=width), :]
    weight = tmp[0:channels, :]
    w_c[:, 0:pair_width], w_c[:, pair_width:] = split(weight)
    high, wt_l[...] = split(weight.T * scale)
    wt2[0:pair_width, :] = high
    wt2[pair_width:, :] = high
    cot = cot_v[...]
    c2[:, 0:pair_width], c2[:, pair_width:] = split(cot)
    ct2[0:pair_width, :], ct2[pair_width:, :] = split(cot.T)
    bsrc[...] = jnp.broadcast_to(jnp.sum(cot, axis=0, keepdims=True), (8, pair_width))
    brow[row] = bsrc[...]
    each(nrow, row, lambda p: bias_row(p, row).start())

    scrs = [scr_a, scr_b]
    steps = channels // lanes_step

    def grad_block(b):
        lanes = slice(b * lanes_step, (b + 1) * lanes_step)
        scrs[b % 2][...] = dot(c2[...], wt2[:, lanes]) + dot(c2[:, 0:pair_width], wt_l[:, lanes])

    def grad_swap(b):
        scr = scrs[b % 2]
        for u in range(STEP // per):
            for v in range(tile_rows // per):
                pieces = [
                    scr[(v * per + a) * tile_cols : (v * per + a + 1) * tile_cols, u * 128 : (u + 1) * 128]
                    for a in range(per)
                ]
                for a, piece in enumerate(swap_groups(pieces)):
                    at = (b * STEP + u * per + a) * tile_cols
                    high, low = split(piece)
                    h_h[at : at + tile_cols, v * 128 : (v + 1) * 128] = high
                    h_l[at : at + tile_cols, v * 128 : (v + 1) * 128] = low

    grad_block(0)
    for b in range(steps):
        if b + 1 < steps:
            grad_block(b + 1)
        grad_swap(b)

    def relay(k):
        @pl.when(inner)
        def _():
            q = along(k)
            for s in range(2):
                left_on(q, s).wait_recv()
                left_on(q, s).start()

    def arrive(k):
        @pl.when(jnp.logical_not(inner))
        def _():
            q = along(k)
            for s in range(2):
                left_on(q, s).wait_recv()

    for k in range(1, min(ncol, 3)):
        relay(k)
    each_chip(lambda m: right_gather(2 * m + core, 2 * m + core).wait_recv())
    each_chip(lambda m: right_pass(2 * m + core, 2 * m + core).start())
    loads[2].wait()
    right_gather(mate, mate).wait_recv()
    each_chip(lambda m: right_pass(2 * m + 1 - core, 2 * m + 1 - core).wait_recv())
    for d in range(width):
        tmp[d * tile_cols : (d + 1) * tile_cols, :] = ro[pl.ds(d, tile_cols, stride=width), :]
    right = tmp[0:rights, :]
    rt_c[:, 0:samples], rt_c[:, samples:] = split(right)
    r2[0:samples, :], r2[samples:, :] = split(right.T)

    @pl.loop(0, groups)
    def _(k):
        g = group_at(groups - 1 - k)
        lanes = pl.ds(pl.multiple_of(g * glanes, glanes), glanes)
        lp[lanes, :] = dot_tall(r2[...], h_h[:, lanes], h_l[:, lanes]).T
        for a in range(gcols):
            peer = g * gcols + a

            @pl.when(via_end(col, peer))
            def _():
                left_via(peer).start()

            @pl.when(jnp.logical_not(jnp.logical_or(peer == col, jnp.logical_or(via_end(col, peer), via_here(peer)))))
            def _():
                left_term(peer, col).start()

            @pl.when(via_end(peer, col))
            def _():
                lbuf[peer] = jnp.zeros(lbuf.shape[1:], F32)

    lbuf[col] = lp[own_left, :]
    if ncol > 3:
        @pl.loop(3, ncol)
        def _(k):
            relay(k)

    each(nrow, row, lambda p: bias_row(p, p).wait_recv())
    bmid[...] = total([brow[q] for q in range(nrow)])
    bcol[col] = bmid[...]
    each(ncol, col, lambda p: bias_col(p, col).start())
    loads[3].wait()
    loads[4].wait()
    acc[...] = jnp.zeros_like(acc)
    rpa[...] = jnp.zeros_like(rpa)

    if gcols > 1:
        @pl.loop(1, ncol)
        def _(k):
            arrive(k)

    def outer_weight(g):
        left = lo[pl.ds(pl.multiple_of(g * glanes, glanes), glanes), :]
        lt_c[:, 0:samples], lt_c[:, samples:] = split(left)
        high, l_l[...] = split(left.T * scale)
        l_c[0:samples, :] = high
        l_c[samples:, :] = high
        half = rights // 2
        for s in range(2):
            at = slice(s * half, (s + 1) * half)
            scrs[s][0:half, 0:glanes] = dot(rt_c[at, :], l_c[...]) + dot(rt_c[at, 0:samples], l_l[...])
        for s in range(2):
            for u in range(width // per // 2):
                for v in range(glanes // 128):
                    pieces = [
                        scrs[s][(u * per + a) * tile_cols : (u * per + a + 1) * tile_cols, v * 128 : (v + 1) * 128]
                        for a in range(per)
                    ]
                    lanes = slice((s * (width // per // 2) + u) * 128, (s * (width // per // 2) + u + 1) * 128)
                    for a, piece in enumerate(swap_groups(pieces)):
                        at = (v * per + a) * tile_cols
                        high, low = split(piece)
                        t_h[at : at + tile_cols, lanes] = high
                        t_l[at : at + tile_cols, lanes] = low
        rows = pl.ds(pl.multiple_of(g * grows, grows), grows)
        acc[...] += dot_tall(ct2[:, rows], t_h[...], t_l[...])

    def pair_right(g):
        rows = pl.ds(pl.multiple_of(g * grows, grows), grows)
        lanes = pl.ds(pl.multiple_of(g * glanes, glanes), glanes)
        pair_ref[rows, :] = dot_wide(t_h[...], t_l[...], w_c[...]) + b_v[...]
        rpa[...] += dot_wide(h_h[:, lanes], h_l[:, lanes], lt_c[...])

    @pl.loop(0, groups - 1)
    def _(k):
        g = group_at(k)
        if gcols == 1:
            @pl.when(k > 0)
            def _():
                arrive(k)

        outer_weight(g)
        pair_right(g)

    last = group_at(groups - 1)
    if gcols == 1 and groups > 1:
        arrive(groups - 1)
    outer_weight(last)
    for i in range(channels // 128):
        terms = acc[:, i * 128 : (i + 1) * 128].T
        for n in range(128 // share):
            q, m = divmod((i * 128) // share + n, chips)
            b, q = divmod(q, ncol)
            wp[b, q, m] = terms[n * share : (n + 1) * share, :]

    @pl.loop(0, ncol)
    def _(k):
        core_term(along(ncol - 1 - k)).start()

    pair_right(last)
    for p in range(ncol):
        @pl.when(via_here(p))
        def _():
            left_via(p).wait_recv()
            lp[p * lw : (p + 1) * lw, :] += vbuf[p]
            left_term(p, col).start()

    @pl.loop(0, ncol)
    def _(k):
        q = along(ncol - 1 - k)
        core_term(q).wait_recv()
        xs[q] = wp[core, q] + cbuf[q]
        xbuf[q, chip] = xs[q, chip]
        each_chip(lambda m: chip_term(q, m, chip).start())

    for d in range(width):
        rp[pl.ds(d, tile_cols, stride=width), :] = rpa[d * tile_cols : (d + 1) * tile_cols, :]
    each(nrow, row, lambda p: right_term(p, row).start())
    rbuf[row] = rp[own_right, :]

    @pl.loop(0, ncol)
    def _(k):
        q = along(ncol - 1 - k)
        each_chip(lambda m: chip_term(q, m, m).wait_recv())
        zs[q] = total([xbuf[q, m] for m in range(chips)])

        @pl.when(k < ncol - 1)
        def _():
            col_term(q, col).start()

    zbuf[col] = zs[col]
    each(ncol, col, lambda p: bias_col(p, p).wait_recv())
    bg_ref[...] = total([bcol[q] for q in range(ncol)])[0:1, :] / (tile_rows * nrow)
    def left_terms(p):
        @pl.when(jnp.logical_not(via_end(p, col)))
        def _():
            left_term(p, p).wait_recv()

    each(ncol, col, left_terms)
    lg_ref[...] = total([lbuf[q] for q in range(ncol)])
    each(ncol, col, lambda p: col_term(p, p).wait_recv())
    wg_ref[core, col, chip] = total([zbuf[q] for q in range(ncol)]) / (tile_rows * nrow)

    @pl.loop(1, ncol)
    def _(k):
        col_whole(along(ncol - k), col).start()

    each_chip(lambda m: chip_whole(col, m, chip).start())
    ends(lambda copy: copy.wait_send())

    @pl.when(inner)
    def _():
        @pl.loop(1, ncol)
        def _(k):
            for s in range(2):
                left_on(along(k), s).wait_send()

    each_chip(lambda m: right_gather(2 * m + core, row).wait_send())
    right_gather(mate, row).wait_send()
    each_chip(lambda m: right_pass(2 * m + core, 2 * m + core).wait_send())
    each(nrow, row, lambda p: bias_row(p, row).wait_send())
    each(ncol, col, lambda p: bias_col(p, col).wait_send())
    each(ncol, col, lambda p: left_term(p, col).wait_send())
    each(ncol, col, lambda p: col_term(p, col).wait_send())

    @pl.loop(0, ncol)
    def _(q):
        core_term(q).wait_send()
        each_chip(lambda m: chip_term(q, m, chip).wait_send())

    each(nrow, row, lambda p: right_term(p, row).wait_send())

    @pl.loop(1, ncol)
    def _(k):
        q = along(k)
        col_whole(q, q).wait_recv()
        each_chip(lambda m: chip_whole(q, m, chip).start())

    @pl.loop(0, ncol)
    def _(k):
        q = along(k)
        each_chip(lambda m: chip_whole(q, m, m).wait_recv())
        core_whole(core, q).start()

    each(nrow, row, lambda p: right_term(p, p).wait_recv())
    rg_ref[...] = total([rbuf[q] for q in range(nrow)])
    each(ncol, col, lambda p: col_whole(p, col).wait_send())

    @pl.loop(0, ncol)
    def _(q):
        each_chip(lambda m: chip_whole(q, m, chip).wait_send())
        core_whole(core, q).wait_send()

    @pl.loop(0, ncol)
    def _(q):
        core_whole(1 - core, q).wait_recv()


def finish_kernel(
    width, pair_ref, lg_ref, rg_ref, wg_ref, bg_ref,
    pair_out, lg_out, rg_out, w_out, bg_out, held, sems,
):
    copies = [
        pltpu.make_async_copy(src, dst, sems.at[k])
        for k, (src, dst) in enumerate([
            (pair_ref, pair_out), (lg_ref, lg_out), (rg_ref, rg_out), (bg_ref, bg_out),
        ])
    ]
    for copy in copies:
        copy.start()
    halves, ncol, chips, share, _ = wg_ref.shape
    for s in range(halves * ncol * chips):
        d, c = divmod(s * share, width)
        q, m = divmod(s, chips)
        b, q = divmod(q, ncol)
        held[pl.ds(c * width + d, share, stride=width), :] = wg_ref[b, q, m]
    last = pltpu.make_async_copy(held, w_out, sems.at[4])
    last.start()
    for copy in [*copies, last]:
        copy.wait()


def per_device(nrow, ncol, left_factors, right_factors, weight, bias, cotangent):
    samples, li, width = left_factors.shape
    rj = right_factors.shape[1]
    tile_rows, tile_cols, pair_width = cotangent.shape
    channels = weight.shape[0]
    lw, rw = li * width, rj * width
    lefts, rights = tile_rows * width, tile_cols * width
    pairs = tile_rows * tile_cols
    chips, share = nrow // 2, channels // (nrow * ncol)
    group = max(lw, STEP * width)
    dma = pltpu.SemaphoreType.DMA

    def shape(*dims):
        return jax.ShapeDtypeStruct(dims, F32)

    def half(*dims):
        return pltpu.VMEM(dims, BF16)

    def buf(*dims):
        return pltpu.VMEM(dims, F32)

    scratch = [
        buf(lefts, samples), buf(rights, samples), buf(lefts, samples), *[buf(ncol, lw, samples)] * 2,
        buf(rights, samples), buf(rights, samples), buf(nrow, rw, samples),
        buf(2, ncol, chips, share, pair_width), *[buf(ncol, chips, share, pair_width)] * 3,
        *[buf(ncol, share, pair_width)] * 2,
        buf(8, pair_width), buf(nrow, 8, pair_width), buf(8, pair_width), buf(ncol, 8, pair_width),
        buf(channels, pair_width), buf(1, pair_width), buf(pairs, pair_width),
        buf(max(rights, channels), 128),
        *[buf(max(pairs, rights), max(group, STEP * width))] * 2, buf(pair_width, channels),
        half(pairs, 2 * pair_width), half(2 * pair_width, pairs), half(channels, 2 * pair_width),
        half(2 * pair_width, channels), half(pair_width, channels),
        half(rights, lefts), half(rights, lefts), half(rights, 2 * samples), half(2 * samples, rights),
        *[half(group // width * tile_cols, channels)] * 2,
        half(2 * samples, group), half(samples, group), half(group, 2 * samples),
        dma((5,)), dma((ncol, 2, 2)), dma((ncol, 2)), dma((nrow,)), dma((nrow,)), dma((chips,)),
        dma((ncol,)), dma((ncol,)), dma((nrow,)), dma((nrow,)),
        dma((nrow,)), dma((nrow,)), dma((ncol,)), dma((ncol,)),
        dma((ncol,)), dma((ncol,)), dma((ncol,)), dma((ncol, chips)), dma((ncol, chips)),
        dma((ncol,)), dma((ncol,)), dma((ncol,)), dma((ncol,)),
        dma((ncol, chips)), dma((ncol, chips)), dma((ncol,)), dma((ncol,)),
    ]
    pair, lg, rg, wg, bg = pl.pallas_call(
        functools.partial(tile_kernel, nrow, ncol, width),
        out_shape=(
            shape(pairs, pair_width), shape(lw, samples), shape(rw, samples),
            shape(2, ncol, chips, share, pair_width), shape(1, pair_width),
        ),
        in_specs=[HBM] * 5,
        out_specs=[VMEM] * 5,
        scratch_shapes=scratch,
        compiler_params=pltpu.CompilerParams(
            collective_id=0, has_side_effects=True, vmem_limit_bytes=40 * 2**20
        ),
        name="tile",
    )(
        in_hbm(left_factors.transpose(1, 2, 0).reshape(lw, samples)),
        in_hbm(right_factors.transpose(1, 2, 0).reshape(rw, samples)),
        in_hbm(weight),
        in_hbm(bias.reshape(1, pair_width)),
        in_hbm(cotangent.reshape(pairs, pair_width)),
    )
    pair, lg, rg, wg, bg = pl.pallas_call(
        functools.partial(finish_kernel, width),
        out_shape=(
            shape(pairs, pair_width), shape(lw, samples), shape(rw, samples),
            shape(channels, pair_width), shape(1, pair_width),
        ),
        in_specs=[VMEM] * 5,
        out_specs=[HBM] * 5,
        scratch_shapes=[buf(channels, pair_width), dma((5,))],
        compiler_params=pltpu.CompilerParams(vmem_limit_bytes=8 * 2**20),
        name="finish",
    )(pair, lg, rg, wg, bg)
    return (
        pair.reshape(tile_rows, tile_cols, pair_width),
        lg.reshape(li, width, samples).transpose(2, 0, 1),
        rg.reshape(rj, width, samples).transpose(2, 0, 1),
        wg,
        bg.reshape(pair_width),
    )


def solution(mesh):
    nrow, ncol = mesh.shape["row"], mesh.shape["col"]
    in_specs = (
        P(None, ("row", "col"), None),
        P(None, ("col", "row"), None),
        P(),
        P(),
        P("row", "col", None),
    )
    out_specs = (
        P("row", "col", None),
        P(None, ("row", "col"), None),
        P(None, ("col", "row"), None),
        P(),
        P(),
    )
    return jax.shard_map(
        functools.partial(per_device, nrow, ncol),
        mesh=mesh, in_specs=in_specs, out_specs=out_specs, check_vma=False,
    )
```

```python
import functools

import jax
import jax.numpy as jnp
from jax import lax
from jax.experimental import pallas as pl
from jax.experimental.pallas import tpu as pltpu
from jax.sharding import PartitionSpec as P

F32 = jnp.float32
BF16 = jnp.bfloat16
MESH = pl.DeviceIdType.MESH
VMEM = pl.BlockSpec(memory_space=pltpu.VMEM)
HBM = pl.BlockSpec(memory_space=pltpu.HBM)
STEP = 8
SINGLE = (
    "left", "relay", "right", "pass", "same", "mate", "passed", "terms", "term", "via", "swap", "swapped",
    "rterms", "rterm", "brow", "browed", "bcol", "bcoled", "core", "chip", "col", "coled",
    "allcol", "allchip", "allcore", "done",
)


def in_hbm(x):
    return pltpu.with_memory_space_constraint(x, pltpu.HBM)


def split(x):
    high = x.astype(BF16)
    return high, (x - high.astype(F32)).astype(BF16)


def dot(a, b):
    return lax.dot_general(a, b, (((1,), (0,)), ((), ())), preferred_element_type=F32)


def dot_wide(a_high, a_low, b_both):
    half = b_both.shape[1] // 2
    wide = dot(a_high, b_both)
    return wide[:, 0:half] + (wide[:, half:] + dot(a_low, b_both[:, 0:half]))


def dot_tall(a_both, b_high, b_low):
    half = a_both.shape[0] // 2
    tall = dot(a_both, b_high)
    return tall[0:half] + (tall[half:] + dot(a_both[0:half], b_low))


def total(parts):
    return functools.reduce(lambda a, b: a + b, parts)


def swap_groups(pieces):
    lane = lax.broadcasted_iota(jnp.int32, pieces[0].shape, 1)
    low = lane < 64
    even = (lane & 32) == 0

    def far(a, b):
        moved = pltpu.roll(jnp.where(low, b, a), 64, 1)
        return jnp.where(low, a, moved), jnp.where(low, moved, b)

    def near(a, b):
        return (
            jnp.where(even, a, pltpu.roll(b, 32, 1)),
            jnp.where(even, pltpu.roll(a, 96, 1), b),
        )

    p0, p2 = far(pieces[0], pieces[2])
    p1, p3 = far(pieces[1], pieces[3])
    p0, p1 = near(p0, p1)
    p2, p3 = near(p2, p3)
    return p0, p1, p2, p3


def tile_kernel(
    nrow, ncol, width, l_ref, r_ref, w_ref, b_ref, cot_ref,
    pair_ref, lg_ref, rg_ref, wg_ref, bg_ref,
    lo, ro, lp, lbuf, vbuf, rpa, rp, mbuf, rsum, rbuf,
    wp, cbuf, xs, xbuf, zs, zbuf, bsrc, brow, bmid, bcol,
    w_v, b_v, cot_v, tmp, scr_a, scr_b, acc,
    c2, ct2, w_c, wt2, wt_l, h_h, h_l, rt_c, r2, t_h, t_l, l_c, l_l, lt_c,
    loc, one, glr, kr, xsr, azr, axr,
):
    row, col = lax.axis_index("row"), lax.axis_index("col")
    chip, core = row // 2, lax.rem(row, 2)
    mate = row + 1 - 2 * core
    chips = nrow // 2
    lw, samples = l_ref.shape
    rw = r_ref.shape[0]
    tile_rows, tile_cols = ncol * lw // width, nrow * rw // width
    channels, pair_width = w_ref.shape
    rights = tile_cols * width
    scale = 1.0 / samples
    per = 128 // width
    share = channels // (nrow * ncol)
    lanes_step = STEP * width
    gcols = max(1, lanes_step // lw)
    groups = ncol // gcols
    glanes = gcols * lw
    grows = glanes // width * tile_cols
    own_group = col // gcols
    piece = lw // 2
    lower, upper = col, ncol - 1 - col
    both = jnp.minimum(lower, upper)
    longer = jnp.where(lower > upper, -1, 1)
    inner = jnp.logical_and(col > 0, col < ncol - 1)

    def along(k):
        paired = k <= 2 * both
        distance = jnp.where(paired, (k + 1) // 2, k - both)
        side = jnp.where(jnp.logical_and(paired, lax.rem(k, 2) == 0), -longer, longer)
        return col + side * distance

    def group_at(k):
        return along(k) if gcols == 1 else lax.rem(own_group + k, groups)

    def via_end(source, target):
        return jnp.logical_or(
            jnp.logical_and(source == 0, target >= 3),
            jnp.logical_and(source == ncol - 1, target <= ncol - 4),
        )

    def via_here(target):
        return jnp.logical_or(
            jnp.logical_and(col == 1, target >= 3),
            jnp.logical_and(col == ncol - 2, target <= ncol - 4),
        )

    def in_row(peer):
        return {"row": peer, "col": col}

    def in_col(peer):
        return {"row": row, "col": peer}

    def block(ref, index, size):
        return ref.at[pl.ds(pl.multiple_of(index * size, size), size)]

    def each(count, here, act):
        @pl.loop(1, count)
        def _(k):
            act(lax.rem(here + k, count))

    wide = chips // 2
    steps_out = sorted(
        ((a, b) for a in range(wide) for b in range(2) if a + b), key=lambda s: -(min(s[0], wide - s[0]) + s[1])
    )

    def each_chip(act):
        for a, b in steps_out:
            act(lax.rem(chip // 2 + a, wide) * 2 + lax.rem(chip + b, 2))

    def send(src, dst, send_sem, recv_sem, device):
        return pltpu.make_async_remote_copy(
            src_ref=src, dst_ref=dst, send_sem=send_sem, recv_sem=recv_sem,
            device_id=device, device_id_type=MESH,
        )

    def part(ref, index, s):
        return ref.at[pl.ds(pl.multiple_of(index * lw + s * piece, piece), piece)]

    def sem(name):
        return one.at[SINGLE.index(name)]

    def settle(ref, semaphore):
        send(ref, ref, semaphore, semaphore, in_row(mate)).wait_recv()

    def left_own(s, side):
        return send(
            part(lo, col, s), part(lo, col, s), sem("left"), glr.at[col, s], in_col(col + side)
        )

    def left_on(q, s):
        return send(
            part(lo, q, s), part(lo, q, s), sem("relay"), glr.at[q, s], in_col(col + jnp.where(q < col, 1, -1))
        )

    def right_own(peer, name):
        return send(block(ro, row, rw), block(ro, row, rw), sem("right"), sem(name), in_row(peer))

    def right_pass(slot):
        return send(block(ro, slot, rw), block(ro, slot, rw), sem("pass"), sem("passed"), in_row(mate))

    def left_term(peer):
        return send(block(lp, peer, lw), lbuf.at[col], sem("terms"), sem("term"), in_col(peer))

    def left_via(peer):
        return send(
            block(lp, peer, lw), vbuf.at[peer], sem("terms"), sem("via"), in_col(jnp.where(col == 0, 1, ncol - 2))
        )

    def right_swap(m):
        return send(block(rp, 2 * m + 1 - core, rw), mbuf.at[m], sem("swap"), sem("swapped"), in_row(mate))

    def right_term(m):
        return send(rsum.at[m], rbuf.at[chip], sem("rterms"), sem("rterm"), in_row(2 * m + core))

    def bias_row(peer):
        return send(bsrc, brow.at[row], sem("brow"), sem("browed"), in_row(peer))

    def bias_col(peer):
        return send(bmid, bcol.at[col], sem("bcol"), sem("bcoled"), in_col(peer))

    def core_term(q):
        return send(wp.at[1 - core, q], cbuf.at[q], sem("core"), kr.at[q], in_row(mate))

    def chip_term(q, m):
        return send(xs.at[q, m], xbuf.at[q, chip], sem("chip"), xsr.at[q], in_row(2 * m + core))

    def col_term(peer):
        return send(zs.at[peer], zbuf.at[col], sem("col"), sem("coled"), in_col(peer))

    def col_whole(peer):
        piece = wg_ref.at[core, col, chip]
        return send(piece, piece, sem("allcol"), azr.at[col], in_col(peer))

    def chip_whole(q, m):
        piece = wg_ref.at[core, q, chip]
        return send(piece, piece, sem("allchip"), axr.at[q], in_row(2 * m + core))

    def core_whole(q):
        piece = wg_ref.at[core, q]
        return send(piece, piece, sem("allcore"), sem("done"), in_row(mate))

    others = pl.ds(0, chips - 1)
    own_left = pl.ds(pl.multiple_of(col * lw, lw), lw)
    own_right = pl.ds(pl.multiple_of(row * rw, rw), rw)
    loads = [
        pltpu.make_async_copy(src, dst, loc.at[k])
        for k, (src, dst) in enumerate([
            (l_ref, lo.at[own_left]), (r_ref, ro.at[own_right]), (w_ref, w_v), (cot_ref, cot_v), (b_ref, b_v),
        ])
    ]
    barrier = pltpu.get_barrier_semaphore()
    for load in loads:
        load.start()
    each(ncol, col, lambda p: pl.semaphore_signal(
        barrier, inc=1, device_id=in_col(p), device_id_type=MESH))
    each(nrow, row, lambda p: pl.semaphore_signal(
        barrier, inc=1, device_id=in_row(p), device_id_type=MESH))
    pl.semaphore_wait(barrier, nrow + ncol - 2)
    loads[0].wait()
    loads[1].wait()

    for s in range(2):
        @pl.when(col < ncol - 1)
        def _():
            left_own(s, 1).start()

        @pl.when(col > 0)
        def _():
            left_own(s, -1).start()

    each_chip(lambda m: right_own(2 * m + core, "same").start())
    right_own(mate, "mate").start()

    loads[2].wait()
    loads[3].wait()
    for d in range(width):
        tmp[d * width : (d + 1) * width, :] = w_v[pl.ds(d, width, stride=width), :]
    weight = tmp[0:channels, :]
    w_c[:, 0:pair_width], w_c[:, pair_width:] = split(weight)
    high, wt_l[...] = split(weight.T * scale)
    wt2[0:pair_width, :] = high
    wt2[pair_width:, :] = high
    cot = cot_v[...]
    c2[:, 0:pair_width], c2[:, pair_width:] = split(cot)
    ct2[0:pair_width, :], ct2[pair_width:, :] = split(cot.T)
    bsrc[...] = jnp.broadcast_to(jnp.sum(cot, axis=0, keepdims=True), (8, pair_width))
    brow[row] = bsrc[...]
    each(nrow, row, lambda p: bias_row(p).start())

    scrs = [scr_a, scr_b]
    steps = channels // lanes_step

    def grad_block(b):
        lanes = slice(b * lanes_step, (b + 1) * lanes_step)
        scrs[b % 2][...] = dot(c2[...], wt2[:, lanes]) + dot(c2[:, 0:pair_width], wt_l[:, lanes])

    def grad_swap(b):
        scr = scrs[b % 2]
        for u in range(STEP // per):
            for v in range(tile_rows // per):
                pieces = [
                    scr[(v * per + a) * tile_cols : (v * per + a + 1) * tile_cols, u * 128 : (u + 1) * 128]
                    for a in range(per)
                ]
                for a, piece in enumerate(swap_groups(pieces)):
                    at = (b * STEP + u * per + a) * tile_cols
                    high, low = split(piece)
                    h_h[at : at + tile_cols, v * 128 : (v + 1) * 128] = high
                    h_l[at : at + tile_cols, v * 128 : (v + 1) * 128] = low

    def relay(k, s):
        @pl.when(inner)
        def _():
            q = along(k)
            left_on(q, s).wait_recv()
            left_on(q, s).start()

    def arrive(k):
        @pl.when(jnp.logical_not(inner))
        def _():
            q = along(k)
            for s in range(2):
                left_on(q, s).wait_recv()

    near = range(1, min(ncol, 3))
    grad_block(0)
    for b in range(steps):
        if b + 1 < steps:
            grad_block(b + 1)
        else:
            for k in near:
                relay(k, 0)
        grad_swap(b)
    for k in near:
        relay(k, 1)

    def right_grad(g, first):
        left = lo[pl.ds(pl.multiple_of(g * glanes, glanes), glanes), :]
        lt_c[:, 0:samples], lt_c[:, samples:] = split(left)
        lanes = pl.ds(pl.multiple_of(g * glanes, glanes), glanes)
        term = dot_wide(h_h[:, lanes], h_l[:, lanes], lt_c[...])
        if first:
            rpa[...] = term
        else:
            rpa[...] += term

    early = 2 if gcols == 1 and groups > 2 else 0
    if early:
        right_grad(group_at(0), True)
    settle(block(ro, 0, (chips - 1) * rw), sem("same"))
    each_chip(lambda m: right_pass(2 * m + core).start())
    if early:
        arrive(1)
        right_grad(group_at(1), False)
    settle(block(ro, 0, rw), sem("mate"))
    settle(block(ro, 0, (chips - 1) * rw), sem("passed"))
    for d in range(width):
        tmp[d * tile_cols : (d + 1) * tile_cols, :] = ro[pl.ds(d, tile_cols, stride=width), :]
    right = tmp[0:rights, :]
    rt_c[:, 0:samples], rt_c[:, samples:] = split(right)
    r2[0:samples, :], r2[samples:, :] = split(right.T)

    @pl.loop(0, groups)
    def _(k):
        g = group_at(groups - 1 - k)
        lanes = pl.ds(pl.multiple_of(g * glanes, glanes), glanes)
        lp[lanes, :] = dot_tall(r2[...], h_h[:, lanes], h_l[:, lanes]).T

    if ncol > 3:
        @pl.loop(3, ncol)
        def _(k):
            relay(k, 0)
            relay(k, 1)

    @pl.loop(0, ncol - 1)
    def _(k):
        peer = along(ncol - 1 - k)

        @pl.when(via_end(col, peer))
        def _():
            left_via(peer).start()

        @pl.when(jnp.logical_not(jnp.logical_or(via_end(col, peer), via_here(peer))))
        def _():
            left_term(peer).start()

        @pl.when(via_end(peer, col))
        def _():
            lbuf[peer] = jnp.zeros(lbuf.shape[1:], F32)

    lbuf[col] = lp[own_left, :]
    settle(brow.at[pl.ds(0, nrow - 1)], sem("browed"))
    bmid[...] = total([brow[q] for q in range(nrow)])
    bcol[col] = bmid[...]
    each(ncol, col, lambda p: bias_col(p).start())
    loads[4].wait()

    if gcols > 1:
        @pl.loop(1, ncol)
        def _(k):
            arrive(k)

    def outer(g):
        left = lo[pl.ds(pl.multiple_of(g * glanes, glanes), glanes), :]
        high, l_l[...] = split(left.T * scale)
        l_c[0:samples, :] = high
        l_c[samples:, :] = high
        half = rights // 2
        for s in range(2):
            at = slice(s * half, (s + 1) * half)
            scrs[s][0:half, 0:glanes] = dot(rt_c[at, :], l_c[...]) + dot(rt_c[at, 0:samples], l_l[...])
        for s in range(2):
            for u in range(width // per // 2):
                for v in range(glanes // 128):
                    pieces = [
                        scrs[s][(u * per + a) * tile_cols : (u * per + a + 1) * tile_cols, v * 128 : (v + 1) * 128]
                        for a in range(per)
                    ]
                    lanes = slice((s * (width // per // 2) + u) * 128, (s * (width // per // 2) + u + 1) * 128)
                    for a, piece in enumerate(swap_groups(pieces)):
                        at = (v * per + a) * tile_cols
                        high, low = split(piece)
                        t_h[at : at + tile_cols, lanes] = high
                        t_l[at : at + tile_cols, lanes] = low

    def weight_grad(g, lanes, first):
        rows = pl.ds(pl.multiple_of(g * grows, grows), grows)
        term = dot_tall(ct2[:, rows], t_h[:, lanes], t_l[:, lanes])
        if first:
            acc[:, lanes] = term
        else:
            acc[:, lanes] += term

    def pair_rows(g):
        rows = pl.ds(pl.multiple_of(g * grows, grows), grows)
        pair_ref[rows, :] = dot_wide(t_h[...], t_l[...], w_c[...]) + b_v[...]

    for k in range(groups - 1):
        g = group_at(k)
        if gcols == 1 and k >= max(1, early):
            arrive(k)
        outer(g)
        weight_grad(g, slice(0, channels), k == 0)
        pair_rows(g)
        if k >= early:
            right_grad(g, k == 0)

    last = group_at(groups - 1)
    if gcols == 1 and groups > 1:
        arrive(groups - 1)
    outer(last)
    weight_grad(last, slice(0, channels), groups == 1)
    for i in range(channels // 128):
        terms = acc[:, i * 128 : (i + 1) * 128].T
        for n in range(128 // share):
            q, m = divmod((i * 128) // share + n, chips)
            b, q = divmod(q, ncol)
            wp[b, q, m] = terms[n * share : (n + 1) * share, :]

    @pl.loop(0, ncol)
    def _(k):
        core_term(along(ncol - 1 - k)).start()

    pair_rows(last)
    right_grad(last, groups == 1)
    if ncol > 3:
        @pl.when(jnp.logical_or(col == 1, col == ncol - 2))
        def _():
            settle(vbuf.at[pl.ds(0, ncol - 3)], sem("via"))

    for p in range(ncol):
        @pl.when(via_here(p))
        def _():
            lp[p * lw : (p + 1) * lw, :] += vbuf[p]
            left_term(p).start()

    @pl.loop(0, ncol)
    def _(k):
        q = along(ncol - 1 - k)
        core_term(q).wait_recv()
        xs[q] = wp[core, q] + cbuf[q]
        xbuf[q, chip] = xs[q, chip]
        each_chip(lambda m: chip_term(q, m).start())

    for d in range(width):
        rp[pl.ds(d, tile_cols, stride=width), :] = rpa[d * tile_cols : (d + 1) * tile_cols, :]
    for m in range(chips):
        right_swap(m).start()
    @pl.loop(0, ncol - 1)
    def _(k):
        q = along(ncol - 1 - k)
        settle(xbuf.at[q, others], xsr.at[q])
        zs[q] = total([xbuf[q, m] for m in range(chips)])
        col_term(q).start()

    settle(mbuf, sem("swapped"))
    for m in range(chips):
        rsum[m] = rp[pl.ds(pl.multiple_of((2 * m + core) * rw, rw), rw), :] + mbuf[m]
    each_chip(lambda m: right_term(m).start())
    rbuf[chip] = rsum[chip]
    settle(xbuf.at[col, others], xsr.at[col])
    zbuf[col] = total([xbuf[col, m] for m in range(chips)])
    settle(bcol.at[pl.ds(0, ncol - 1)], sem("bcoled"))
    bg_ref[...] = total([bcol[q] for q in range(ncol)])[0:1, :] / (tile_rows * nrow)
    near_ends = [jnp.logical_and(ncol > 3, col >= 3), jnp.logical_and(ncol > 3, col <= ncol - 4)]
    absent = near_ends[0].astype(jnp.int32) + near_ends[1].astype(jnp.int32)
    for n in range(3):
        if ncol - 1 - n > 0:
            @pl.when(absent == n)
            def _():
                settle(lbuf.at[pl.ds(0, ncol - 1 - n)], sem("term"))

    lg_ref[...] = total([lbuf[q] for q in range(ncol)])
    settle(zbuf.at[pl.ds(0, ncol - 1)], sem("coled"))
    wg_ref[core, col, chip] = total([zbuf[q] for q in range(ncol)]) / (tile_rows * nrow)

    @pl.loop(1, ncol)
    def _(k):
        col_whole(along(ncol - k)).start()

    each_chip(lambda m: chip_whole(col, m).start())
    ends = jnp.logical_not(inner)

    @pl.when(inner)
    def _():
        settle(lo.at[pl.ds(0, 2 * lw)], sem("left"))
        settle(lo.at[pl.ds(0, (ncol - 1) * lw)], sem("relay"))

    @pl.when(ends)
    def _():
        settle(lo.at[pl.ds(0, lw)], sem("left"))

    settle(ro.at[pl.ds(0, chips * rw)], sem("right"))
    settle(ro.at[pl.ds(0, (chips - 1) * rw)], sem("pass"))
    settle(brow.at[pl.ds(0, nrow - 1)], sem("brow"))
    settle(bcol.at[pl.ds(0, ncol - 1)], sem("bcol"))
    settle(wp.at[0], sem("core"))
    settle(xs.at[:, others], sem("chip"))
    settle(mbuf, sem("swap"))

    @pl.loop(1, ncol)
    def _(k):
        q = along(k)
        piece_in = wg_ref.at[core, q, chip]
        settle(piece_in, azr.at[q])
        each_chip(lambda m: chip_whole(q, m).start())

    @pl.loop(0, ncol)
    def _(k):
        q = along(k)
        settle(wg_ref.at[core, q, others], axr.at[q])
        core_whole(q).start()

    settle(rbuf.at[others], sem("rterm"))
    rg_ref[...] = total([rbuf[m] for m in range(chips)])
    settle(lbuf.at[pl.ds(0, ncol - 1)], sem("terms"))
    settle(rbuf.at[others], sem("rterms"))
    settle(zs.at[pl.ds(0, ncol - 1)], sem("col"))
    settle(zs.at[pl.ds(0, ncol - 1)], sem("allcol"))
    settle(xs.at[:, others], sem("allchip"))
    settle(wg_ref.at[1 - core], sem("done"))
    settle(wg_ref.at[core], sem("allcore"))


def finish_kernel(
    width, pair_ref, lg_ref, rg_ref, wg_ref, bg_ref,
    pair_out, lg_out, rg_out, w_out, bg_out, held, sems,
):
    copies = [
        pltpu.make_async_copy(src, dst, sems.at[k])
        for k, (src, dst) in enumerate([
            (pair_ref, pair_out), (lg_ref, lg_out), (rg_ref, rg_out), (bg_ref, bg_out),
        ])
    ]
    for copy in copies:
        copy.start()
    halves, ncol, chips, share, _ = wg_ref.shape
    for s in range(halves * ncol * chips):
        d, c = divmod(s * share, width)
        q, m = divmod(s, chips)
        b, q = divmod(q, ncol)
        held[pl.ds(c * width + d, share, stride=width), :] = wg_ref[b, q, m]
    last = pltpu.make_async_copy(held, w_out, sems.at[4])
    last.start()
    for copy in [*copies, last]:
        copy.wait()


def per_device(nrow, ncol, left_factors, right_factors, weight, bias, cotangent):
    samples, li, width = left_factors.shape
    rj = right_factors.shape[1]
    tile_rows, tile_cols, pair_width = cotangent.shape
    channels = weight.shape[0]
    lw, rw = li * width, rj * width
    lefts, rights = tile_rows * width, tile_cols * width
    pairs = tile_rows * tile_cols
    chips, share = nrow // 2, channels // (nrow * ncol)
    group = max(lw, STEP * width)
    dma = pltpu.SemaphoreType.DMA

    def shape(*dims):
        return jax.ShapeDtypeStruct(dims, F32)

    def half(*dims):
        return pltpu.VMEM(dims, BF16)

    def buf(*dims):
        return pltpu.VMEM(dims, F32)

    scratch = [
        buf(lefts, samples), buf(rights, samples), buf(lefts, samples), *[buf(ncol, lw, samples)] * 2,
        buf(rights, samples), buf(rights, samples), *[buf(chips, rw, samples)] * 3,
        buf(2, ncol, chips, share, pair_width), *[buf(ncol, chips, share, pair_width)] * 3,
        *[buf(ncol, share, pair_width)] * 2,
        buf(8, pair_width), buf(nrow, 8, pair_width), buf(8, pair_width), buf(ncol, 8, pair_width),
        buf(channels, pair_width), buf(1, pair_width), buf(pairs, pair_width),
        buf(max(rights, channels), 128),
        *[buf(max(pairs, rights), max(group, STEP * width))] * 2, buf(pair_width, channels),
        half(pairs, 2 * pair_width), half(2 * pair_width, pairs), half(channels, 2 * pair_width),
        half(2 * pair_width, channels), half(pair_width, channels),
        half(rights, lefts), half(rights, lefts), half(rights, 2 * samples), half(2 * samples, rights),
        *[half(group // width * tile_cols, channels)] * 2,
        half(2 * samples, group), half(samples, group), half(group, 2 * samples),
        dma((5,)), dma((len(SINGLE),)), dma((ncol, 2)),
        dma((ncol,)), dma((ncol,)), dma((ncol,)), dma((ncol,)),
    ]
    pair, lg, rg, wg, bg = pl.pallas_call(
        functools.partial(tile_kernel, nrow, ncol, width),
        out_shape=(
            shape(pairs, pair_width), shape(lw, samples), shape(rw, samples),
            shape(2, ncol, chips, share, pair_width), shape(1, pair_width),
        ),
        in_specs=[HBM] * 5,
        out_specs=[VMEM] * 5,
        scratch_shapes=scratch,
        compiler_params=pltpu.CompilerParams(
            collective_id=0, has_side_effects=True, vmem_limit_bytes=40 * 2**20
        ),
        name="tile",
    )(
        in_hbm(left_factors.transpose(1, 2, 0).reshape(lw, samples)),
        in_hbm(right_factors.transpose(1, 2, 0).reshape(rw, samples)),
        in_hbm(weight),
        in_hbm(bias.reshape(1, pair_width)),
        in_hbm(cotangent.reshape(pairs, pair_width)),
    )
    pair, lg, rg, wg, bg = pl.pallas_call(
        functools.partial(finish_kernel, width),
        out_shape=(
            shape(pairs, pair_width), shape(lw, samples), shape(rw, samples),
            shape(channels, pair_width), shape(1, pair_width),
        ),
        in_specs=[VMEM] * 5,
        out_specs=[HBM] * 5,
        scratch_shapes=[buf(channels, pair_width), dma((5,))],
        compiler_params=pltpu.CompilerParams(vmem_limit_bytes=8 * 2**20),
        name="finish",
    )(pair, lg, rg, wg, bg)
    return (
        pair.reshape(tile_rows, tile_cols, pair_width),
        lg.reshape(li, width, samples).transpose(2, 0, 1),
        rg.reshape(rj, width, samples).transpose(2, 0, 1),
        wg,
        bg.reshape(pair_width),
    )


def solution(mesh):
    nrow, ncol = mesh.shape["row"], mesh.shape["col"]
    in_specs = (
        P(None, ("row", "col"), None),
        P(None, ("col", "row"), None),
        P(),
        P(),
        P("row", "col", None),
    )
    out_specs = (
        P("row", "col", None),
        P(None, ("row", "col"), None),
        P(None, ("col", "row"), None),
        P(),
        P(),
    )
    return jax.shard_map(
        functools.partial(per_device, nrow, ncol),
        mesh=mesh, in_specs=in_specs, out_specs=out_specs, check_vma=False,
    )
```

```python
import functools

import jax
import jax.numpy as jnp
from jax import lax
from jax.experimental import pallas as pl
from jax.experimental.pallas import tpu as pltpu
from jax.sharding import PartitionSpec as P

F32 = jnp.float32
BF16 = jnp.bfloat16
MESH = pl.DeviceIdType.MESH
VMEM = pl.BlockSpec(memory_space=pltpu.VMEM)
HBM = pl.BlockSpec(memory_space=pltpu.HBM)
STEP = 8
SINGLE = (
    "left", "relay", "right", "pass", "mate", "passed", "terms", "term", "via", "swap", "swapped",
    "rterms", "rterm", "bmate", "bmated", "bchip", "bchiped", "bcol", "bcoled", "core", "chip", "col", "coled",
    "allcol", "allchip", "allcore", "done",
)


def in_hbm(x):
    return pltpu.with_memory_space_constraint(x, pltpu.HBM)


def split(x):
    high = x.astype(BF16)
    return high, (x - high.astype(F32)).astype(BF16)


def dot(a, b):
    return lax.dot_general(a, b, (((1,), (0,)), ((), ())), preferred_element_type=F32)


def dot_wide(a_high, a_low, b_both):
    half = b_both.shape[1] // 2
    wide = dot(a_high, b_both)
    return wide[:, 0:half] + (wide[:, half:] + dot(a_low, b_both[:, 0:half]))


def dot_tall(a_both, b_high, b_low):
    half = a_both.shape[0] // 2
    tall = dot(a_both, b_high)
    return tall[0:half] + (tall[half:] + dot(a_both[0:half], b_low))


def total(parts):
    return functools.reduce(lambda a, b: a + b, parts)


def swap_groups(pieces):
    lane = lax.broadcasted_iota(jnp.int32, pieces[0].shape, 1)
    low = lane < 64
    even = (lane & 32) == 0

    def far(a, b):
        moved = pltpu.roll(jnp.where(low, b, a), 64, 1)
        return jnp.where(low, a, moved), jnp.where(low, moved, b)

    def near(a, b):
        return (
            jnp.where(even, a, pltpu.roll(b, 32, 1)),
            jnp.where(even, pltpu.roll(a, 96, 1), b),
        )

    p0, p2 = far(pieces[0], pieces[2])
    p1, p3 = far(pieces[1], pieces[3])
    p0, p1 = near(p0, p1)
    p2, p3 = near(p2, p3)
    return p0, p1, p2, p3


def tile_kernel(
    nrow, ncol, width, l_ref, r_ref, w_ref, b_ref, cot_ref,
    pair_ref, lg_ref, rg_ref, wg_ref, bg_ref,
    lo, ro, lp, lbuf, vbuf, rpa, rp, mbuf, rsum, rbuf,
    wp, cbuf, xs, xbuf, zs, zbuf, bown, bmate, bsrc, brow, bmid, bcol,
    w_v, b_v, cot_v, tmp, scr_a, scr_b, acc,
    c2, ct2, w_c, wt2, wt_l, h_h, h_l, rt_c, r2, t_h, t_l, l_c, l_l, lt_c,
    loc, one, glr, grr, kr, xsr, azr, axr,
):
    row, col = lax.axis_index("row"), lax.axis_index("col")
    chip, core = row // 2, lax.rem(row, 2)
    mate = row + 1 - 2 * core
    chips = nrow // 2
    lw, samples = l_ref.shape
    rw = r_ref.shape[0]
    tile_rows, tile_cols = ncol * lw // width, nrow * rw // width
    channels, pair_width = w_ref.shape
    rights = tile_cols * width
    scale = 1.0 / samples
    per = 128 // width
    share = channels // (nrow * ncol)
    lanes_step = STEP * width
    gcols = max(1, lanes_step // lw)
    groups = ncol // gcols
    glanes = gcols * lw
    grows = glanes // width * tile_cols
    own_group = col // gcols
    piece = lw // 2
    lower, upper = col, ncol - 1 - col
    both = jnp.minimum(lower, upper)
    longer = jnp.where(lower > upper, -1, 1)
    halfway = ncol // 2
    low_half = col < halfway
    inner = jnp.logical_and(col > 0, col < ncol - 1)

    def along(k):
        paired = k <= 2 * both
        distance = jnp.where(paired, (k + 1) // 2, k - both)
        side = jnp.where(jnp.logical_and(paired, lax.rem(k, 2) == 0), -longer, longer)
        return col + side * distance

    def order(k):
        far = jnp.where(low_half, ncol - 1 - k, k)
        base = jnp.where(low_half, 0, halfway)
        near = base + lax.rem(col - base + 1 + lax.rem(k, halfway), halfway)
        return jnp.where(k < halfway, far, near)

    def group_at(k):
        return along(k) if gcols == 1 else lax.rem(own_group + k, groups)

    def via_end(source, target):
        return jnp.logical_or(
            jnp.logical_and(source == 0, target >= 3),
            jnp.logical_and(source == ncol - 1, target <= ncol - 4),
        )

    def via_here(target):
        return jnp.logical_or(
            jnp.logical_and(col == 1, target >= 3),
            jnp.logical_and(col == ncol - 2, target <= ncol - 4),
        )

    def in_row(peer):
        return {"row": peer, "col": col}

    def in_col(peer):
        return {"row": row, "col": peer}

    def block(ref, index, size):
        return ref.at[pl.ds(pl.multiple_of(index * size, size), size)]

    def each(count, here, act):
        @pl.loop(1, count)
        def _(k):
            act(lax.rem(here + k, count))

    wide = chips // 2
    steps_out = sorted(
        ((a, b) for a in range(wide) for b in range(2) if a + b), key=lambda s: -(min(s[0], wide - s[0]) + s[1])
    )

    def each_chip(act):
        for a, b in steps_out:
            act(lax.rem(chip // 2 + a, wide) * 2 + lax.rem(chip + b, 2))

    def send(src, dst, send_sem, recv_sem, device):
        return pltpu.make_async_remote_copy(
            src_ref=src, dst_ref=dst, send_sem=send_sem, recv_sem=recv_sem,
            device_id=device, device_id_type=MESH,
        )

    def part(ref, index, s):
        return ref.at[pl.ds(pl.multiple_of(index * lw + s * piece, piece), piece)]

    def sem(name):
        return one.at[SINGLE.index(name)]

    def settle(ref, semaphore):
        send(ref, ref, semaphore, semaphore, in_row(mate)).wait_recv()

    def left_own(s, side):
        return send(
            part(lo, col, s), part(lo, col, s), sem("left"), glr.at[col, s], in_col(col + side)
        )

    def left_on(q, s):
        return send(
            part(lo, q, s), part(lo, q, s), sem("relay"), glr.at[q, s], in_col(col + jnp.where(q < col, 1, -1))
        )

    def right_own(peer, recv):
        return send(block(ro, row, rw), block(ro, row, rw), sem("right"), recv, in_row(peer))

    def right_pass(slot):
        return send(block(ro, slot, rw), block(ro, slot, rw), sem("pass"), sem("passed"), in_row(mate))

    def left_term(peer):
        return send(block(lp, peer, lw), lbuf.at[col], sem("terms"), sem("term"), in_col(peer))

    def left_via(peer):
        return send(
            block(lp, peer, lw), vbuf.at[peer], sem("terms"), sem("via"), in_col(jnp.where(col == 0, 1, ncol - 2))
        )

    def right_swap(m):
        return send(block(rp, 2 * m + 1 - core, rw), mbuf.at[m], sem("swap"), sem("swapped"), in_row(mate))

    def right_term(m):
        return send(rsum.at[m], rbuf.at[chip], sem("rterms"), sem("rterm"), in_row(2 * m + core))

    def bias_mate():
        return send(bown, bmate, sem("bmate"), sem("bmated"), in_row(mate))

    def bias_chip(m):
        return send(bsrc, brow.at[chip], sem("bchip"), sem("bchiped"), in_row(2 * m + core))

    def bias_col(peer):
        return send(bmid, bcol.at[col], sem("bcol"), sem("bcoled"), in_col(peer))

    def core_term(q):
        return send(wp.at[1 - core, q], cbuf.at[q], sem("core"), kr.at[q], in_row(mate))

    def chip_term(q, m):
        return send(xs.at[q, m], xbuf.at[q, chip], sem("chip"), xsr.at[q], in_row(2 * m + core))

    def col_term(peer):
        return send(zs.at[peer], zbuf.at[col], sem("col"), sem("coled"), in_col(peer))

    def col_whole(peer):
        piece = wg_ref.at[core, col, chip]
        return send(piece, piece, sem("allcol"), azr.at[col], in_col(peer))

    def chip_whole(q, m):
        piece = wg_ref.at[core, q, chip]
        return send(piece, piece, sem("allchip"), axr.at[q], in_row(2 * m + core))

    def core_whole(q):
        piece = wg_ref.at[core, q]
        return send(piece, piece, sem("allcore"), sem("done"), in_row(mate))

    others = pl.ds(0, chips - 1)
    own_left = pl.ds(pl.multiple_of(col * lw, lw), lw)
    own_right = pl.ds(pl.multiple_of(row * rw, rw), rw)
    loads = [
        pltpu.make_async_copy(src, dst, loc.at[k])
        for k, (src, dst) in enumerate([
            (l_ref, lo.at[own_left]), (r_ref, ro.at[own_right]), (w_ref, w_v), (cot_ref, cot_v), (b_ref, b_v),
        ])
    ]
    barrier = pltpu.get_barrier_semaphore()
    for load in loads:
        load.start()
    def hello(device):
        pl.semaphore_signal(barrier, inc=1, device_id=device, device_id_type=MESH)

    for k in range(1, ncol):
        hello(in_col(lax.rem(col + k, ncol)))
    each_chip(lambda m: hello(in_row(2 * m + core)))
    hello(in_row(mate))
    pl.semaphore_wait(barrier, ncol + chips - 1)
    loads[0].wait()
    loads[1].wait()

    for s in range(2):
        @pl.when(col < ncol - 1)
        def _():
            left_own(s, 1).start()

        @pl.when(col > 0)
        def _():
            left_own(s, -1).start()

    each_chip(lambda m: right_own(2 * m + core, grr.at[chip]).start())
    right_own(mate, sem("mate")).start()

    loads[2].wait()
    loads[3].wait()
    for d in range(width):
        tmp[d * width : (d + 1) * width, :] = w_v[pl.ds(d, width, stride=width), :]
    weight = tmp[0:channels, :]
    w_c[:, 0:pair_width], w_c[:, pair_width:] = split(weight)
    high, wt_l[...] = split(weight.T * scale)
    wt2[0:pair_width, :] = high
    wt2[pair_width:, :] = high
    cot = cot_v[...]
    c2[:, 0:pair_width], c2[:, pair_width:] = split(cot)
    ct2[0:pair_width, :], ct2[pair_width:, :] = split(cot.T)
    bown[...] = jnp.broadcast_to(jnp.sum(cot, axis=0, keepdims=True), (8, pair_width))
    bias_mate().start()

    scrs = [scr_a, scr_b]
    steps = channels // lanes_step

    def grad_block(b):
        lanes = slice(b * lanes_step, (b + 1) * lanes_step)
        scrs[b % 2][...] = dot(c2[...], wt2[:, lanes]) + dot(c2[:, 0:pair_width], wt_l[:, lanes])

    def grad_swap(b):
        scr = scrs[b % 2]
        for u in range(STEP // per):
            for v in range(tile_rows // per):
                pieces = [
                    scr[(v * per + a) * tile_cols : (v * per + a + 1) * tile_cols, u * 128 : (u + 1) * 128]
                    for a in range(per)
                ]
                for a, piece in enumerate(swap_groups(pieces)):
                    at = (b * STEP + u * per + a) * tile_cols
                    high, low = split(piece)
                    h_h[at : at + tile_cols, v * 128 : (v + 1) * 128] = high
                    h_l[at : at + tile_cols, v * 128 : (v + 1) * 128] = low

    def relay(k, s):
        @pl.when(inner)
        def _():
            q = along(k)
            left_on(q, s).wait_recv()
            left_on(q, s).start()

    def arrive(k):
        @pl.when(jnp.logical_not(inner))
        def _():
            q = along(k)
            for s in range(2):
                left_on(q, s).wait_recv()

    near = range(1, min(ncol, 3))
    grad_block(0)
    for b in range(steps):
        if b + 1 < steps:
            grad_block(b + 1)
        grad_swap(b)
    for k in near:
        relay(k, 0)

    def right_grad(g, first):
        left = lo[pl.ds(pl.multiple_of(g * glanes, glanes), glanes), :]
        lt_c[:, 0:samples], lt_c[:, samples:] = split(left)
        lanes = pl.ds(pl.multiple_of(g * glanes, glanes), glanes)
        term = dot_wide(h_h[:, lanes], h_l[:, lanes], lt_c[...])
        if first:
            rpa[...] = term
        else:
            rpa[...] += term

    early = 2 if gcols == 1 and groups > 2 else 0
    if early:
        right_grad(group_at(0), True)
    for k in near:
        relay(k, 1)
    settle(bmate, sem("bmated"))
    bsrc[...] = bown[...] + bmate[...]
    brow[chip] = bsrc[...]
    each_chip(lambda m: bias_chip(m).start())

    def hand_over(m):
        settle(block(ro, 0, rw), grr.at[m])
        right_pass(2 * m + core).start()

    for a, b in reversed(steps_out):
        hand_over(lax.rem(chip // 2 + a, wide) * 2 + lax.rem(chip + b, 2))
    if early:
        arrive(1)
        right_grad(group_at(1), False)
    settle(block(ro, 0, rw), sem("mate"))
    settle(block(ro, 0, (chips - 1) * rw), sem("passed"))
    for d in range(width):
        tmp[d * tile_cols : (d + 1) * tile_cols, :] = ro[pl.ds(d, tile_cols, stride=width), :]
    right = tmp[0:rights, :]
    rt_c[:, 0:samples], rt_c[:, samples:] = split(right)
    r2[0:samples, :], r2[samples:, :] = split(right.T)

    def left_grad(k):
        g = group_at(groups - 1 - k)
        lanes = pl.ds(pl.multiple_of(g * glanes, glanes), glanes)
        lp[lanes, :] = dot_tall(r2[...], h_h[:, lanes], h_l[:, lanes]).T

    def far_relay(s):
        if ncol > 3:
            @pl.loop(3, ncol)
            def _(k):
                relay(k, s)

    half = groups // 2

    @pl.loop(0, half)
    def _(k):
        left_grad(k)

    far_relay(0)
    @pl.loop(half, groups)
    def _(k):
        left_grad(k)

    far_relay(1)

    @pl.loop(0, ncol - 1)
    def _(k):
        peer = along(ncol - 1 - k)

        @pl.when(via_end(col, peer))
        def _():
            left_via(peer).start()

        @pl.when(jnp.logical_not(jnp.logical_or(via_end(col, peer), via_here(peer))))
        def _():
            left_term(peer).start()

        @pl.when(via_end(peer, col))
        def _():
            lbuf[peer] = jnp.zeros(lbuf.shape[1:], F32)

    lbuf[col] = lp[own_left, :]
    settle(brow.at[others], sem("bchiped"))
    bmid[...] = total([brow[m] for m in range(chips)])
    bcol[col] = bmid[...]
    each(ncol, col, lambda p: bias_col(p).start())
    loads[4].wait()

    if gcols > 1:
        @pl.loop(1, ncol)
        def _(k):
            arrive(k)

    middle = channels // 2

    def outer(g, halves, then):
        left = lo[pl.ds(pl.multiple_of(g * glanes, glanes), glanes), :]
        high, l_l[...] = split(left.T * scale)
        l_c[0:samples, :] = high
        l_c[samples:, :] = high
        half = rights // 2
        units = width // per // 2
        for scr, h in zip(scrs, halves):
            at = pl.ds(pl.multiple_of(h * half, half), half)
            scr[0:half, 0:glanes] = dot(rt_c[at, :], l_c[...]) + dot(rt_c[at, 0:samples], l_l[...])
        for scr, h in zip(scrs, halves):
            for u in range(units):
                for v in range(glanes // 128):
                    pieces = [
                        scr[(u * per + a) * tile_cols : (u * per + a + 1) * tile_cols, v * 128 : (v + 1) * 128]
                        for a in range(per)
                    ]
                    lanes = pl.ds(pl.multiple_of(h * middle + u * 128, 128), 128)
                    for a, piece in enumerate(swap_groups(pieces)):
                        at = (v * per + a) * tile_cols
                        high, low = split(piece)
                        rows = pl.ds(pl.multiple_of(g * grows + at, tile_cols), tile_cols)
                        t_h[rows, lanes] = high
                        t_l[rows, lanes] = low
            then(h)

    def weight_grad(g, lanes, first):
        rows = pl.ds(pl.multiple_of(g * grows, grows), grows)
        term = dot_tall(ct2[:, rows], t_h[rows, lanes], t_l[rows, lanes])
        if first:
            acc[:, lanes] = term
        else:
            acc[:, lanes] += term

    for k in range(groups - 1):
        g = group_at(k)
        if gcols == 1 and k >= max(1, early):
            arrive(k)
        outer(g, (0, 1), lambda h: None)
        weight_grad(g, slice(0, channels), k == 0)

    last = group_at(groups - 1)
    if gcols == 1 and groups > 1:
        arrive(groups - 1)
    turned = jnp.where(low_half, 1, 0)

    def last_half(h):
        start = pl.multiple_of(h * middle, middle)
        weight_grad(last, pl.ds(start, middle), groups == 1)
        for i in range(middle // 128):
            terms = acc[:, pl.ds(pl.multiple_of(start + i * 128, 128), 128)].T
            for n in range(128 // share):
                b, q = divmod((i * 128) // share + n, halfway * chips)
                q, m = divmod(q, chips)
                wp[b, h * halfway + q, m] = terms[n * share : (n + 1) * share, :]
        for q in range(halfway):
            core_term(h * halfway + q).start()

    outer(last, (turned, 1 - turned), last_half)

    def chip_terms(first):
        for k in range(first, first + halfway):
            q = order(k)
            core_term(q).wait_recv()
            xs[q] = wp[core, q] + cbuf[q]
            xbuf[q, chip] = xs[q, chip]
            each_chip(lambda m: chip_term(q, m).start())

    chip_terms(0)
    if ncol > 3:
        @pl.when(jnp.logical_or(col == 1, col == ncol - 2))
        def _():
            settle(vbuf.at[pl.ds(0, ncol - 3)], sem("via"))

    for p in range(ncol):
        @pl.when(via_here(p))
        def _():
            lp[p * lw : (p + 1) * lw, :] += vbuf[p]
            left_term(p).start()

    for k in range(early, groups):
        right_grad(group_at(k), k == 0)
    chip_terms(halfway)
    for d in range(width):
        rp[pl.ds(d, tile_cols, stride=width), :] = rpa[d * tile_cols : (d + 1) * tile_cols, :]
    for m in range(chips):
        right_swap(m).start()
    pair_ref[...] = dot_wide(t_h[...], t_l[...], w_c[...]) + b_v[...]
    settle(mbuf, sem("swapped"))
    for m in range(chips):
        rsum[m] = rp[pl.ds(pl.multiple_of((2 * m + core) * rw, rw), rw), :] + mbuf[m]
    each_chip(lambda m: right_term(m).start())
    rbuf[chip] = rsum[chip]
    for k in range(ncol - 1):
        q = order(k)
        settle(xbuf.at[q, others], xsr.at[q])
        zs[q] = total([xbuf[q, m] for m in range(chips)])
        col_term(q).start()

    settle(xbuf.at[col, others], xsr.at[col])
    zbuf[col] = total([xbuf[col, m] for m in range(chips)])
    settle(bcol.at[pl.ds(0, ncol - 1)], sem("bcoled"))
    bg_ref[...] = total([bcol[q] for q in range(ncol)])[0:1, :] / (tile_rows * nrow)
    near_ends = [jnp.logical_and(ncol > 3, col >= 3), jnp.logical_and(ncol > 3, col <= ncol - 4)]
    absent = near_ends[0].astype(jnp.int32) + near_ends[1].astype(jnp.int32)
    for n in range(3):
        if ncol - 1 - n > 0:
            @pl.when(absent == n)
            def _():
                settle(lbuf.at[pl.ds(0, ncol - 1 - n)], sem("term"))

    lg_ref[...] = total([lbuf[q] for q in range(ncol)])
    settle(zbuf.at[pl.ds(0, ncol - 1)], sem("coled"))
    wg_ref[core, col, chip] = total([zbuf[q] for q in range(ncol)]) / (tile_rows * nrow)

    @pl.loop(1, ncol)
    def _(k):
        col_whole(along(ncol - k)).start()

    each_chip(lambda m: chip_whole(col, m).start())
    ends = jnp.logical_not(inner)

    @pl.when(inner)
    def _():
        settle(lo.at[pl.ds(0, 2 * lw)], sem("left"))
        settle(lo.at[pl.ds(0, (ncol - 1) * lw)], sem("relay"))

    @pl.when(ends)
    def _():
        settle(lo.at[pl.ds(0, lw)], sem("left"))

    settle(ro.at[pl.ds(0, chips * rw)], sem("right"))
    settle(ro.at[pl.ds(0, (chips - 1) * rw)], sem("pass"))
    settle(bown, sem("bmate"))
    settle(brow.at[others], sem("bchip"))
    settle(bcol.at[pl.ds(0, ncol - 1)], sem("bcol"))
    settle(wp.at[0], sem("core"))
    settle(xs.at[:, others], sem("chip"))
    settle(mbuf, sem("swap"))

    @pl.loop(1, ncol)
    def _(k):
        q = along(k)
        piece_in = wg_ref.at[core, q, chip]
        settle(piece_in, azr.at[q])
        each_chip(lambda m: chip_whole(q, m).start())

    @pl.loop(0, ncol)
    def _(k):
        q = along(k)
        settle(wg_ref.at[core, q, others], axr.at[q])
        core_whole(q).start()

    settle(rbuf.at[others], sem("rterm"))
    rg_ref[...] = total([rbuf[m] for m in range(chips)])
    settle(lbuf.at[pl.ds(0, ncol - 1)], sem("terms"))
    settle(rbuf.at[others], sem("rterms"))
    settle(zs.at[pl.ds(0, ncol - 1)], sem("col"))
    settle(zs.at[pl.ds(0, ncol - 1)], sem("allcol"))
    settle(xs.at[:, others], sem("allchip"))
    settle(wg_ref.at[1 - core], sem("done"))
    settle(wg_ref.at[core], sem("allcore"))


def finish_kernel(
    width, pair_ref, lg_ref, rg_ref, wg_ref, bg_ref,
    pair_out, lg_out, rg_out, w_out, bg_out, sems,
):
    halves, ncol, chips, share, _ = wg_ref.shape
    copies = [
        pltpu.make_async_copy(src, dst, sems.at[k])
        for k, (src, dst) in enumerate([
            (pair_ref, pair_out), (lg_ref, lg_out), (rg_ref, rg_out), (bg_ref, bg_out),
        ])
    ]
    for s in range(halves * ncol * chips):
        d, c = divmod(s * share, width)
        q, m = divmod(s, chips)
        h, q = divmod(q, ncol)
        b, q = divmod(q, ncol // 2)
        q += h * (ncol // 2)
        pltpu.make_async_copy(wg_ref.at[b, q, m], w_out.at[pl.ds(c, share), d], sems.at[4]).start()
    for copy in copies:
        copy.start()
    for copy in copies:
        copy.wait()
    pltpu.make_async_copy(wg_ref, wg_ref, sems.at[4]).wait()


def per_device(nrow, ncol, left_factors, right_factors, weight, bias, cotangent):
    samples, li, width = left_factors.shape
    rj = right_factors.shape[1]
    tile_rows, tile_cols, pair_width = cotangent.shape
    channels = weight.shape[0]
    lw, rw = li * width, rj * width
    lefts, rights = tile_rows * width, tile_cols * width
    pairs = tile_rows * tile_cols
    chips, share = nrow // 2, channels // (nrow * ncol)
    group = max(lw, STEP * width)
    dma = pltpu.SemaphoreType.DMA

    def shape(*dims):
        return jax.ShapeDtypeStruct(dims, F32)

    def half(*dims):
        return pltpu.VMEM(dims, BF16)

    def buf(*dims):
        return pltpu.VMEM(dims, F32)

    scratch = [
        buf(lefts, samples), buf(rights, samples), buf(lefts, samples), *[buf(ncol, lw, samples)] * 2,
        buf(rights, samples), buf(rights, samples), *[buf(chips, rw, samples)] * 3,
        buf(2, ncol, chips, share, pair_width), *[buf(ncol, chips, share, pair_width)] * 3,
        *[buf(ncol, share, pair_width)] * 2,
        *[buf(8, pair_width)] * 3, buf(chips, 8, pair_width), buf(8, pair_width), buf(ncol, 8, pair_width),
        buf(channels, pair_width), buf(1, pair_width), buf(pairs, pair_width),
        buf(max(rights, channels), 128),
        *[buf(max(pairs, rights), max(group, STEP * width))] * 2, buf(pair_width, channels),
        half(pairs, 2 * pair_width), half(2 * pair_width, pairs), half(channels, 2 * pair_width),
        half(2 * pair_width, channels), half(pair_width, channels),
        half(rights, lefts), half(rights, lefts), half(rights, 2 * samples), half(2 * samples, rights),
        half(pairs, channels), half(pairs, channels),
        half(2 * samples, group), half(samples, group), half(group, 2 * samples),
        dma((5,)), dma((len(SINGLE),)), dma((ncol, 2)), dma((chips,)),
        dma((ncol,)), dma((ncol,)), dma((ncol,)), dma((ncol,)),
    ]
    pair, lg, rg, wg, bg = pl.pallas_call(
        functools.partial(tile_kernel, nrow, ncol, width),
        out_shape=(
            shape(pairs, pair_width), shape(lw, samples), shape(rw, samples),
            shape(2, ncol, chips, share, pair_width), shape(1, pair_width),
        ),
        in_specs=[HBM] * 5,
        out_specs=[VMEM] * 5,
        scratch_shapes=scratch,
        compiler_params=pltpu.CompilerParams(
            collective_id=0, has_side_effects=True, vmem_limit_bytes=40 * 2**20
        ),
        name="tile",
    )(
        in_hbm(left_factors.transpose(1, 2, 0).reshape(lw, samples)),
        in_hbm(right_factors.transpose(1, 2, 0).reshape(rw, samples)),
        in_hbm(weight),
        in_hbm(bias.reshape(1, pair_width)),
        in_hbm(cotangent.reshape(pairs, pair_width)),
    )
    pair, lg, rg, wg, bg = pl.pallas_call(
        functools.partial(finish_kernel, width),
        out_shape=(
            shape(pairs, pair_width), shape(lw, samples), shape(rw, samples),
            shape(width, channels // width, pair_width), shape(1, pair_width),
        ),
        in_specs=[VMEM] * 5,
        out_specs=[HBM] * 5,
        scratch_shapes=[dma((5,))],
        compiler_params=pltpu.CompilerParams(vmem_limit_bytes=8 * 2**20),
        name="finish",
    )(pair, lg, rg, wg, bg)
    return (
        pair.reshape(tile_rows, tile_cols, pair_width),
        lg.reshape(li, width, samples).transpose(2, 0, 1),
        rg.reshape(rj, width, samples).transpose(2, 0, 1),
        wg.reshape(channels, pair_width),
        bg.reshape(pair_width),
    )


def solution(mesh):
    nrow, ncol = mesh.shape["row"], mesh.shape["col"]
    in_specs = (
        P(None, ("row", "col"), None),
        P(None, ("col", "row"), None),
        P(),
        P(),
        P("row", "col", None),
    )
    out_specs = (
        P("row", "col", None),
        P(None, ("row", "col"), None),
        P(None, ("col", "row"), None),
        P(),
        P(),
    )
    return jax.shard_map(
        functools.partial(per_device, nrow, ncol),
        mesh=mesh, in_specs=in_specs, out_specs=out_specs, check_vma=False,
    )
```

```python
import functools

import jax
import jax.numpy as jnp
from jax import lax
from jax.experimental import pallas as pl
from jax.experimental.pallas import tpu as pltpu
from jax.sharding import PartitionSpec as P

F32 = jnp.float32
BF16 = jnp.bfloat16
MESH = pl.DeviceIdType.MESH
VMEM = pl.BlockSpec(memory_space=pltpu.VMEM)
HBM = pl.BlockSpec(memory_space=pltpu.HBM)
STEP = 8
SINGLE = (
    "left", "leftfar", "relay", "right", "pass", "mate", "passed", "terms", "term", "via", "swap", "swapped",
    "rterms", "rterm", "bmate", "bmated", "bchip", "bchiped", "bcol", "bcoled", "core", "chip", "col", "coled",
    "allcol", "allchip", "allcore", "done",
)


def in_hbm(x):
    return pltpu.with_memory_space_constraint(x, pltpu.HBM)


def split(x):
    high = x.astype(BF16)
    return high, (x - high.astype(F32)).astype(BF16)


def dot(a, b):
    return lax.dot_general(a, b, (((1,), (0,)), ((), ())), preferred_element_type=F32)


def dot_wide(a_high, a_low, b_both):
    half = b_both.shape[1] // 2
    wide = dot(a_high, b_both)
    return wide[:, 0:half] + (wide[:, half:] + dot(a_low, b_both[:, 0:half]))


def dot_tall(a_both, b_high, b_low):
    half = a_both.shape[0] // 2
    tall = dot(a_both, b_high)
    return tall[0:half] + (tall[half:] + dot(a_both[0:half], b_low))


def total(parts):
    return functools.reduce(lambda a, b: a + b, parts)


def swap_groups(pieces):
    lane = lax.broadcasted_iota(jnp.int32, pieces[0].shape, 1)
    low = lane < 64
    even = (lane & 32) == 0

    def far(a, b):
        moved = pltpu.roll(jnp.where(low, b, a), 64, 1)
        return jnp.where(low, a, moved), jnp.where(low, moved, b)

    def near(a, b):
        return (
            jnp.where(even, a, pltpu.roll(b, 32, 1)),
            jnp.where(even, pltpu.roll(a, 96, 1), b),
        )

    p0, p2 = far(pieces[0], pieces[2])
    p1, p3 = far(pieces[1], pieces[3])
    p0, p1 = near(p0, p1)
    p2, p3 = near(p2, p3)
    return p0, p1, p2, p3


def tile_kernel(
    nrow, ncol, width, l_ref, r_ref, w_ref, b_ref, cot_ref,
    pair_ref, lg_ref, rg_ref, wg_ref, bg_ref,
    lo, ro, lp, lbuf, vbuf, rpa, rp, mbuf, rsum, rbuf,
    wp, cbuf, xs, xbuf, zs, zbuf, bown, bmate, bsrc, brow, bmid, bcol,
    w_v, b_v, cot_v, tmp, scr_a, scr_b, acc,
    c2, ct2, w_c, wt2, wt_l, h_h, h_l, rt_c, r2, t_h, t_l, l_c, l_l, lt_c,
    loc, one, glr, grr, kr, xsr, azr, axr,
):
    row, col = lax.axis_index("row"), lax.axis_index("col")
    chip, core = row // 2, lax.rem(row, 2)
    mate = row + 1 - 2 * core
    chips = nrow // 2
    lw, samples = l_ref.shape
    rw = r_ref.shape[0]
    tile_rows, tile_cols = ncol * lw // width, nrow * rw // width
    channels, pair_width = w_ref.shape
    rights = tile_cols * width
    scale = 1.0 / samples
    per = 128 // width
    share = channels // (nrow * ncol)
    lanes_step = STEP * width
    gcols = max(1, lanes_step // lw)
    groups = ncol // gcols
    glanes = gcols * lw
    grows = glanes // width * tile_cols
    own_group = col // gcols
    piece = lw // 2
    lower, upper = col, ncol - 1 - col
    both = jnp.minimum(lower, upper)
    longer = jnp.where(lower > upper, -1, 1)
    halfway = ncol // 2
    low_half = col < halfway
    inner = jnp.logical_and(col > 0, col < ncol - 1)

    def along(k):
        paired = k <= 2 * both
        distance = jnp.where(paired, (k + 1) // 2, k - both)
        side = jnp.where(jnp.logical_and(paired, lax.rem(k, 2) == 0), -longer, longer)
        return col + side * distance

    def order(k):
        far = jnp.where(low_half, ncol - 1 - k, k)
        base = jnp.where(low_half, 0, halfway)
        near = base + lax.rem(col - base + 1 + lax.rem(k, halfway), halfway)
        return jnp.where(k < halfway, far, near)

    def group_at(k):
        return along(k) if gcols == 1 else lax.rem(own_group + k, groups)

    def via_end(source, target):
        return jnp.logical_or(
            jnp.logical_and(source == 0, target >= 3),
            jnp.logical_and(source == ncol - 1, target <= ncol - 4),
        )

    def via_here(target):
        return jnp.logical_or(
            jnp.logical_and(col == 1, target >= 3),
            jnp.logical_and(col == ncol - 2, target <= ncol - 4),
        )

    def in_row(peer):
        return {"row": peer, "col": col}

    def in_col(peer):
        return {"row": row, "col": peer}

    def block(ref, index, size):
        return ref.at[pl.ds(pl.multiple_of(index * size, size), size)]

    def each(count, here, act):
        @pl.loop(1, count)
        def _(k):
            act(lax.rem(here + k, count))

    wide = chips // 2
    steps_out = sorted(
        ((a, b) for a in range(wide) for b in range(2) if a + b), key=lambda s: -(min(s[0], wide - s[0]) + s[1])
    )

    def each_chip(act):
        for a, b in steps_out:
            act(lax.rem(chip // 2 + a, wide) * 2 + lax.rem(chip + b, 2))

    def send(src, dst, send_sem, recv_sem, device):
        return pltpu.make_async_remote_copy(
            src_ref=src, dst_ref=dst, send_sem=send_sem, recv_sem=recv_sem,
            device_id=device, device_id_type=MESH,
        )

    def part(ref, index, s):
        return ref.at[pl.ds(pl.multiple_of(index * lw + s * piece, piece), piece)]

    def sem(name):
        return one.at[SINGLE.index(name)]

    def here(act):
        pl.when(row >= 0)(act)

    def settle(ref, semaphore):
        send(ref, ref, semaphore, semaphore, in_row(mate)).wait_recv()

    def left_own(s, side):
        return send(
            part(lo, col, s), part(lo, col, s), sem("left"), glr.at[col, s], in_col(col + side)
        )

    def left_far(peer, s):
        return send(part(lo, col, s), part(lo, col, s), sem("leftfar"), glr.at[col, s], in_col(peer))

    def far_off(peer):
        return jnp.abs(peer - col) >= 3

    def left_on(q, s):
        return send(
            part(lo, q, s), part(lo, q, s), sem("relay"), glr.at[q, s], in_col(col + jnp.where(q < col, 1, -1))
        )

    def right_own(peer, recv):
        return send(block(ro, row, rw), block(ro, row, rw), sem("right"), recv, in_row(peer))

    def right_pass(slot):
        return send(block(ro, slot, rw), block(ro, slot, rw), sem("pass"), sem("passed"), in_row(mate))

    def left_term(peer):
        return send(block(lp, peer, lw), lbuf.at[col], sem("terms"), sem("term"), in_col(peer))

    def left_via(peer):
        return send(
            block(lp, peer, lw), vbuf.at[peer], sem("terms"), sem("via"), in_col(jnp.where(col == 0, 1, ncol - 2))
        )

    def right_swap(m):
        return send(block(rp, 2 * m + 1 - core, rw), mbuf.at[m], sem("swap"), sem("swapped"), in_row(mate))

    def right_term(m):
        return send(rsum.at[m], rbuf.at[chip], sem("rterms"), sem("rterm"), in_row(2 * m + core))

    def bias_mate():
        return send(bown, bmate, sem("bmate"), sem("bmated"), in_row(mate))

    def bias_chip(m):
        return send(bsrc, brow.at[chip], sem("bchip"), sem("bchiped"), in_row(2 * m + core))

    def bias_col(peer):
        return send(bmid, bcol.at[col], sem("bcol"), sem("bcoled"), in_col(peer))

    def core_term(q):
        return send(wp.at[1 - core, q], cbuf.at[q], sem("core"), kr.at[q], in_row(mate))

    def chip_term(q, m):
        return send(xs.at[q, m], xbuf.at[q, chip], sem("chip"), xsr.at[q], in_row(2 * m + core))

    def col_term(peer):
        return send(zs.at[peer], zbuf.at[col], sem("col"), sem("coled"), in_col(peer))

    def col_whole(peer):
        piece = wg_ref.at[core, col, chip]
        return send(piece, piece, sem("allcol"), azr.at[col], in_col(peer))

    def chip_whole(q, m):
        piece = wg_ref.at[core, q, chip]
        return send(piece, piece, sem("allchip"), axr.at[q], in_row(2 * m + core))

    def core_whole(q):
        piece = wg_ref.at[core, q]
        return send(piece, piece, sem("allcore"), sem("done"), in_row(mate))

    others = pl.ds(0, chips - 1)
    own_left = pl.ds(pl.multiple_of(col * lw, lw), lw)
    own_right = pl.ds(pl.multiple_of(row * rw, rw), rw)
    loads = [
        pltpu.make_async_copy(src, dst, loc.at[k])
        for k, (src, dst) in enumerate([
            (l_ref, lo.at[own_left]), (r_ref, ro.at[own_right]), (w_ref, w_v), (cot_ref, cot_v), (b_ref, b_v),
        ])
    ]
    barrier = pltpu.get_barrier_semaphore()
    for load in loads:
        load.start()
    def hello(device):
        pl.semaphore_signal(barrier, inc=1, device_id=device, device_id_type=MESH)

    for k in range(1, ncol):
        hello(in_col(lax.rem(col + k, ncol)))
    each_chip(lambda m: hello(in_row(2 * m + core)))
    hello(in_row(mate))
    pl.semaphore_wait(barrier, ncol + chips - 1)
    loads[0].wait()
    loads[1].wait()

    for s in range(2):
        @pl.when(col < ncol - 1)
        def _():
            left_own(s, 1).start()

        @pl.when(col > 0)
        def _():
            left_own(s, -1).start()

    for peer in range(ncol):
        @pl.when(far_off(peer))
        def _():
            for s in range(2):
                left_far(peer, s).start()

    @here
    def _():
        each_chip(lambda m: right_own(2 * m + core, grr.at[chip]).start())
        right_own(mate, sem("mate")).start()


    loads[2].wait()
    loads[3].wait()
    for d in range(width):
        tmp[d * width : (d + 1) * width, :] = w_v[pl.ds(d, width, stride=width), :]
    weight = tmp[0:channels, :]
    w_c[:, 0:pair_width], w_c[:, pair_width:] = split(weight)
    high, wt_l[...] = split(weight.T * scale)
    wt2[0:pair_width, :] = high
    wt2[pair_width:, :] = high
    cot = cot_v[...]
    c2[:, 0:pair_width], c2[:, pair_width:] = split(cot)
    ct2[0:pair_width, :], ct2[pair_width:, :] = split(cot.T)
    bown[...] = jnp.broadcast_to(jnp.sum(cot, axis=0, keepdims=True), (8, pair_width))
    bias_mate().start()

    scrs = [scr_a, scr_b]
    steps = channels // lanes_step

    def grad_block(b):
        lanes = slice(b * lanes_step, (b + 1) * lanes_step)
        scrs[b % 2][...] = dot(c2[...], wt2[:, lanes]) + dot(c2[:, 0:pair_width], wt_l[:, lanes])

    def grad_swap(b):
        scr = scrs[b % 2]
        for u in range(STEP // per):
            for v in range(tile_rows // per):
                pieces = [
                    scr[(v * per + a) * tile_cols : (v * per + a + 1) * tile_cols, u * 128 : (u + 1) * 128]
                    for a in range(per)
                ]
                for a, piece in enumerate(swap_groups(pieces)):
                    at = (b * STEP + u * per + a) * tile_cols
                    high, low = split(piece)
                    h_h[at : at + tile_cols, v * 128 : (v + 1) * 128] = high
                    h_l[at : at + tile_cols, v * 128 : (v + 1) * 128] = low

    def relay(k, s):
        @pl.when(inner)
        def _():
            q = along(k)
            left_on(q, s).wait_recv()
            left_on(q, s).start()

    def arrive(k):
        @pl.when(jnp.logical_or(k > 2, jnp.logical_not(inner)))
        def _():
            q = along(k)
            for s in range(2):
                left_on(q, s).wait_recv()

    near = range(1, min(ncol, 3))
    grad_block(0)
    for b in range(steps):
        if b + 1 < steps:
            grad_block(b + 1)
        grad_swap(b)
    for k in near:
        relay(k, 0)

    def right_grad(g, first):
        left = lo[pl.ds(pl.multiple_of(g * glanes, glanes), glanes), :]
        lt_c[:, 0:samples], lt_c[:, samples:] = split(left)
        lanes = pl.ds(pl.multiple_of(g * glanes, glanes), glanes)
        term = dot_wide(h_h[:, lanes], h_l[:, lanes], lt_c[...])
        if first:
            rpa[...] = term
        else:
            rpa[...] += term

    early = 1 if gcols == 1 and groups > 1 else 0
    if early:
        right_grad(group_at(0), True)
    for k in near:
        relay(k, 1)
    settle(bmate, sem("bmated"))
    bsrc[...] = bown[...] + bmate[...]
    brow[chip] = bsrc[...]
    each_chip(lambda m: bias_chip(m).start())

    def hand_over(m):
        settle(block(ro, 0, rw), grr.at[m])

        @here
        def _():
            right_pass(2 * m + core).start()

    for a, b in reversed(steps_out):
        hand_over(lax.rem(chip // 2 + a, wide) * 2 + lax.rem(chip + b, 2))
    settle(block(ro, 0, rw), sem("mate"))
    settle(block(ro, 0, (chips - 1) * rw), sem("passed"))
    for d in range(width):
        tmp[d * tile_cols : (d + 1) * tile_cols, :] = ro[pl.ds(d, tile_cols, stride=width), :]
    right = tmp[0:rights, :]
    rt_c[:, 0:samples], rt_c[:, samples:] = split(right)
    r2[0:samples, :], r2[samples:, :] = split(right.T)


    def left_grad(k):
        g = group_at(groups - 1 - k)
        lanes = pl.ds(pl.multiple_of(g * glanes, glanes), glanes)
        lp[lanes, :] = dot_tall(r2[...], h_h[:, lanes], h_l[:, lanes]).T

    def send_term(k):
        peer = along(ncol - 1 - k)

        @pl.when(via_end(col, peer))
        def _():
            left_via(peer).start()

        @pl.when(jnp.logical_not(jnp.logical_or(via_end(col, peer), via_here(peer))))
        def _():
            left_term(peer).start()

        @pl.when(via_end(peer, col))
        def _():
            lbuf[peer] = jnp.zeros(lbuf.shape[1:], F32)

    if gcols > 1:
        @pl.loop(1, ncol)
        def _(k):
            arrive(k)

    middle = channels // 2

    def outer(k, halves, beside, then):
        g = group_at(k)
        left = lo[pl.ds(pl.multiple_of(g * glanes, glanes), glanes), :]
        high, l_l[...] = split(left.T * scale)
        l_c[0:samples, :] = high
        l_c[samples:, :] = high
        half = rights // 2
        units = width // per // 2
        for scr, h in zip(scrs, halves):
            at = pl.ds(pl.multiple_of(h * half, half), half)
            scr[0:half, 0:glanes] = dot(rt_c[at, :], l_c[...]) + dot(rt_c[at, 0:samples], l_l[...])
        beside()
        for scr, h in zip(scrs, halves):
            for u in range(units):
                for v in range(glanes // 128):
                    pieces = [
                        scr[(u * per + a) * tile_cols : (u * per + a + 1) * tile_cols, v * 128 : (v + 1) * 128]
                        for a in range(per)
                    ]
                    lanes = pl.ds(pl.multiple_of(h * middle + u * 128, 128), 128)
                    for a, piece in enumerate(swap_groups(pieces)):
                        at = k * grows + (v * per + a) * tile_cols
                        high, low = split(piece)
                        t_h[at : at + tile_cols, lanes] = high
                        t_l[at : at + tile_cols, lanes] = low
            then(h)

    def weight_grad(k, lanes):
        at = slice(k * grows, (k + 1) * grows)
        rows = pl.ds(pl.multiple_of(group_at(k) * grows, grows), grows)
        term = dot_tall(ct2[:, rows], t_h[at, lanes], t_l[at, lanes])
        if k == 0:
            acc[:, lanes] = term
        else:
            acc[:, lanes] += term

    def beside(k):
        if k < groups - 1 or gcols > 1:
            left_grad(k)
        if k > 0:
            weight_grad(k - 1, slice(0, channels))

    for k in range(groups - 1):
        if gcols == 1 and k >= max(1, early):
            arrive(k)
        outer(k, (0, 1), functools.partial(beside, k), lambda h: None)
        if gcols == 1:
            @pl.when(jnp.logical_not(inner))
            def _():
                send_term(k)

    if gcols == 1:
        @pl.when(inner)
        def _():
            for k in range(groups - 1):
                send_term(k)

    if gcols == 1 and groups > 1:
        arrive(groups - 1)
    turned = jnp.where(low_half, 1, 0)

    def last_half(h):
        start = pl.multiple_of(h * middle, middle)
        weight_grad(groups - 1, pl.ds(start, middle))
        for i in range(middle // 128):
            terms = acc[:, pl.ds(pl.multiple_of(start + i * 128, 128), 128)].T
            for n in range(128 // share):
                b, q = divmod((i * 128) // share + n, halfway * chips)
                q, m = divmod(q, chips)
                wp[b, h * halfway + q, m] = terms[n * share : (n + 1) * share, :]

        @here
        def _():
            for q in range(halfway):
                core_term(h * halfway + q).start()

    outer(groups - 1, (turned, 1 - turned), functools.partial(beside, groups - 1), last_half)

    def chip_terms(first):
        for k in range(first, first + halfway):
            q = order(k)
            core_term(q).wait_recv()
            xs[q] = wp[core, q] + cbuf[q]
            xbuf[q, chip] = xs[q, chip]

            @here
            def _():
                each_chip(lambda m: chip_term(q, m).start())

    if gcols > 1:
        for k in range(ncol - 1):
            send_term(k)
    chip_terms(0)
    for k in range(early, groups - 1):
        right_grad(group_at(k), k == 0)
    chip_terms(halfway)
    loads[4].wait()
    if gcols == 1:
        left_grad(groups - 1)
    lbuf[col] = lp[own_left, :]
    right_grad(group_at(groups - 1), groups == 1)
    settle(brow.at[others], sem("bchiped"))
    bmid[...] = total([brow[m] for m in range(chips)])
    bcol[col] = bmid[...]
    each(ncol, col, lambda p: bias_col(p).start())

    for d in range(width):
        rp[pl.ds(d, tile_cols, stride=width), :] = rpa[d * tile_cols : (d + 1) * tile_cols, :]

    @here
    def _():
        for m in range(chips):
            right_swap(m).start()

    pair = dot_wide(t_h[...], t_l[...], w_c[...]) + b_v[...]
    for k in range(groups):
        rows = pl.ds(pl.multiple_of(group_at(k) * grows, grows), grows)
        pair_ref[rows, :] = pair[k * grows : (k + 1) * grows, :]
    settle(mbuf, sem("swapped"))
    for m in range(chips):
        rsum[m] = rp[pl.ds(pl.multiple_of((2 * m + core) * rw, rw), rw), :] + mbuf[m]

    @here
    def _():
        each_chip(lambda m: right_term(m).start())

    rbuf[chip] = rsum[chip]
    for k in range(ncol - 1):
        q = order(k)
        settle(xbuf.at[q, others], xsr.at[q])
        zs[q] = total([xbuf[q, m] for m in range(chips)])

        @here
        def _():
            col_term(q).start()

    if ncol > 3:
        @pl.when(jnp.logical_or(col == 1, col == ncol - 2))
        def _():
            settle(vbuf.at[pl.ds(0, ncol - 3)], sem("via"))

    for p in range(ncol):
        @pl.when(via_here(p))
        def _():
            lp[p * lw : (p + 1) * lw, :] += vbuf[p]
            left_term(p).start()

    settle(xbuf.at[col, others], xsr.at[col])
    zbuf[col] = total([xbuf[col, m] for m in range(chips)])
    settle(zbuf.at[pl.ds(0, ncol - 1)], sem("coled"))
    wg_ref[core, col, chip] = total([zbuf[q] for q in range(ncol)]) / (tile_rows * nrow)

    @pl.loop(1, ncol)
    def _(k):
        col_whole(along(ncol - k)).start()

    @here
    def _():
        each_chip(lambda m: chip_whole(col, m).start())

    ends = jnp.logical_not(inner)

    @pl.when(inner)
    def _():
        settle(lo.at[pl.ds(0, 2 * lw)], sem("left"))
        settle(lo.at[pl.ds(0, 2 * lw)], sem("relay"))

    @pl.when(ends)
    def _():
        settle(lo.at[pl.ds(0, lw)], sem("left"))

    for peer in range(ncol):
        @pl.when(far_off(peer))
        def _():
            settle(lo.at[pl.ds(0, lw)], sem("leftfar"))

    settle(ro.at[pl.ds(0, chips * rw)], sem("right"))
    settle(ro.at[pl.ds(0, (chips - 1) * rw)], sem("pass"))
    settle(bown, sem("bmate"))
    settle(brow.at[others], sem("bchip"))
    settle(bcol.at[pl.ds(0, ncol - 1)], sem("bcol"))
    settle(wp.at[0], sem("core"))
    settle(xs.at[:, others], sem("chip"))
    settle(mbuf, sem("swap"))

    @pl.loop(1, ncol)
    def _(k):
        q = along(k)
        piece_in = wg_ref.at[core, q, chip]
        settle(piece_in, azr.at[q])
        each_chip(lambda m: chip_whole(q, m).start())

    @pl.loop(0, ncol)
    def _(k):
        q = along(k)
        settle(wg_ref.at[core, q, others], axr.at[q])
        core_whole(q).start()

    settle(bcol.at[pl.ds(0, ncol - 1)], sem("bcoled"))
    bg_ref[...] = total([bcol[q] for q in range(ncol)])[0:1, :] / (tile_rows * nrow)
    near_ends = [jnp.logical_and(ncol > 3, col >= 3), jnp.logical_and(ncol > 3, col <= ncol - 4)]
    absent = near_ends[0].astype(jnp.int32) + near_ends[1].astype(jnp.int32)
    for n in range(3):
        if ncol - 1 - n > 0:
            @pl.when(absent == n)
            def _():
                settle(lbuf.at[pl.ds(0, ncol - 1 - n)], sem("term"))

    lg_ref[...] = total([lbuf[q] for q in range(ncol)])
    settle(rbuf.at[others], sem("rterm"))
    rg_ref[...] = total([rbuf[m] for m in range(chips)])
    settle(lbuf.at[pl.ds(0, ncol - 1)], sem("terms"))
    settle(rbuf.at[others], sem("rterms"))
    settle(zs.at[pl.ds(0, ncol - 1)], sem("col"))
    settle(zs.at[pl.ds(0, ncol - 1)], sem("allcol"))
    settle(xs.at[:, others], sem("allchip"))
    settle(wg_ref.at[1 - core], sem("done"))
    settle(wg_ref.at[core], sem("allcore"))


def finish_kernel(
    width, pair_ref, lg_ref, rg_ref, wg_ref, bg_ref,
    pair_out, lg_out, rg_out, w_out, bg_out, sems,
):
    halves, ncol, chips, share, _ = wg_ref.shape
    copies = [
        pltpu.make_async_copy(src, dst, sems.at[k])
        for k, (src, dst) in enumerate([
            (pair_ref, pair_out), (lg_ref, lg_out), (rg_ref, rg_out), (bg_ref, bg_out),
        ])
    ]
    for s in range(halves * ncol * chips):
        d, c = divmod(s * share, width)
        q, m = divmod(s, chips)
        h, q = divmod(q, ncol)
        b, q = divmod(q, ncol // 2)
        q += h * (ncol // 2)
        pltpu.make_async_copy(wg_ref.at[b, q, m], w_out.at[pl.ds(c, share), d], sems.at[4]).start()
    for copy in copies:
        copy.start()
    for copy in copies:
        copy.wait()
    pltpu.make_async_copy(wg_ref, wg_ref, sems.at[4]).wait()


def per_device(nrow, ncol, left_factors, right_factors, weight, bias, cotangent):
    samples, li, width = left_factors.shape
    rj = right_factors.shape[1]
    tile_rows, tile_cols, pair_width = cotangent.shape
    channels = weight.shape[0]
    lw, rw = li * width, rj * width
    lefts, rights = tile_rows * width, tile_cols * width
    pairs = tile_rows * tile_cols
    chips, share = nrow // 2, channels // (nrow * ncol)
    group = max(lw, STEP * width)
    dma = pltpu.SemaphoreType.DMA

    def shape(*dims):
        return jax.ShapeDtypeStruct(dims, F32)

    def half(*dims):
        return pltpu.VMEM(dims, BF16)

    def buf(*dims):
        return pltpu.VMEM(dims, F32)

    scratch = [
        buf(lefts, samples), buf(rights, samples), buf(lefts, samples), *[buf(ncol, lw, samples)] * 2,
        buf(rights, samples), buf(rights, samples), *[buf(chips, rw, samples)] * 3,
        buf(2, ncol, chips, share, pair_width), *[buf(ncol, chips, share, pair_width)] * 3,
        *[buf(ncol, share, pair_width)] * 2,
        *[buf(8, pair_width)] * 3, buf(chips, 8, pair_width), buf(8, pair_width), buf(ncol, 8, pair_width),
        buf(channels, pair_width), buf(1, pair_width), buf(pairs, pair_width),
        buf(max(rights, channels), 128),
        *[buf(max(pairs, rights), max(group, STEP * width))] * 2, buf(pair_width, channels),
        half(pairs, 2 * pair_width), half(2 * pair_width, pairs), half(channels, 2 * pair_width),
        half(2 * pair_width, channels), half(pair_width, channels),
        half(rights, lefts), half(rights, lefts), half(rights, 2 * samples), half(2 * samples, rights),
        half(pairs, channels), half(pairs, channels),
        half(2 * samples, group), half(samples, group), half(group, 2 * samples),
        dma((5,)), dma((len(SINGLE),)), dma((ncol, 2)), dma((chips,)),
        dma((ncol,)), dma((ncol,)), dma((ncol,)), dma((ncol,)),
    ]
    pair, lg, rg, wg, bg = pl.pallas_call(
        functools.partial(tile_kernel, nrow, ncol, width),
        out_shape=(
            shape(pairs, pair_width), shape(lw, samples), shape(rw, samples),
            shape(2, ncol, chips, share, pair_width), shape(1, pair_width),
        ),
        in_specs=[HBM] * 5,
        out_specs=[VMEM] * 5,
        scratch_shapes=scratch,
        compiler_params=pltpu.CompilerParams(
            collective_id=0, has_side_effects=True, vmem_limit_bytes=40 * 2**20
        ),
        name="tile",
    )(
        in_hbm(left_factors.transpose(1, 2, 0).reshape(lw, samples)),
        in_hbm(right_factors.transpose(1, 2, 0).reshape(rw, samples)),
        in_hbm(weight),
        in_hbm(bias.reshape(1, pair_width)),
        in_hbm(cotangent.reshape(pairs, pair_width)),
    )
    pair, lg, rg, wg, bg = pl.pallas_call(
        functools.partial(finish_kernel, width),
        out_shape=(
            shape(pairs, pair_width), shape(lw, samples), shape(rw, samples),
            shape(width, channels // width, pair_width), shape(1, pair_width),
        ),
        in_specs=[VMEM] * 5,
        out_specs=[HBM] * 5,
        scratch_shapes=[dma((5,))],
        compiler_params=pltpu.CompilerParams(vmem_limit_bytes=8 * 2**20),
        name="finish",
    )(pair, lg, rg, wg, bg)
    return (
        pair.reshape(tile_rows, tile_cols, pair_width),
        lg.reshape(li, width, samples).transpose(2, 0, 1),
        rg.reshape(rj, width, samples).transpose(2, 0, 1),
        wg.reshape(channels, pair_width),
        bg.reshape(pair_width),
    )


def solution(mesh):
    nrow, ncol = mesh.shape["row"], mesh.shape["col"]
    in_specs = (
        P(None, ("row", "col"), None),
        P(None, ("col", "row"), None),
        P(),
        P(),
        P("row", "col", None),
    )
    out_specs = (
        P("row", "col", None),
        P(None, ("row", "col"), None),
        P(None, ("col", "row"), None),
        P(),
        P(),
    )
    return jax.shard_map(
        functools.partial(per_device, nrow, ncol),
        mesh=mesh, in_specs=in_specs, out_specs=out_specs, check_vma=False,
    )
```

```python
import functools

import jax
import jax.numpy as jnp
from jax import lax
from jax.experimental import pallas as pl
from jax.experimental.pallas import tpu as pltpu
from jax.sharding import PartitionSpec as P

F32 = jnp.float32
BF16 = jnp.bfloat16
MESH = pl.DeviceIdType.MESH
VMEM = pl.BlockSpec(memory_space=pltpu.VMEM)
HBM = pl.BlockSpec(memory_space=pltpu.HBM)
STEP = 8
SINGLE = (
    "left", "leftfar", "relay", "right", "pass", "mate", "passed", "terms", "term", "via", "swap", "swapped",
    "rterms", "rterm", "bmate", "bmated", "bchip", "bchiped", "bcol", "bcoled", "core", "chip", "col", "coled",
    "allcol", "allchip", "allcore", "done",
)


def in_hbm(x):
    return pltpu.with_memory_space_constraint(x, pltpu.HBM)


def split(x):
    high = x.astype(BF16)
    return high, (x - high.astype(F32)).astype(BF16)


def dot(a, b):
    return lax.dot_general(a, b, (((1,), (0,)), ((), ())), preferred_element_type=F32)


def dot_wide(a_high, a_low, b_both):
    half = b_both.shape[1] // 2
    wide = dot(a_high, b_both)
    return wide[:, 0:half] + (wide[:, half:] + dot(a_low, b_both[:, 0:half]))


def dot_tall(a_both, b_high, b_low):
    half = a_both.shape[0] // 2
    tall = dot(a_both, b_high)
    return tall[0:half] + (tall[half:] + dot(a_both[0:half], b_low))


def total(parts):
    return functools.reduce(lambda a, b: a + b, parts)


def swap_groups(pieces):
    lane = lax.broadcasted_iota(jnp.int32, pieces[0].shape, 1)
    low = lane < 64
    even = (lane & 32) == 0

    def far(a, b):
        moved = pltpu.roll(jnp.where(low, b, a), 64, 1)
        return jnp.where(low, a, moved), jnp.where(low, moved, b)

    def near(a, b):
        return (
            jnp.where(even, a, pltpu.roll(b, 32, 1)),
            jnp.where(even, pltpu.roll(a, 96, 1), b),
        )

    p0, p2 = far(pieces[0], pieces[2])
    p1, p3 = far(pieces[1], pieces[3])
    p0, p1 = near(p0, p1)
    p2, p3 = near(p2, p3)
    return p0, p1, p2, p3


def tile_kernel(
    nrow, ncol, width, l_ref, r_ref, w_ref, b_ref, cot_ref,
    pair_ref, lg_ref, rg_ref, wg_ref, bg_ref,
    lo, ro, lp, lbuf, vbuf, rpa, rp, mbuf, rsum, rbuf,
    wp, cbuf, xs, xbuf, zs, zbuf, bown, bmate, bsrc, brow, bmid, bcol,
    w_v, b_v, cot_v, tmp, scr_a, scr_b, acc,
    c2, ct2, w_c, wt2, wt_l, h_h, h_l, rt_c, r2, t_h, t_l, l_c, l_l, lt_c,
    loc, one, glr, grr, kr, xsr, azr, axr,
):
    row, col = lax.axis_index("row"), lax.axis_index("col")
    chip, core = row // 2, lax.rem(row, 2)
    mate = row + 1 - 2 * core
    chips = nrow // 2
    lw, samples = l_ref.shape
    rw = r_ref.shape[0]
    tile_rows, tile_cols = ncol * lw // width, nrow * rw // width
    channels, pair_width = w_ref.shape
    rights = tile_cols * width
    scale = 1.0 / samples
    per = 128 // width
    share = channels // (nrow * ncol)
    lanes_step = STEP * width
    gcols = max(1, lanes_step // lw)
    groups = ncol // gcols
    glanes = gcols * lw
    grows = glanes // width * tile_cols
    own_group = col // gcols
    piece = lw // 2
    lower, upper = col, ncol - 1 - col
    both = jnp.minimum(lower, upper)
    longer = jnp.where(lower > upper, -1, 1)
    halfway = ncol // 2
    low_half = col < halfway
    inner = jnp.logical_and(col > 0, col < ncol - 1)

    def along(k):
        paired = k <= 2 * both
        distance = jnp.where(paired, (k + 1) // 2, k - both)
        side = jnp.where(jnp.logical_and(paired, lax.rem(k, 2) == 0), -longer, longer)
        return col + side * distance

    def order(k):
        far = jnp.where(low_half, ncol - 1 - k, k)
        base = jnp.where(low_half, 0, halfway)
        near = base + lax.rem(col - base + 1 + lax.rem(k, halfway), halfway)
        return jnp.where(k < halfway, far, near)

    def group_at(k):
        return along(k) if gcols == 1 else lax.rem(own_group + k, groups)

    crossed = gcols == 1 and groups >= 4
    span = glanes // 2
    deep = grows // 2

    def units(k):
        if crossed and k >= groups - 2:
            return [2 * group_at(n) + k - (groups - 2) for n in (groups - 2, groups - 1)]
        return [2 * group_at(k) + n for n in range(2)]

    def lanes_of(ref, k):
        return jnp.concatenate([ref[:, pl.ds(pl.multiple_of(n * span, span), span)] for n in units(k)], axis=1)

    def rows_of(ref, k):
        return jnp.concatenate([ref[pl.ds(pl.multiple_of(n * span, span), span), :] for n in units(k)], axis=0)

    def via_end(source, target):
        return jnp.logical_or(
            jnp.logical_and(source == 0, target >= 3),
            jnp.logical_and(source == ncol - 1, target <= ncol - 4),
        )

    def via_here(target):
        return jnp.logical_or(
            jnp.logical_and(col == 1, target >= 3),
            jnp.logical_and(col == ncol - 2, target <= ncol - 4),
        )

    def in_row(peer):
        return {"row": peer, "col": col}

    def in_col(peer):
        return {"row": row, "col": peer}

    def block(ref, index, size):
        return ref.at[pl.ds(pl.multiple_of(index * size, size), size)]

    def each(count, here, act):
        @pl.loop(1, count)
        def _(k):
            act(lax.rem(here + k, count))

    wide = chips // 2
    steps_out = sorted(
        ((a, b) for a in range(wide) for b in range(2) if a + b), key=lambda s: -(min(s[0], wide - s[0]) + s[1])
    )

    def each_chip(act):
        for a, b in steps_out:
            act(lax.rem(chip // 2 + a, wide) * 2 + lax.rem(chip + b, 2))

    def send(src, dst, send_sem, recv_sem, device):
        return pltpu.make_async_remote_copy(
            src_ref=src, dst_ref=dst, send_sem=send_sem, recv_sem=recv_sem,
            device_id=device, device_id_type=MESH,
        )

    def part(ref, index, s):
        return ref.at[pl.ds(pl.multiple_of(index * lw + s * piece, piece), piece)]

    def sem(name):
        return one.at[SINGLE.index(name)]

    def here(act):
        pl.when(row >= 0)(act)

    def settle(ref, semaphore):
        send(ref, ref, semaphore, semaphore, in_row(mate)).wait_recv()

    def left_own(s, side):
        return send(
            part(lo, col, s), part(lo, col, s), sem("left"), glr.at[col, s], in_col(col + side)
        )

    def left_far(peer, s):
        return send(part(lo, col, s), part(lo, col, s), sem("leftfar"), glr.at[col, s], in_col(peer))

    def far_off(peer):
        return jnp.abs(peer - col) >= 3

    def left_on(q, s):
        return send(
            part(lo, q, s), part(lo, q, s), sem("relay"), glr.at[q, s], in_col(col + jnp.where(q < col, 1, -1))
        )

    def right_own(peer, recv):
        return send(block(ro, row, rw), block(ro, row, rw), sem("right"), recv, in_row(peer))

    def right_pass(slot):
        return send(block(ro, slot, rw), block(ro, slot, rw), sem("pass"), sem("passed"), in_row(mate))

    def left_term(peer):
        return send(block(lp, peer, lw), lbuf.at[col], sem("terms"), sem("term"), in_col(peer))

    def left_via(peer):
        return send(
            block(lp, peer, lw), vbuf.at[peer], sem("terms"), sem("via"), in_col(jnp.where(col == 0, 1, ncol - 2))
        )

    def right_swap(m):
        return send(block(rp, 2 * m + 1 - core, rw), mbuf.at[m], sem("swap"), sem("swapped"), in_row(mate))

    def right_term(m):
        return send(rsum.at[m], rbuf.at[chip], sem("rterms"), sem("rterm"), in_row(2 * m + core))

    def bias_mate():
        return send(bown, bmate, sem("bmate"), sem("bmated"), in_row(mate))

    def bias_chip(m):
        return send(bsrc, brow.at[chip], sem("bchip"), sem("bchiped"), in_row(2 * m + core))

    def bias_col(peer):
        return send(bmid, bcol.at[col], sem("bcol"), sem("bcoled"), in_col(peer))

    def core_term(q):
        return send(wp.at[1 - core, q], cbuf.at[q], sem("core"), kr.at[q], in_row(mate))

    def chip_term(q, m):
        return send(xs.at[q, m], xbuf.at[q, chip], sem("chip"), xsr.at[q], in_row(2 * m + core))

    def col_term(peer):
        return send(zs.at[peer], zbuf.at[col], sem("col"), sem("coled"), in_col(peer))

    def col_whole(peer):
        piece = wg_ref.at[core, col, chip]
        return send(piece, piece, sem("allcol"), azr.at[col], in_col(peer))

    def chip_whole(q, m):
        piece = wg_ref.at[core, q, chip]
        return send(piece, piece, sem("allchip"), axr.at[q], in_row(2 * m + core))

    def core_whole(q):
        piece = wg_ref.at[core, q]
        return send(piece, piece, sem("allcore"), sem("done"), in_row(mate))

    others = pl.ds(0, chips - 1)
    own_left = pl.ds(pl.multiple_of(col * lw, lw), lw)
    own_right = pl.ds(pl.multiple_of(row * rw, rw), rw)
    loads = [
        pltpu.make_async_copy(src, dst, loc.at[k])
        for k, (src, dst) in enumerate([
            (l_ref, lo.at[own_left]), (r_ref, ro.at[own_right]), (w_ref, w_v), (cot_ref, cot_v), (b_ref, b_v),
        ])
    ]
    barrier = pltpu.get_barrier_semaphore()
    for load in loads:
        load.start()
    def hello(device):
        pl.semaphore_signal(barrier, inc=1, device_id=device, device_id_type=MESH)

    for k in range(1, ncol):
        hello(in_col(lax.rem(col + k, ncol)))
    each_chip(lambda m: hello(in_row(2 * m + core)))
    hello(in_row(mate))
    pl.semaphore_wait(barrier, ncol + chips - 1)
    loads[0].wait()
    loads[1].wait()

    for s in range(2):
        @pl.when(col < ncol - 1)
        def _():
            left_own(s, 1).start()

        @pl.when(col > 0)
        def _():
            left_own(s, -1).start()

    for peer in range(ncol):
        @pl.when(far_off(peer))
        def _():
            for s in range(2):
                left_far(peer, s).start()

    @here
    def _():
        each_chip(lambda m: right_own(2 * m + core, grr.at[chip]).start())
        right_own(mate, sem("mate")).start()


    loads[2].wait()
    loads[3].wait()
    for d in range(width):
        tmp[d * width : (d + 1) * width, :] = w_v[pl.ds(d, width, stride=width), :]
    weight = tmp[0:channels, :]
    w_c[:, 0:pair_width], w_c[:, pair_width:] = split(weight)
    high, wt_l[...] = split(weight.T * scale)
    wt2[0:pair_width, :] = high
    wt2[pair_width:, :] = high
    cot = cot_v[...]
    c2[:, 0:pair_width], c2[:, pair_width:] = split(cot)
    ct2[0:pair_width, :], ct2[pair_width:, :] = split(cot.T)
    bown[...] = jnp.broadcast_to(jnp.sum(cot, axis=0, keepdims=True), (8, pair_width))
    bias_mate().start()

    scrs = [scr_a, scr_b]
    steps = channels // lanes_step

    def grad_block(b):
        lanes = slice(b * lanes_step, (b + 1) * lanes_step)
        scrs[b % 2][...] = dot(c2[...], wt2[:, lanes]) + dot(c2[:, 0:pair_width], wt_l[:, lanes])

    def grad_swap(b):
        scr = scrs[b % 2]
        for u in range(STEP // per):
            for v in range(tile_rows // per):
                pieces = [
                    scr[(v * per + a) * tile_cols : (v * per + a + 1) * tile_cols, u * 128 : (u + 1) * 128]
                    for a in range(per)
                ]
                for a, piece in enumerate(swap_groups(pieces)):
                    at = (b * STEP + u * per + a) * tile_cols
                    high, low = split(piece)
                    h_h[at : at + tile_cols, v * 128 : (v + 1) * 128] = high
                    h_l[at : at + tile_cols, v * 128 : (v + 1) * 128] = low

    def relay(k, s):
        @pl.when(inner)
        def _():
            q = along(k)
            left_on(q, s).wait_recv()
            left_on(q, s).start()

    def arrive(k, pieces=(0, 1)):
        @pl.when(jnp.logical_or(k > 2, jnp.logical_not(inner)))
        def _():
            q = along(k)
            for s in pieces:
                left_on(q, s).wait_recv()

    def ready(k):
        if crossed and k >= groups - 2:
            for n in (groups - 2, groups - 1):
                arrive(n, (k - (groups - 2),))
        elif gcols == 1 and k > 0:
            arrive(k)

    near = range(1, min(ncol, 3))
    grad_block(0)
    for b in range(steps):
        if b + 1 < steps:
            grad_block(b + 1)
        grad_swap(b)
    for k in near:
        relay(k, 0)

    def right_grad(k):
        lt_c[:, 0:samples], lt_c[:, samples:] = split(rows_of(lo, k))
        term = dot_wide(lanes_of(h_h, k), lanes_of(h_l, k), lt_c[...])
        if k == 0:
            rpa[...] = term
        else:
            rpa[...] += term

    early = 1 if gcols == 1 and groups > 1 else 0
    if early:
        right_grad(0)
    for k in near:
        relay(k, 1)
    settle(bmate, sem("bmated"))
    bsrc[...] = bown[...] + bmate[...]
    brow[chip] = bsrc[...]
    each_chip(lambda m: bias_chip(m).start())

    def hand_over(m):
        settle(block(ro, 0, rw), grr.at[m])

        @here
        def _():
            right_pass(2 * m + core).start()

    for a, b in reversed(steps_out):
        hand_over(lax.rem(chip // 2 + a, wide) * 2 + lax.rem(chip + b, 2))
    settle(block(ro, 0, rw), sem("mate"))
    settle(block(ro, 0, (chips - 1) * rw), sem("passed"))
    for d in range(width):
        tmp[d * tile_cols : (d + 1) * tile_cols, :] = ro[pl.ds(d, tile_cols, stride=width), :]
    right = tmp[0:rights, :]
    rt_c[:, 0:samples], rt_c[:, samples:] = split(right)
    r2[0:samples, :], r2[samples:, :] = split(right.T)


    def left_grad(k):
        g = group_at(groups - 1 - k)
        lanes = pl.ds(pl.multiple_of(g * glanes, glanes), glanes)
        lp[lanes, :] = dot_tall(r2[...], h_h[:, lanes], h_l[:, lanes]).T

    def send_term(k):
        peer = along(ncol - 1 - k)

        @pl.when(via_end(col, peer))
        def _():
            left_via(peer).start()

        @pl.when(jnp.logical_not(jnp.logical_or(via_end(col, peer), via_here(peer))))
        def _():
            left_term(peer).start()

        @pl.when(via_end(peer, col))
        def _():
            lbuf[peer] = jnp.zeros(lbuf.shape[1:], F32)

    if gcols > 1:
        @pl.loop(1, ncol)
        def _(k):
            arrive(k)

    middle = channels // 2

    def outer(k, halves, beside, then):
        high, l_l[...] = split(rows_of(lo, k).T * scale)
        l_c[0:samples, :] = high
        l_c[samples:, :] = high
        half = rights // 2
        units = width // per // 2
        for scr, h in zip(scrs, halves):
            at = pl.ds(pl.multiple_of(h * half, half), half)
            scr[0:half, 0:glanes] = dot(rt_c[at, :], l_c[...]) + dot(rt_c[at, 0:samples], l_l[...])
        beside()
        for scr, h in zip(scrs, halves):
            for u in range(units):
                for v in range(glanes // 128):
                    pieces = [
                        scr[(u * per + a) * tile_cols : (u * per + a + 1) * tile_cols, v * 128 : (v + 1) * 128]
                        for a in range(per)
                    ]
                    lanes = pl.ds(pl.multiple_of(h * middle + u * 128, 128), 128)
                    for a, piece in enumerate(swap_groups(pieces)):
                        at = k * grows + (v * per + a) * tile_cols
                        high, low = split(piece)
                        t_h[at : at + tile_cols, lanes] = high
                        t_l[at : at + tile_cols, lanes] = low
            then(h)

    def weight_grad(k, lanes):
        at = slice(k * grows, (k + 1) * grows)
        both = jnp.concatenate([ct2[:, pl.ds(pl.multiple_of(n * deep, deep), deep)] for n in units(k)], axis=1)
        term = dot_tall(both, t_h[at, lanes], t_l[at, lanes])
        if k == 0:
            acc[:, lanes] = term
        else:
            acc[:, lanes] += term

    def beside(k):
        if k < groups - 1 or gcols > 1:
            left_grad(k)
        if k > 0:
            weight_grad(k - 1, slice(0, channels))

    for k in range(groups - 1):
        ready(k)
        outer(k, (0, 1), functools.partial(beside, k), lambda h: None)
        if gcols == 1:
            @pl.when(jnp.logical_not(inner))
            def _():
                send_term(k)

    if gcols == 1:
        @pl.when(inner)
        def _():
            for k in range(groups - 1):
                send_term(k)

    ready(groups - 1)
    turned = jnp.where(low_half, 1, 0)

    def last_half(h):
        start = pl.multiple_of(h * middle, middle)
        weight_grad(groups - 1, pl.ds(start, middle))
        for i in range(middle // 128):
            terms = acc[:, pl.ds(pl.multiple_of(start + i * 128, 128), 128)].T
            for n in range(128 // share):
                b, q = divmod((i * 128) // share + n, halfway * chips)
                q, m = divmod(q, chips)
                wp[b, h * halfway + q, m] = terms[n * share : (n + 1) * share, :]

        @here
        def _():
            for q in range(halfway):
                core_term(h * halfway + q).start()

    outer(groups - 1, (turned, 1 - turned), functools.partial(beside, groups - 1), last_half)

    def chip_terms(first):
        for k in range(first, first + halfway):
            q = order(k)
            core_term(q).wait_recv()
            xs[q] = wp[core, q] + cbuf[q]
            xbuf[q, chip] = xs[q, chip]

            @here
            def _():
                each_chip(lambda m: chip_term(q, m).start())

    if gcols > 1:
        for k in range(ncol - 1):
            send_term(k)
    chip_terms(0)
    for k in range(early, groups - 1):
        right_grad(k)
    chip_terms(halfway)
    loads[4].wait()
    if gcols == 1:
        left_grad(groups - 1)
    lbuf[col] = lp[own_left, :]
    right_grad(groups - 1)
    settle(brow.at[others], sem("bchiped"))
    bmid[...] = total([brow[m] for m in range(chips)])
    bcol[col] = bmid[...]
    each(ncol, col, lambda p: bias_col(p).start())

    for d in range(width):
        rp[pl.ds(d, tile_cols, stride=width), :] = rpa[d * tile_cols : (d + 1) * tile_cols, :]

    @here
    def _():
        for m in range(chips):
            right_swap(m).start()

    pair = dot_wide(t_h[...], t_l[...], w_c[...]) + b_v[...]
    for k in range(groups):
        for n, unit in enumerate(units(k)):
            at = k * grows + n * deep
            pair_ref[pl.ds(pl.multiple_of(unit * deep, deep), deep), :] = pair[at : at + deep, :]
    settle(mbuf, sem("swapped"))
    for m in range(chips):
        rsum[m] = rp[pl.ds(pl.multiple_of((2 * m + core) * rw, rw), rw), :] + mbuf[m]

    @here
    def _():
        each_chip(lambda m: right_term(m).start())

    rbuf[chip] = rsum[chip]
    for k in range(ncol - 1):
        q = order(k)
        settle(xbuf.at[q, others], xsr.at[q])
        zs[q] = total([xbuf[q, m] for m in range(chips)])

        @here
        def _():
            col_term(q).start()

    settle(xbuf.at[col, others], xsr.at[col])
    zbuf[col] = total([xbuf[col, m] for m in range(chips)])
    settle(zbuf.at[pl.ds(0, ncol - 1)], sem("coled"))
    wg_ref[core, col, chip] = total([zbuf[q] for q in range(ncol)]) / (tile_rows * nrow)

    @pl.loop(1, ncol)
    def _(k):
        col_whole(along(ncol - k)).start()

    @here
    def _():
        each_chip(lambda m: chip_whole(col, m).start())

    if ncol > 3:
        @pl.when(jnp.logical_or(col == 1, col == ncol - 2))
        def _():
            settle(vbuf.at[pl.ds(0, ncol - 3)], sem("via"))

    for p in range(ncol):
        @pl.when(via_here(p))
        def _():
            lp[p * lw : (p + 1) * lw, :] += vbuf[p]
            left_term(p).start()

    ends = jnp.logical_not(inner)

    @pl.when(inner)
    def _():
        settle(lo.at[pl.ds(0, 2 * lw)], sem("left"))
        settle(lo.at[pl.ds(0, 2 * lw)], sem("relay"))

    @pl.when(ends)
    def _():
        settle(lo.at[pl.ds(0, lw)], sem("left"))

    for peer in range(ncol):
        @pl.when(far_off(peer))
        def _():
            settle(lo.at[pl.ds(0, lw)], sem("leftfar"))

    settle(ro.at[pl.ds(0, chips * rw)], sem("right"))
    settle(ro.at[pl.ds(0, (chips - 1) * rw)], sem("pass"))
    settle(bown, sem("bmate"))
    settle(brow.at[others], sem("bchip"))
    settle(bcol.at[pl.ds(0, ncol - 1)], sem("bcol"))
    settle(wp.at[0], sem("core"))
    settle(xs.at[:, others], sem("chip"))
    settle(mbuf, sem("swap"))

    @pl.loop(1, ncol)
    def _(k):
        q = along(k)
        piece_in = wg_ref.at[core, q, chip]
        settle(piece_in, azr.at[q])
        each_chip(lambda m: chip_whole(q, m).start())

    @pl.loop(0, ncol)
    def _(k):
        q = along(k)
        settle(wg_ref.at[core, q, others], axr.at[q])
        core_whole(q).start()

    settle(bcol.at[pl.ds(0, ncol - 1)], sem("bcoled"))
    bg_ref[...] = total([bcol[q] for q in range(ncol)])[0:1, :] / (tile_rows * nrow)
    near_ends = [jnp.logical_and(ncol > 3, col >= 3), jnp.logical_and(ncol > 3, col <= ncol - 4)]
    absent = near_ends[0].astype(jnp.int32) + near_ends[1].astype(jnp.int32)
    for n in range(3):
        if ncol - 1 - n > 0:
            @pl.when(absent == n)
            def _():
                settle(lbuf.at[pl.ds(0, ncol - 1 - n)], sem("term"))

    lg_ref[...] = total([lbuf[q] for q in range(ncol)])
    settle(rbuf.at[others], sem("rterm"))
    rg_ref[...] = total([rbuf[m] for m in range(chips)])
    settle(lbuf.at[pl.ds(0, ncol - 1)], sem("terms"))
    settle(rbuf.at[others], sem("rterms"))
    settle(zs.at[pl.ds(0, ncol - 1)], sem("col"))
    settle(zs.at[pl.ds(0, ncol - 1)], sem("allcol"))
    settle(xs.at[:, others], sem("allchip"))
    settle(wg_ref.at[1 - core], sem("done"))
    settle(wg_ref.at[core], sem("allcore"))


def finish_kernel(
    width, pair_ref, lg_ref, rg_ref, wg_ref, bg_ref,
    pair_out, lg_out, rg_out, w_out, bg_out, sems,
):
    halves, ncol, chips, share, _ = wg_ref.shape
    copies = [
        pltpu.make_async_copy(src, dst, sems.at[k])
        for k, (src, dst) in enumerate([
            (pair_ref, pair_out), (lg_ref, lg_out), (rg_ref, rg_out), (bg_ref, bg_out),
        ])
    ]
    for s in range(halves * ncol * chips):
        d, c = divmod(s * share, width)
        q, m = divmod(s, chips)
        h, q = divmod(q, ncol)
        b, q = divmod(q, ncol // 2)
        q += h * (ncol // 2)
        pltpu.make_async_copy(wg_ref.at[b, q, m], w_out.at[pl.ds(c, share), d], sems.at[4]).start()
    for copy in copies:
        copy.start()
    for copy in copies:
        copy.wait()
    pltpu.make_async_copy(wg_ref, wg_ref, sems.at[4]).wait()


def per_device(nrow, ncol, left_factors, right_factors, weight, bias, cotangent):
    samples, li, width = left_factors.shape
    rj = right_factors.shape[1]
    tile_rows, tile_cols, pair_width = cotangent.shape
    channels = weight.shape[0]
    lw, rw = li * width, rj * width
    lefts, rights = tile_rows * width, tile_cols * width
    pairs = tile_rows * tile_cols
    chips, share = nrow // 2, channels // (nrow * ncol)
    group = max(lw, STEP * width)
    dma = pltpu.SemaphoreType.DMA

    def shape(*dims):
        return jax.ShapeDtypeStruct(dims, F32)

    def half(*dims):
        return pltpu.VMEM(dims, BF16)

    def buf(*dims):
        return pltpu.VMEM(dims, F32)

    scratch = [
        buf(lefts, samples), buf(rights, samples), buf(lefts, samples), *[buf(ncol, lw, samples)] * 2,
        buf(rights, samples), buf(rights, samples), *[buf(chips, rw, samples)] * 3,
        buf(2, ncol, chips, share, pair_width), *[buf(ncol, chips, share, pair_width)] * 3,
        *[buf(ncol, share, pair_width)] * 2,
        *[buf(8, pair_width)] * 3, buf(chips, 8, pair_width), buf(8, pair_width), buf(ncol, 8, pair_width),
        buf(channels, pair_width), buf(1, pair_width), buf(pairs, pair_width),
        buf(max(rights, channels), 128),
        *[buf(max(pairs, rights), max(group, STEP * width))] * 2, buf(pair_width, channels),
        half(pairs, 2 * pair_width), half(2 * pair_width, pairs), half(channels, 2 * pair_width),
        half(2 * pair_width, channels), half(pair_width, channels),
        half(rights, lefts), half(rights, lefts), half(rights, 2 * samples), half(2 * samples, rights),
        half(pairs, channels), half(pairs, channels),
        half(2 * samples, group), half(samples, group), half(group, 2 * samples),
        dma((5,)), dma((len(SINGLE),)), dma((ncol, 2)), dma((chips,)),
        dma((ncol,)), dma((ncol,)), dma((ncol,)), dma((ncol,)),
    ]
    pair, lg, rg, wg, bg = pl.pallas_call(
        functools.partial(tile_kernel, nrow, ncol, width),
        out_shape=(
            shape(pairs, pair_width), shape(lw, samples), shape(rw, samples),
            shape(2, ncol, chips, share, pair_width), shape(1, pair_width),
        ),
        in_specs=[HBM] * 5,
        out_specs=[VMEM] * 5,
        scratch_shapes=scratch,
        compiler_params=pltpu.CompilerParams(
            collective_id=0, has_side_effects=True, vmem_limit_bytes=40 * 2**20
        ),
        name="tile",
    )(
        in_hbm(left_factors.transpose(1, 2, 0).reshape(lw, samples)),
        in_hbm(right_factors.transpose(1, 2, 0).reshape(rw, samples)),
        in_hbm(weight),
        in_hbm(bias.reshape(1, pair_width)),
        in_hbm(cotangent.reshape(pairs, pair_width)),
    )
    pair, lg, rg, wg, bg = pl.pallas_call(
        functools.partial(finish_kernel, width),
        out_shape=(
            shape(pairs, pair_width), shape(lw, samples), shape(rw, samples),
            shape(width, channels // width, pair_width), shape(1, pair_width),
        ),
        in_specs=[VMEM] * 5,
        out_specs=[HBM] * 5,
        scratch_shapes=[dma((5,))],
        compiler_params=pltpu.CompilerParams(vmem_limit_bytes=8 * 2**20),
        name="finish",
    )(pair, lg, rg, wg, bg)
    return (
        pair.reshape(tile_rows, tile_cols, pair_width),
        lg.reshape(li, width, samples).transpose(2, 0, 1),
        rg.reshape(rj, width, samples).transpose(2, 0, 1),
        wg.reshape(channels, pair_width),
        bg.reshape(pair_width),
    )


def solution(mesh):
    nrow, ncol = mesh.shape["row"], mesh.shape["col"]
    in_specs = (
        P(None, ("row", "col"), None),
        P(None, ("col", "row"), None),
        P(),
        P(),
        P("row", "col", None),
    )
    out_specs = (
        P("row", "col", None),
        P(None, ("row", "col"), None),
        P(None, ("col", "row"), None),
        P(),
        P(),
    )
    return jax.shard_map(
        functools.partial(per_device, nrow, ncol),
        mesh=mesh, in_specs=in_specs, out_specs=out_specs, check_vma=False,
    )
```

```python
import functools

import jax
import jax.numpy as jnp
from jax import lax
from jax.experimental import pallas as pl
from jax.experimental.pallas import tpu as pltpu
from jax.sharding import PartitionSpec as P

F32 = jnp.float32
BF16 = jnp.bfloat16
MESH = pl.DeviceIdType.MESH
VMEM = pl.BlockSpec(memory_space=pltpu.VMEM)
HBM = pl.BlockSpec(memory_space=pltpu.HBM)
STEP = 8
SINGLE = (
    "left", "leftfar", "relay", "right", "pass", "mate", "passed", "terms", "term", "via", "swap", "swapped",
    "rterms", "rterm", "bmate", "bmated", "bchip", "bchiped", "bcol", "bcoled", "core", "chip", "col", "coled",
    "allcol", "allchip", "allcore", "alldirect", "done",
)


def in_hbm(x):
    return pltpu.with_memory_space_constraint(x, pltpu.HBM)


def split(x):
    high = x.astype(BF16)
    return high, (x - high.astype(F32)).astype(BF16)


def dot(a, b):
    return lax.dot_general(a, b, (((1,), (0,)), ((), ())), preferred_element_type=F32)


def dot_wide(a_high, a_low, b_both):
    half = b_both.shape[1] // 2
    wide = dot(a_high, b_both)
    return wide[:, 0:half] + (wide[:, half:] + dot(a_low, b_both[:, 0:half]))


def dot_tall(a_both, b_high, b_low):
    half = a_both.shape[0] // 2
    tall = dot(a_both, b_high)
    return tall[0:half] + (tall[half:] + dot(a_both[0:half], b_low))


def total(parts):
    return functools.reduce(lambda a, b: a + b, parts)


def swap_groups(pieces):
    lane = lax.broadcasted_iota(jnp.int32, pieces[0].shape, 1)
    low = lane < 64
    even = (lane & 32) == 0

    def far(a, b):
        moved = pltpu.roll(jnp.where(low, b, a), 64, 1)
        return jnp.where(low, a, moved), jnp.where(low, moved, b)

    def near(a, b):
        return (
            jnp.where(even, a, pltpu.roll(b, 32, 1)),
            jnp.where(even, pltpu.roll(a, 96, 1), b),
        )

    p0, p2 = far(pieces[0], pieces[2])
    p1, p3 = far(pieces[1], pieces[3])
    p0, p1 = near(p0, p1)
    p2, p3 = near(p2, p3)
    return p0, p1, p2, p3


def tile_kernel(
    nrow, ncol, width, l_ref, r_ref, w_ref, b_ref, cot_ref,
    pair_ref, lg_ref, rg_ref, wg_ref, bg_ref,
    lo, ro, lp, lbuf, vbuf, rpa, rp, mbuf, rsum, rbuf,
    wp, cbuf, xs, xbuf, zs, zbuf, bown, bmate, bsrc, brow, bmid, bcol,
    w_v, b_v, cot_v, tmp, scr_a, scr_b, acc,
    c2, ct2, w_c, wt2, wt_l, h_h, h_l, rt_c, r2, t_h, t_l, l_c, l_l, lt_c,
    loc, one, glr, grr, kr, xsr, azr, axr,
):
    row, col = lax.axis_index("row"), lax.axis_index("col")
    chip, core = row // 2, lax.rem(row, 2)
    mate = row + 1 - 2 * core
    chips = nrow // 2
    lw, samples = l_ref.shape
    rw = r_ref.shape[0]
    tile_rows, tile_cols = ncol * lw // width, nrow * rw // width
    channels, pair_width = w_ref.shape
    rights = tile_cols * width
    scale = 1.0 / samples
    per = 128 // width
    share = channels // (nrow * ncol)
    lanes_step = STEP * width
    gcols = max(1, lanes_step // lw)
    groups = ncol // gcols
    glanes = gcols * lw
    grows = glanes // width * tile_cols
    own_group = col // gcols
    piece = lw // 2
    lower, upper = col, ncol - 1 - col
    both = jnp.minimum(lower, upper)
    longer = jnp.where(lower > upper, -1, 1)
    halfway = ncol // 2
    low_half = col < halfway
    inner = jnp.logical_and(col > 0, col < ncol - 1)

    def along(k):
        paired = k <= 2 * both
        distance = jnp.where(paired, (k + 1) // 2, k - both)
        side = jnp.where(jnp.logical_and(paired, lax.rem(k, 2) == 0), -longer, longer)
        return col + side * distance

    def order(k):
        far = jnp.where(low_half, ncol - 1 - k, k)
        base = jnp.where(low_half, 0, halfway)
        near = base + lax.rem(col - base + 1 + lax.rem(k, halfway), halfway)
        return jnp.where(k < halfway, far, near)

    def group_at(k):
        return along(k) if gcols == 1 else lax.rem(own_group + k, groups)

    crossed = gcols == 1 and groups >= 4
    span = glanes // 2
    deep = grows // 2

    def units(k):
        if crossed and k >= groups - 2:
            return [2 * group_at(n) + k - (groups - 2) for n in (groups - 2, groups - 1)]
        return [2 * group_at(k) + n for n in range(2)]

    def lanes_of(ref, k):
        return jnp.concatenate([ref[:, pl.ds(pl.multiple_of(n * span, span), span)] for n in units(k)], axis=1)

    def rows_of(ref, k):
        return jnp.concatenate([ref[pl.ds(pl.multiple_of(n * span, span), span), :] for n in units(k)], axis=0)

    def via_end(source, target):
        return jnp.logical_or(
            jnp.logical_and(source == 0, target >= 3),
            jnp.logical_and(source == ncol - 1, target <= ncol - 4),
        )

    def via_here(target):
        return jnp.logical_or(
            jnp.logical_and(col == 1, target >= 3),
            jnp.logical_and(col == ncol - 2, target <= ncol - 4),
        )

    def in_row(peer):
        return {"row": peer, "col": col}

    def in_col(peer):
        return {"row": row, "col": peer}

    def block(ref, index, size):
        return ref.at[pl.ds(pl.multiple_of(index * size, size), size)]

    def each(count, here, act):
        @pl.loop(1, count)
        def _(k):
            act(lax.rem(here + k, count))

    wide = chips // 2
    steps_out = sorted(
        ((a, b) for a in range(wide) for b in range(2) if a + b), key=lambda s: -(min(s[0], wide - s[0]) + s[1])
    )

    def each_chip(act):
        for a, b in steps_out:
            act(lax.rem(chip // 2 + a, wide) * 2 + lax.rem(chip + b, 2))

    def send(src, dst, send_sem, recv_sem, device):
        return pltpu.make_async_remote_copy(
            src_ref=src, dst_ref=dst, send_sem=send_sem, recv_sem=recv_sem,
            device_id=device, device_id_type=MESH,
        )

    def part(ref, index, s):
        return ref.at[pl.ds(pl.multiple_of(index * lw + s * piece, piece), piece)]

    def sem(name):
        return one.at[SINGLE.index(name)]

    def here(act):
        pl.when(row >= 0)(act)

    def settle(ref, semaphore):
        send(ref, ref, semaphore, semaphore, in_row(mate)).wait_recv()

    def left_own(s, side):
        return send(
            part(lo, col, s), part(lo, col, s), sem("left"), glr.at[col, s], in_col(col + side)
        )

    def left_far(peer, s):
        return send(part(lo, col, s), part(lo, col, s), sem("leftfar"), glr.at[col, s], in_col(peer))

    def far_off(peer):
        return jnp.abs(peer - col) >= 3

    def left_on(q, s):
        return send(
            part(lo, q, s), part(lo, q, s), sem("relay"), glr.at[q, s], in_col(col + jnp.where(q < col, 1, -1))
        )

    def right_own(peer, recv):
        return send(block(ro, row, rw), block(ro, row, rw), sem("right"), recv, in_row(peer))

    def right_pass(slot):
        return send(block(ro, slot, rw), block(ro, slot, rw), sem("pass"), sem("passed"), in_row(mate))

    def left_term(peer):
        return send(block(lp, peer, lw), lbuf.at[col], sem("terms"), sem("term"), in_col(peer))

    def left_via(peer):
        return send(
            block(lp, peer, lw), vbuf.at[peer], sem("terms"), sem("via"), in_col(jnp.where(col == 0, 1, ncol - 2))
        )

    def right_swap(m):
        return send(block(rp, 2 * m + 1 - core, rw), mbuf.at[m], sem("swap"), sem("swapped"), in_row(mate))

    def right_term(m):
        return send(rsum.at[m], rbuf.at[chip], sem("rterms"), sem("rterm"), in_row(2 * m + core))

    def bias_mate():
        return send(bown, bmate, sem("bmate"), sem("bmated"), in_row(mate))

    def bias_chip(m):
        return send(bsrc, brow.at[chip], sem("bchip"), sem("bchiped"), in_row(2 * m + core))

    def bias_col(peer):
        return send(bmid, bcol.at[col], sem("bcol"), sem("bcoled"), in_col(peer))

    def core_term(q):
        return send(wp.at[1 - core, q], cbuf.at[q], sem("core"), kr.at[q], in_row(mate))

    def chip_term(q, m):
        return send(xs.at[q, m], xbuf.at[q, chip], sem("chip"), xsr.at[q], in_row(2 * m + core))

    def col_term(peer):
        return send(zs.at[peer], zbuf.at[col], sem("col"), sem("coled"), in_col(peer))

    def col_whole(peer):
        piece = wg_ref.at[core, col, chip]
        return send(piece, piece, sem("allcol"), azr.at[col], in_col(peer))

    def chip_whole(q, m):
        piece = wg_ref.at[core, q, chip]
        return send(piece, piece, sem("allchip"), axr.at[q], in_row(2 * m + core))

    def core_whole(q):
        piece = wg_ref.at[core, q]
        return send(piece, piece, sem("allcore"), sem("done"), in_row(mate))

    def direct_whole(q, to):
        piece = wg_ref.at[core, q, chip]
        return send(piece, piece, sem("alldirect"), sem("done"), in_row(to))

    others = pl.ds(0, chips - 1)
    own_left = pl.ds(pl.multiple_of(col * lw, lw), lw)
    own_right = pl.ds(pl.multiple_of(row * rw, rw), rw)
    loads = [
        pltpu.make_async_copy(src, dst, loc.at[k])
        for k, (src, dst) in enumerate([
            (l_ref, lo.at[own_left]), (r_ref, ro.at[own_right]), (w_ref, w_v), (cot_ref, cot_v), (b_ref, b_v),
        ])
    ]
    barrier = pltpu.get_barrier_semaphore()
    for load in loads:
        load.start()
    def hello(device):
        pl.semaphore_signal(barrier, inc=1, device_id=device, device_id_type=MESH)

    for k in range(1, ncol):
        hello(in_col(lax.rem(col + k, ncol)))
    each_chip(lambda m: hello(in_row(2 * m + core)))
    hello(in_row(mate))
    pl.semaphore_wait(barrier, ncol + chips - 1)
    loads[0].wait()
    loads[1].wait()

    for s in range(2):
        @pl.when(col < ncol - 1)
        def _():
            left_own(s, 1).start()

        @pl.when(col > 0)
        def _():
            left_own(s, -1).start()

    for peer in range(ncol):
        @pl.when(far_off(peer))
        def _():
            for s in range(2):
                left_far(peer, s).start()

    @here
    def _():
        each_chip(lambda m: right_own(2 * m + core, grr.at[chip]).start())
        right_own(mate, sem("mate")).start()


    loads[2].wait()
    loads[3].wait()
    for d in range(width):
        tmp[d * width : (d + 1) * width, :] = w_v[pl.ds(d, width, stride=width), :]
    weight = tmp[0:channels, :]
    w_c[:, 0:pair_width], w_c[:, pair_width:] = split(weight)
    high, wt_l[...] = split(weight.T * scale)
    wt2[0:pair_width, :] = high
    wt2[pair_width:, :] = high
    cot = cot_v[...]
    c2[:, 0:pair_width], c2[:, pair_width:] = split(cot)
    ct2[0:pair_width, :], ct2[pair_width:, :] = split(cot.T)
    bown[...] = jnp.broadcast_to(jnp.sum(cot, axis=0, keepdims=True), (8, pair_width))
    bias_mate().start()

    scrs = [scr_a, scr_b]
    steps = channels // lanes_step

    def grad_block(b):
        lanes = slice(b * lanes_step, (b + 1) * lanes_step)
        scrs[b % 2][...] = dot(c2[...], wt2[:, lanes]) + dot(c2[:, 0:pair_width], wt_l[:, lanes])

    def grad_swap(b):
        scr = scrs[b % 2]
        for u in range(STEP // per):
            for v in range(tile_rows // per):
                pieces = [
                    scr[(v * per + a) * tile_cols : (v * per + a + 1) * tile_cols, u * 128 : (u + 1) * 128]
                    for a in range(per)
                ]
                for a, piece in enumerate(swap_groups(pieces)):
                    at = (b * STEP + u * per + a) * tile_cols
                    high, low = split(piece)
                    h_h[at : at + tile_cols, v * 128 : (v + 1) * 128] = high
                    h_l[at : at + tile_cols, v * 128 : (v + 1) * 128] = low

    def relay(k, s):
        @pl.when(inner)
        def _():
            q = along(k)
            left_on(q, s).wait_recv()
            left_on(q, s).start()

    def arrive(k, pieces=(0, 1)):
        @pl.when(jnp.logical_or(k > 2, jnp.logical_not(inner)))
        def _():
            q = along(k)
            for s in pieces:
                left_on(q, s).wait_recv()

    def ready(k):
        if crossed and k >= groups - 2:
            for n in (groups - 2, groups - 1):
                arrive(n, (k - (groups - 2),))
        elif gcols == 1 and k > 0:
            arrive(k)

    near = range(1, min(ncol, 3))
    grad_block(0)
    for b in range(steps):
        if b + 1 < steps:
            grad_block(b + 1)
        grad_swap(b)
    for k in near:
        relay(k, 0)

    def right_grad(k):
        lt_c[:, 0:samples], lt_c[:, samples:] = split(rows_of(lo, k))
        term = dot_wide(lanes_of(h_h, k), lanes_of(h_l, k), lt_c[...])
        if k == 0:
            rpa[...] = term
        else:
            rpa[...] += term

    early = 1 if gcols == 1 and groups > 1 else 0
    if early:
        right_grad(0)
    for k in near:
        relay(k, 1)
    settle(bmate, sem("bmated"))
    bsrc[...] = bown[...] + bmate[...]
    brow[chip] = bsrc[...]
    each_chip(lambda m: bias_chip(m).start())

    def hand_over(m):
        settle(block(ro, 0, rw), grr.at[m])

        @here
        def _():
            right_pass(2 * m + core).start()

    for a, b in reversed(steps_out):
        hand_over(lax.rem(chip // 2 + a, wide) * 2 + lax.rem(chip + b, 2))
    settle(block(ro, 0, rw), sem("mate"))
    settle(block(ro, 0, (chips - 1) * rw), sem("passed"))
    for d in range(width):
        tmp[d * tile_cols : (d + 1) * tile_cols, :] = ro[pl.ds(d, tile_cols, stride=width), :]
    right = tmp[0:rights, :]
    rt_c[:, 0:samples], rt_c[:, samples:] = split(right)
    r2[0:samples, :], r2[samples:, :] = split(right.T)


    def left_grad(k):
        g = group_at(groups - 1 - k)
        lanes = pl.ds(pl.multiple_of(g * glanes, glanes), glanes)
        lp[lanes, :] = dot_tall(r2[...], h_h[:, lanes], h_l[:, lanes]).T

    def send_term(k):
        peer = along(ncol - 1 - k)

        @pl.when(via_end(col, peer))
        def _():
            left_via(peer).start()

        @pl.when(jnp.logical_not(jnp.logical_or(via_end(col, peer), via_here(peer))))
        def _():
            left_term(peer).start()

        @pl.when(via_end(peer, col))
        def _():
            lbuf[peer] = jnp.zeros(lbuf.shape[1:], F32)

    if gcols > 1:
        @pl.loop(1, ncol)
        def _(k):
            arrive(k)

    middle = channels // 2

    def outer(k, halves, beside, then):
        high, l_l[...] = split(rows_of(lo, k).T * scale)
        l_c[0:samples, :] = high
        l_c[samples:, :] = high
        half = rights // 2
        units = width // per // 2
        for scr, h in zip(scrs, halves):
            at = pl.ds(pl.multiple_of(h * half, half), half)
            scr[0:half, 0:glanes] = dot(rt_c[at, :], l_c[...]) + dot(rt_c[at, 0:samples], l_l[...])
        beside()
        for scr, h in zip(scrs, halves):
            for u in range(units):
                for v in range(glanes // 128):
                    pieces = [
                        scr[(u * per + a) * tile_cols : (u * per + a + 1) * tile_cols, v * 128 : (v + 1) * 128]
                        for a in range(per)
                    ]
                    lanes = pl.ds(pl.multiple_of(h * middle + u * 128, 128), 128)
                    for a, piece in enumerate(swap_groups(pieces)):
                        at = k * grows + (v * per + a) * tile_cols
                        high, low = split(piece)
                        t_h[at : at + tile_cols, lanes] = high
                        t_l[at : at + tile_cols, lanes] = low
            then(h)

    def weight_grad(k, lanes):
        at = slice(k * grows, (k + 1) * grows)
        both = jnp.concatenate([ct2[:, pl.ds(pl.multiple_of(n * deep, deep), deep)] for n in units(k)], axis=1)
        term = dot_tall(both, t_h[at, lanes], t_l[at, lanes])
        if k == 0:
            acc[:, lanes] = term
        else:
            acc[:, lanes] += term

    def beside(k):
        if k < groups - 1 or gcols > 1:
            left_grad(k)
        if k > 0:
            weight_grad(k - 1, slice(0, channels))

    for k in range(groups - 1):
        ready(k)
        outer(k, (0, 1), functools.partial(beside, k), lambda h: None)
        if gcols == 1:
            @pl.when(jnp.logical_not(inner))
            def _():
                send_term(k)

    if gcols == 1:
        @pl.when(inner)
        def _():
            for k in range(groups - 1):
                send_term(k)

    ready(groups - 1)
    turned = jnp.where(low_half, 1, 0)

    def last_half(h):
        start = pl.multiple_of(h * middle, middle)
        weight_grad(groups - 1, pl.ds(start, middle))
        for i in range(middle // 128):
            terms = acc[:, pl.ds(pl.multiple_of(start + i * 128, 128), 128)].T
            for n in range(128 // share):
                b, q = divmod((i * 128) // share + n, halfway * chips)
                q, m = divmod(q, chips)
                wp[b, h * halfway + q, m] = terms[n * share : (n + 1) * share, :]

        @here
        def _():
            for q in range(halfway):
                core_term(h * halfway + q).start()

    outer(groups - 1, (turned, 1 - turned), functools.partial(beside, groups - 1), last_half)

    def chip_terms(first):
        for k in range(first, first + halfway):
            q = order(k)
            core_term(q).wait_recv()
            xs[q] = wp[core, q] + cbuf[q]
            xbuf[q, chip] = xs[q, chip]

            @here
            def _():
                each_chip(lambda m: chip_term(q, m).start())

    if gcols > 1:
        for k in range(ncol - 1):
            send_term(k)
    chip_terms(0)
    chip_terms(halfway)
    for k in range(early, groups - 1):
        right_grad(k)
    loads[4].wait()
    if gcols == 1:
        left_grad(groups - 1)
    lbuf[col] = lp[own_left, :]
    right_grad(groups - 1)
    settle(brow.at[others], sem("bchiped"))
    bmid[...] = total([brow[m] for m in range(chips)])
    bcol[col] = bmid[...]
    each(ncol, col, lambda p: bias_col(p).start())

    for d in range(width):
        rp[pl.ds(d, tile_cols, stride=width), :] = rpa[d * tile_cols : (d + 1) * tile_cols, :]

    @here
    def _():
        for m in range(chips):
            right_swap(m).start()

    for k in range(ncol - 1):
        q = order(k)
        settle(xbuf.at[q, others], xsr.at[q])
        zs[q] = total([xbuf[q, m] for m in range(chips)])

        @here
        def _():
            col_term(q).start()

    settle(mbuf, sem("swapped"))
    for m in range(chips):
        rsum[m] = rp[pl.ds(pl.multiple_of((2 * m + core) * rw, rw), rw), :] + mbuf[m]

    @here
    def _():
        each_chip(lambda m: right_term(m).start())

    rbuf[chip] = rsum[chip]
    settle(xbuf.at[col, others], xsr.at[col])
    zbuf[col] = total([xbuf[col, m] for m in range(chips)])
    pair = dot_wide(t_h[...], t_l[...], w_c[...]) + b_v[...]
    for k in range(groups):
        for n, unit in enumerate(units(k)):
            at = k * grows + n * deep
            pair_ref[pl.ds(pl.multiple_of(unit * deep, deep), deep), :] = pair[at : at + deep, :]
    settle(zbuf.at[pl.ds(0, ncol - 1)], sem("coled"))
    wg_ref[core, col, chip] = total([zbuf[q] for q in range(ncol)]) / (tile_rows * nrow)

    @pl.loop(1, ncol)
    def _(k):
        col_whole(along(ncol - k)).start()

    @here
    def _():
        each_chip(lambda m: chip_whole(col, m).start())

    def combine():
        if ncol > 3:
            @pl.when(jnp.logical_or(col == 1, col == ncol - 2))
            def _():
                settle(vbuf.at[pl.ds(0, ncol - 3)], sem("via"))

        for p in range(ncol):
            @pl.when(via_here(p))
            def _():
                lp[p * lw : (p + 1) * lw, :] += vbuf[p]
                left_term(p).start()

    @pl.when(core == 0)
    def _():
        combine()

    ends = jnp.logical_not(inner)

    @pl.when(inner)
    def _():
        settle(lo.at[pl.ds(0, 2 * lw)], sem("left"))
        settle(lo.at[pl.ds(0, 2 * lw)], sem("relay"))

    @pl.when(ends)
    def _():
        settle(lo.at[pl.ds(0, lw)], sem("left"))

    for peer in range(ncol):
        @pl.when(far_off(peer))
        def _():
            settle(lo.at[pl.ds(0, lw)], sem("leftfar"))

    settle(ro.at[pl.ds(0, chips * rw)], sem("right"))
    settle(ro.at[pl.ds(0, (chips - 1) * rw)], sem("pass"))
    settle(bown, sem("bmate"))
    settle(brow.at[others], sem("bchip"))
    settle(bcol.at[pl.ds(0, ncol - 1)], sem("bcol"))
    settle(wp.at[0], sem("core"))
    settle(xs.at[:, others], sem("chip"))
    settle(mbuf, sem("swap"))

    @pl.loop(1, ncol)
    def _(k):
        q = along(k)
        piece_in = wg_ref.at[core, q, chip]
        settle(piece_in, azr.at[q])
        each_chip(lambda m: chip_whole(q, m).start())

    @pl.when(core == 0)
    def _():
        q = along(ncol - 1)
        each_chip(lambda m: direct_whole(q, 2 * m + 1).start())
        direct_whole(q, mate).start()

    @pl.when(core == 1)
    def _():
        combine()

    @pl.loop(0, ncol)
    def _(k):
        q = along(k)
        settle(wg_ref.at[core, q, others], axr.at[q])

        @pl.when(jnp.logical_or(core == 1, k < ncol - 1))
        def _():
            core_whole(q).start()

    settle(rbuf.at[others], sem("rterm"))
    rg_ref[...] = total([rbuf[m] for m in range(chips)])
    settle(rbuf.at[others], sem("rterms"))
    settle(zs.at[pl.ds(0, ncol - 1)], sem("col"))
    settle(zs.at[pl.ds(0, ncol - 1)], sem("allcol"))
    settle(xs.at[:, others], sem("allchip"))
    settle(wg_ref.at[1 - core], sem("done"))

    @pl.when(core == 0)
    def _():
        settle(wg_ref.at[core, 0], sem("alldirect"))
        settle(wg_ref.at[core, pl.ds(0, ncol - 1)], sem("allcore"))

    @pl.when(core == 1)
    def _():
        settle(wg_ref.at[core], sem("allcore"))
    settle(bcol.at[pl.ds(0, ncol - 1)], sem("bcoled"))
    bg_ref[...] = total([bcol[q] for q in range(ncol)])[0:1, :] / (tile_rows * nrow)
    near_ends = [jnp.logical_and(ncol > 3, col >= 3), jnp.logical_and(ncol > 3, col <= ncol - 4)]
    absent = near_ends[0].astype(jnp.int32) + near_ends[1].astype(jnp.int32)
    for n in range(3):
        if ncol - 1 - n > 0:
            @pl.when(absent == n)
            def _():
                settle(lbuf.at[pl.ds(0, ncol - 1 - n)], sem("term"))

    lg_ref[...] = total([lbuf[q] for q in range(ncol)])
    settle(lbuf.at[pl.ds(0, ncol - 1)], sem("terms"))


def finish_kernel(
    width, pair_ref, lg_ref, rg_ref, wg_ref, bg_ref,
    pair_out, lg_out, rg_out, w_out, bg_out, sems,
):
    halves, ncol, chips, share, _ = wg_ref.shape
    copies = [
        pltpu.make_async_copy(src, dst, sems.at[k])
        for k, (src, dst) in enumerate([
            (pair_ref, pair_out), (lg_ref, lg_out), (rg_ref, rg_out), (bg_ref, bg_out),
        ])
    ]
    for s in range(halves * ncol * chips):
        d, c = divmod(s * share, width)
        q, m = divmod(s, chips)
        h, q = divmod(q, ncol)
        b, q = divmod(q, ncol // 2)
        q += h * (ncol // 2)
        pltpu.make_async_copy(wg_ref.at[b, q, m], w_out.at[pl.ds(c, share), d], sems.at[4]).start()
    for copy in copies:
        copy.start()
    for copy in copies:
        copy.wait()
    pltpu.make_async_copy(wg_ref, wg_ref, sems.at[4]).wait()


def per_device(nrow, ncol, left_factors, right_factors, weight, bias, cotangent):
    samples, li, width = left_factors.shape
    rj = right_factors.shape[1]
    tile_rows, tile_cols, pair_width = cotangent.shape
    channels = weight.shape[0]
    lw, rw = li * width, rj * width
    lefts, rights = tile_rows * width, tile_cols * width
    pairs = tile_rows * tile_cols
    chips, share = nrow // 2, channels // (nrow * ncol)
    group = max(lw, STEP * width)
    dma = pltpu.SemaphoreType.DMA

    def shape(*dims):
        return jax.ShapeDtypeStruct(dims, F32)

    def half(*dims):
        return pltpu.VMEM(dims, BF16)

    def buf(*dims):
        return pltpu.VMEM(dims, F32)

    scratch = [
        buf(lefts, samples), buf(rights, samples), buf(lefts, samples), *[buf(ncol, lw, samples)] * 2,
        buf(rights, samples), buf(rights, samples), *[buf(chips, rw, samples)] * 3,
        buf(2, ncol, chips, share, pair_width), *[buf(ncol, chips, share, pair_width)] * 3,
        *[buf(ncol, share, pair_width)] * 2,
        *[buf(8, pair_width)] * 3, buf(chips, 8, pair_width), buf(8, pair_width), buf(ncol, 8, pair_width),
        buf(channels, pair_width), buf(1, pair_width), buf(pairs, pair_width),
        buf(max(rights, channels), 128),
        *[buf(max(pairs, rights), max(group, STEP * width))] * 2, buf(pair_width, channels),
        half(pairs, 2 * pair_width), half(2 * pair_width, pairs), half(channels, 2 * pair_width),
        half(2 * pair_width, channels), half(pair_width, channels),
        half(rights, lefts), half(rights, lefts), half(rights, 2 * samples), half(2 * samples, rights),
        half(pairs, channels), half(pairs, channels),
        half(2 * samples, group), half(samples, group), half(group, 2 * samples),
        dma((5,)), dma((len(SINGLE),)), dma((ncol, 2)), dma((chips,)),
        dma((ncol,)), dma((ncol,)), dma((ncol,)), dma((ncol,)),
    ]
    pair, lg, rg, wg, bg = pl.pallas_call(
        functools.partial(tile_kernel, nrow, ncol, width),
        out_shape=(
            shape(pairs, pair_width), shape(lw, samples), shape(rw, samples),
            shape(2, ncol, chips, share, pair_width), shape(1, pair_width),
        ),
        in_specs=[HBM] * 5,
        out_specs=[VMEM] * 5,
        scratch_shapes=scratch,
        compiler_params=pltpu.CompilerParams(
            collective_id=0, has_side_effects=True, vmem_limit_bytes=40 * 2**20
        ),
        name="tile",
    )(
        in_hbm(left_factors.transpose(1, 2, 0).reshape(lw, samples)),
        in_hbm(right_factors.transpose(1, 2, 0).reshape(rw, samples)),
        in_hbm(weight),
        in_hbm(bias.reshape(1, pair_width)),
        in_hbm(cotangent.reshape(pairs, pair_width)),
    )
    pair, lg, rg, wg, bg = pl.pallas_call(
        functools.partial(finish_kernel, width),
        out_shape=(
            shape(pairs, pair_width), shape(lw, samples), shape(rw, samples),
            shape(width, channels // width, pair_width), shape(1, pair_width),
        ),
        in_specs=[VMEM] * 5,
        out_specs=[HBM] * 5,
        scratch_shapes=[dma((5,))],
        compiler_params=pltpu.CompilerParams(vmem_limit_bytes=8 * 2**20),
        name="finish",
    )(pair, lg, rg, wg, bg)
    return (
        pair.reshape(tile_rows, tile_cols, pair_width),
        lg.reshape(li, width, samples).transpose(2, 0, 1),
        rg.reshape(rj, width, samples).transpose(2, 0, 1),
        wg.reshape(channels, pair_width),
        bg.reshape(pair_width),
    )


def solution(mesh):
    nrow, ncol = mesh.shape["row"], mesh.shape["col"]
    in_specs = (
        P(None, ("row", "col"), None),
        P(None, ("col", "row"), None),
        P(),
        P(),
        P("row", "col", None),
    )
    out_specs = (
        P("row", "col", None),
        P(None, ("row", "col"), None),
        P(None, ("col", "row"), None),
        P(),
        P(),
    )
    return jax.shard_map(
        functools.partial(per_device, nrow, ncol),
        mesh=mesh, in_specs=in_specs, out_specs=out_specs, check_vma=False,
    )
```

```python
import functools

import jax
import jax.numpy as jnp
from jax import lax
from jax.experimental import pallas as pl
from jax.experimental.pallas import tpu as pltpu
from jax.sharding import PartitionSpec as P

F32 = jnp.float32
BF16 = jnp.bfloat16
MESH = pl.DeviceIdType.MESH
VMEM = pl.BlockSpec(memory_space=pltpu.VMEM)
HBM = pl.BlockSpec(memory_space=pltpu.HBM)
STEP = 8
SINGLE = (
    "left", "leftfar", "relay", "right", "pass", "mate", "passed", "terms", "term", "via", "swap", "swapped",
    "rterms", "rterm", "bmate", "bmated", "bchip", "bchiped", "bcol", "bcoled", "core", "chip", "col", "coled",
    "allcol", "allchip", "allcore", "alldirect", "done",
)


def in_hbm(x):
    return pltpu.with_memory_space_constraint(x, pltpu.HBM)


def split(x):
    high = x.astype(BF16)
    return high, (x - high.astype(F32)).astype(BF16)


def dot(a, b):
    return lax.dot_general(a, b, (((1,), (0,)), ((), ())), preferred_element_type=F32)


def dot_wide(a_high, a_low, b_both):
    half = b_both.shape[1] // 2
    wide = dot(a_high, b_both)
    return wide[:, 0:half] + (wide[:, half:] + dot(a_low, b_both[:, 0:half]))


def dot_tall(a_both, b_high, b_low):
    half = a_both.shape[0] // 2
    tall = dot(a_both, b_high)
    return tall[0:half] + (tall[half:] + dot(a_both[0:half], b_low))


def total(parts):
    return functools.reduce(lambda a, b: a + b, parts)


def swap_groups(pieces):
    lane = lax.broadcasted_iota(jnp.int32, pieces[0].shape, 1)
    low = lane < 64
    even = (lane & 32) == 0

    def far(a, b):
        moved = pltpu.roll(jnp.where(low, b, a), 64, 1)
        return jnp.where(low, a, moved), jnp.where(low, moved, b)

    def near(a, b):
        return (
            jnp.where(even, a, pltpu.roll(b, 32, 1)),
            jnp.where(even, pltpu.roll(a, 96, 1), b),
        )

    p0, p2 = far(pieces[0], pieces[2])
    p1, p3 = far(pieces[1], pieces[3])
    p0, p1 = near(p0, p1)
    p2, p3 = near(p2, p3)
    return p0, p1, p2, p3


def tile_kernel(
    nrow, ncol, width, l_ref, r_ref, w_ref, b_ref, cot_ref,
    pair_ref, lg_ref, rg_ref, wg_ref, bg_ref,
    lo, ro, lp, lbuf, vbuf, rpa, rp, mbuf, rsum, rbuf,
    wp, cbuf, xs, xbuf, zs, zbuf, bown, bmate, bsrc, brow, bmid, bcol,
    w_v, b_v, cot_v, tmp, scr_a, scr_b, acc,
    c2, ct2, w_c, wt2, wt_l, h_h, h_l, rt_c, r2, t_h, t_l, l_c, l_l, lt_c,
    loc, one, glr, grr, kr, xsr, azr, axr,
):
    row, col = lax.axis_index("row"), lax.axis_index("col")
    chip, core = row // 2, lax.rem(row, 2)
    mate = row + 1 - 2 * core
    chips = nrow // 2
    lw, samples = l_ref.shape
    rw = r_ref.shape[0]
    tile_rows, tile_cols = ncol * lw // width, nrow * rw // width
    channels, pair_width = w_ref.shape
    rights = tile_cols * width
    scale = 1.0 / samples
    per = 128 // width
    share = channels // (nrow * ncol)
    lanes_step = STEP * width
    gcols = max(1, lanes_step // lw)
    groups = ncol // gcols
    glanes = gcols * lw
    grows = glanes // width * tile_cols
    own_group = col // gcols
    piece = lw // 2
    lower, upper = col, ncol - 1 - col
    both = jnp.minimum(lower, upper)
    longer = jnp.where(lower > upper, -1, 1)
    halfway = ncol // 2
    low_half = col < halfway
    inner = jnp.logical_and(col > 0, col < ncol - 1)

    def along(k):
        paired = k <= 2 * both
        distance = jnp.where(paired, (k + 1) // 2, k - both)
        side = jnp.where(jnp.logical_and(paired, lax.rem(k, 2) == 0), -longer, longer)
        return col + side * distance

    def order(k):
        far = jnp.where(low_half, ncol - 1 - k, k)
        base = jnp.where(low_half, 0, halfway)
        near = base + lax.rem(col - base + 1 + lax.rem(k, halfway), halfway)
        return jnp.where(k < halfway, far, near)

    def group_at(k):
        return along(k) if gcols == 1 else lax.rem(own_group + k, groups)

    crossed = gcols == 1 and groups >= 4
    span = glanes // 2
    deep = grows // 2

    def units(k):
        if crossed and k >= groups - 2:
            return [2 * group_at(n) + k - (groups - 2) for n in (groups - 2, groups - 1)]
        return [2 * group_at(k) + n for n in range(2)]

    def lanes_of(ref, k):
        return jnp.concatenate([ref[:, pl.ds(pl.multiple_of(n * span, span), span)] for n in units(k)], axis=1)

    def rows_of(ref, k):
        return jnp.concatenate([ref[pl.ds(pl.multiple_of(n * span, span), span), :] for n in units(k)], axis=0)

    def via_end(source, target):
        return jnp.logical_or(
            jnp.logical_and(source == 0, target >= 3),
            jnp.logical_and(source == ncol - 1, target <= ncol - 4),
        )

    def via_here(target):
        return jnp.logical_or(
            jnp.logical_and(col == 1, target >= 3),
            jnp.logical_and(col == ncol - 2, target <= ncol - 4),
        )

    def in_row(peer):
        return {"row": peer, "col": col}

    def in_col(peer):
        return {"row": row, "col": peer}

    def block(ref, index, size):
        return ref.at[pl.ds(pl.multiple_of(index * size, size), size)]

    def each(count, here, act):
        @pl.loop(1, count)
        def _(k):
            act(lax.rem(here + k, count))

    wide = chips // 2
    steps_out = sorted(
        ((a, b) for a in range(wide) for b in range(2) if a + b), key=lambda s: -(min(s[0], wide - s[0]) + s[1])
    )

    def each_chip(act):
        for a, b in steps_out:
            act(lax.rem(chip // 2 + a, wide) * 2 + lax.rem(chip + b, 2))

    def send(src, dst, send_sem, recv_sem, device):
        return pltpu.make_async_remote_copy(
            src_ref=src, dst_ref=dst, send_sem=send_sem, recv_sem=recv_sem,
            device_id=device, device_id_type=MESH,
        )

    def part(ref, index, s):
        return ref.at[pl.ds(pl.multiple_of(index * lw + s * piece, piece), piece)]

    def sem(name):
        return one.at[SINGLE.index(name)]

    def here(act):
        pl.when(row >= 0)(act)

    def fence():
        @pl.when(row < 0)
        def _():
            tmp[0:8, :] = jnp.zeros((8, tmp.shape[1]), F32)

    def settle(ref, semaphore):
        send(ref, ref, semaphore, semaphore, in_row(mate)).wait_recv()

    def left_own(s, side):
        return send(
            part(lo, col, s), part(lo, col, s), sem("left"), glr.at[col, s], in_col(col + side)
        )

    def left_far(peer, s):
        return send(part(lo, col, s), part(lo, col, s), sem("leftfar"), glr.at[col, s], in_col(peer))

    def far_off(peer):
        return jnp.abs(peer - col) >= 3

    def left_on(q, s):
        return send(
            part(lo, q, s), part(lo, q, s), sem("relay"), glr.at[q, s], in_col(col + jnp.where(q < col, 1, -1))
        )

    def right_own(peer, recv):
        return send(block(ro, row, rw), block(ro, row, rw), sem("right"), recv, in_row(peer))

    def right_pass(slot):
        return send(block(ro, slot, rw), block(ro, slot, rw), sem("pass"), sem("passed"), in_row(mate))

    def left_term(peer):
        return send(block(lp, peer, lw), lbuf.at[col], sem("terms"), sem("term"), in_col(peer))

    def left_via(peer):
        return send(
            block(lp, peer, lw), vbuf.at[peer], sem("terms"), sem("via"), in_col(jnp.where(col == 0, 1, ncol - 2))
        )

    def right_swap(m):
        return send(block(rp, 2 * m + 1 - core, rw), mbuf.at[m], sem("swap"), sem("swapped"), in_row(mate))

    def right_term(m):
        return send(rsum.at[m], rbuf.at[chip], sem("rterms"), sem("rterm"), in_row(2 * m + core))

    def bias_mate():
        return send(bown, bmate, sem("bmate"), sem("bmated"), in_row(mate))

    def bias_chip(m):
        return send(bsrc, brow.at[chip], sem("bchip"), sem("bchiped"), in_row(2 * m + core))

    def bias_col(peer):
        return send(bmid, bcol.at[col], sem("bcol"), sem("bcoled"), in_col(peer))

    def core_term(q):
        return send(wp.at[1 - core, q], cbuf.at[q], sem("core"), kr.at[q], in_row(mate))

    def chip_term(q, m):
        return send(xs.at[q, m], xbuf.at[q, chip], sem("chip"), xsr.at[q], in_row(2 * m + core))

    def col_term(peer):
        return send(zs.at[peer], zbuf.at[col], sem("col"), sem("coled"), in_col(peer))

    def col_whole(peer):
        piece = wg_ref.at[core, col, chip]
        return send(piece, piece, sem("allcol"), azr.at[col], in_col(peer))

    def chip_whole(q, m):
        piece = wg_ref.at[core, q, chip]
        return send(piece, piece, sem("allchip"), axr.at[q], in_row(2 * m + core))

    def core_whole(q):
        piece = wg_ref.at[core, q]
        return send(piece, piece, sem("allcore"), sem("done"), in_row(mate))

    def direct_whole(q, to):
        piece = wg_ref.at[core, q, chip]
        return send(piece, piece, sem("alldirect"), sem("done"), in_row(to))

    others = pl.ds(0, chips - 1)
    own_left = pl.ds(pl.multiple_of(col * lw, lw), lw)
    own_right = pl.ds(pl.multiple_of(row * rw, rw), rw)
    loads = [
        pltpu.make_async_copy(src, dst, loc.at[k])
        for k, (src, dst) in enumerate([
            (l_ref, lo.at[own_left]), (r_ref, ro.at[own_right]), (w_ref, w_v), (cot_ref, cot_v), (b_ref, b_v),
        ])
    ]
    barrier = pltpu.get_barrier_semaphore()
    for load in loads:
        load.start()
    def hello(device):
        pl.semaphore_signal(barrier, inc=1, device_id=device, device_id_type=MESH)

    for k in range(1, ncol):
        hello(in_col(lax.rem(col + k, ncol)))
    each_chip(lambda m: hello(in_row(2 * m + core)))
    hello(in_row(mate))
    pl.semaphore_wait(barrier, ncol + chips - 1)
    loads[0].wait()
    loads[1].wait()

    for s in range(2):
        @pl.when(col < ncol - 1)
        def _():
            left_own(s, 1).start()

        @pl.when(col > 0)
        def _():
            left_own(s, -1).start()

    for peer in range(ncol):
        @pl.when(far_off(peer))
        def _():
            for s in range(2):
                left_far(peer, s).start()

    @here
    def _():
        each_chip(lambda m: right_own(2 * m + core, grr.at[chip]).start())
        right_own(mate, sem("mate")).start()


    fence()

    loads[2].wait()
    loads[3].wait()
    for d in range(width):
        tmp[d * width : (d + 1) * width, :] = w_v[pl.ds(d, width, stride=width), :]
    weight = tmp[0:channels, :]
    w_c[:, 0:pair_width], w_c[:, pair_width:] = split(weight)
    high, wt_l[...] = split(weight.T * scale)
    wt2[0:pair_width, :] = high
    wt2[pair_width:, :] = high
    cot = cot_v[...]
    c2[:, 0:pair_width], c2[:, pair_width:] = split(cot)
    ct2[0:pair_width, :], ct2[pair_width:, :] = split(cot.T)
    bown[...] = jnp.broadcast_to(jnp.sum(cot, axis=0, keepdims=True), (8, pair_width))
    bias_mate().start()

    fence()

    scrs = [scr_a, scr_b]
    steps = channels // lanes_step

    def grad_block(b):
        lanes = slice(b * lanes_step, (b + 1) * lanes_step)
        scrs[b % 2][...] = dot(c2[...], wt2[:, lanes]) + dot(c2[:, 0:pair_width], wt_l[:, lanes])

    def grad_swap(b):
        scr = scrs[b % 2]
        for u in range(STEP // per):
            for v in range(tile_rows // per):
                pieces = [
                    scr[(v * per + a) * tile_cols : (v * per + a + 1) * tile_cols, u * 128 : (u + 1) * 128]
                    for a in range(per)
                ]
                for a, piece in enumerate(swap_groups(pieces)):
                    at = (b * STEP + u * per + a) * tile_cols
                    high, low = split(piece)
                    h_h[at : at + tile_cols, v * 128 : (v + 1) * 128] = high
                    h_l[at : at + tile_cols, v * 128 : (v + 1) * 128] = low

    def relay(k, s):
        @pl.when(inner)
        def _():
            q = along(k)
            left_on(q, s).wait_recv()
            left_on(q, s).start()

    def arrive(k, pieces=(0, 1)):
        @pl.when(jnp.logical_or(k > 2, jnp.logical_not(inner)))
        def _():
            q = along(k)
            for s in pieces:
                left_on(q, s).wait_recv()

    def ready(k):
        if crossed and k >= groups - 2:
            for n in (groups - 2, groups - 1):
                arrive(n, (k - (groups - 2),))
        elif gcols == 1 and k > 0:
            arrive(k)

    near = range(1, min(ncol, 3))
    grad_block(0)
    for b in range(steps):
        if b + 1 < steps:
            grad_block(b + 1)
        grad_swap(b)
    fence()

    for k in near:
        relay(k, 0)

    def right_grad(k):
        lt_c[:, 0:samples], lt_c[:, samples:] = split(rows_of(lo, k))
        term = dot_wide(lanes_of(h_h, k), lanes_of(h_l, k), lt_c[...])
        if k == 0:
            rpa[...] = term
        else:
            rpa[...] += term

    early = 1 if gcols == 1 and groups > 1 else 0
    fence()

    if early:
        right_grad(0)
    for k in near:
        relay(k, 1)
    fence()

    settle(bmate, sem("bmated"))
    bsrc[...] = bown[...] + bmate[...]
    brow[chip] = bsrc[...]
    each_chip(lambda m: bias_chip(m).start())

    def hand_over(m):
        settle(block(ro, 0, rw), grr.at[m])

        @here
        def _():
            right_pass(2 * m + core).start()

    for a, b in reversed(steps_out):
        hand_over(lax.rem(chip // 2 + a, wide) * 2 + lax.rem(chip + b, 2))
    settle(block(ro, 0, rw), sem("mate"))
    settle(block(ro, 0, (chips - 1) * rw), sem("passed"))
    fence()

    for d in range(width):
        tmp[d * tile_cols : (d + 1) * tile_cols, :] = ro[pl.ds(d, tile_cols, stride=width), :]
    right = tmp[0:rights, :]
    rt_c[:, 0:samples], rt_c[:, samples:] = split(right)
    r2[0:samples, :], r2[samples:, :] = split(right.T)


    def left_grad(k):
        g = group_at(groups - 1 - k)
        lanes = pl.ds(pl.multiple_of(g * glanes, glanes), glanes)
        lp[lanes, :] = dot_tall(r2[...], h_h[:, lanes], h_l[:, lanes]).T

    def send_term(k):
        peer = along(ncol - 1 - k)

        @pl.when(via_end(col, peer))
        def _():
            left_via(peer).start()

        @pl.when(jnp.logical_not(jnp.logical_or(via_end(col, peer), via_here(peer))))
        def _():
            left_term(peer).start()

        @pl.when(via_end(peer, col))
        def _():
            lbuf[peer] = jnp.zeros(lbuf.shape[1:], F32)

    if gcols > 1:
        @pl.loop(1, ncol)
        def _(k):
            arrive(k)

    middle = channels // 2

    def outer(k, halves, beside, then):
        high, l_l[...] = split(rows_of(lo, k).T * scale)
        l_c[0:samples, :] = high
        l_c[samples:, :] = high
        half = rights // 2
        units = width // per // 2
        for scr, h in zip(scrs, halves):
            at = pl.ds(pl.multiple_of(h * half, half), half)
            scr[0:half, 0:glanes] = dot(rt_c[at, :], l_c[...]) + dot(rt_c[at, 0:samples], l_l[...])
        beside()
        for scr, h in zip(scrs, halves):
            for u in range(units):
                for v in range(glanes // 128):
                    pieces = [
                        scr[(u * per + a) * tile_cols : (u * per + a + 1) * tile_cols, v * 128 : (v + 1) * 128]
                        for a in range(per)
                    ]
                    lanes = pl.ds(pl.multiple_of(h * middle + u * 128, 128), 128)
                    for a, piece in enumerate(swap_groups(pieces)):
                        at = k * grows + (v * per + a) * tile_cols
                        high, low = split(piece)
                        t_h[at : at + tile_cols, lanes] = high
                        t_l[at : at + tile_cols, lanes] = low
            then(h)

    def weight_grad(k, lanes):
        at = slice(k * grows, (k + 1) * grows)
        both = jnp.concatenate([ct2[:, pl.ds(pl.multiple_of(n * deep, deep), deep)] for n in units(k)], axis=1)
        term = dot_tall(both, t_h[at, lanes], t_l[at, lanes])
        if k == 0:
            acc[:, lanes] = term
        else:
            acc[:, lanes] += term

    def beside(k):
        if k < groups - 1 or gcols > 1:
            left_grad(k)
        if k > 0:
            weight_grad(k - 1, slice(0, channels))

    for k in range(groups - 1):
        ready(k)
        outer(k, (0, 1), functools.partial(beside, k), lambda h: None)
        if gcols == 1:
            @pl.when(jnp.logical_not(inner))
            def _():
                send_term(k)

    if gcols == 1:
        @pl.when(inner)
        def _():
            for k in range(groups - 1):
                send_term(k)

    ready(groups - 1)
    turned = jnp.where(low_half, 1, 0)

    def last_half(h):
        start = pl.multiple_of(h * middle, middle)
        weight_grad(groups - 1, pl.ds(start, middle))
        for i in range(middle // 128):
            terms = acc[:, pl.ds(pl.multiple_of(start + i * 128, 128), 128)].T
            for n in range(128 // share):
                b, q = divmod((i * 128) // share + n, halfway * chips)
                q, m = divmod(q, chips)
                wp[b, h * halfway + q, m] = terms[n * share : (n + 1) * share, :]

        @here
        def _():
            for q in range(halfway):
                core_term(h * halfway + q).start()

    outer(groups - 1, (turned, 1 - turned), functools.partial(beside, groups - 1), last_half)

    def chip_terms(first):
        for k in range(first, first + halfway):
            q = order(k)
            core_term(q).wait_recv()
            xs[q] = wp[core, q] + cbuf[q]
            xbuf[q, chip] = xs[q, chip]

            @here
            def _():
                each_chip(lambda m: chip_term(q, m).start())

    if gcols > 1:
        for k in range(ncol - 1):
            send_term(k)
    chip_terms(0)
    chip_terms(halfway)
    for k in range(early, groups - 1):
        right_grad(k)
    loads[4].wait()
    if gcols == 1:
        left_grad(groups - 1)
    lbuf[col] = lp[own_left, :]
    right_grad(groups - 1)
    settle(brow.at[others], sem("bchiped"))
    bmid[...] = total([brow[m] for m in range(chips)])
    bcol[col] = bmid[...]
    each(ncol, col, lambda p: bias_col(p).start())

    for d in range(width):
        rp[pl.ds(d, tile_cols, stride=width), :] = rpa[d * tile_cols : (d + 1) * tile_cols, :]

    @here
    def _():
        for m in range(chips):
            right_swap(m).start()

    for k in range(ncol - 1):
        q = order(k)
        settle(xbuf.at[q, others], xsr.at[q])
        zs[q] = total([xbuf[q, m] for m in range(chips)])

        @here
        def _():
            col_term(q).start()

    settle(mbuf, sem("swapped"))
    for m in range(chips):
        rsum[m] = rp[pl.ds(pl.multiple_of((2 * m + core) * rw, rw), rw), :] + mbuf[m]

    @here
    def _():
        each_chip(lambda m: right_term(m).start())

    rbuf[chip] = rsum[chip]
    settle(xbuf.at[col, others], xsr.at[col])
    zbuf[col] = total([xbuf[col, m] for m in range(chips)])
    pair = dot_wide(t_h[...], t_l[...], w_c[...]) + b_v[...]
    for k in range(groups):
        for n, unit in enumerate(units(k)):
            at = k * grows + n * deep
            pair_ref[pl.ds(pl.multiple_of(unit * deep, deep), deep), :] = pair[at : at + deep, :]
    settle(zbuf.at[pl.ds(0, ncol - 1)], sem("coled"))
    wg_ref[core, col, chip] = total([zbuf[q] for q in range(ncol)]) / (tile_rows * nrow)

    @pl.loop(1, ncol)
    def _(k):
        col_whole(along(ncol - k)).start()

    @here
    def _():
        each_chip(lambda m: chip_whole(col, m).start())

    def combine():
        if ncol > 3:
            @pl.when(jnp.logical_or(col == 1, col == ncol - 2))
            def _():
                settle(vbuf.at[pl.ds(0, ncol - 3)], sem("via"))

        for p in range(ncol):
            @pl.when(via_here(p))
            def _():
                lp[p * lw : (p + 1) * lw, :] += vbuf[p]
                left_term(p).start()

    @pl.when(core == 0)
    def _():
        combine()

    ends = jnp.logical_not(inner)

    @pl.when(inner)
    def _():
        settle(lo.at[pl.ds(0, 2 * lw)], sem("left"))
        settle(lo.at[pl.ds(0, 2 * lw)], sem("relay"))

    @pl.when(ends)
    def _():
        settle(lo.at[pl.ds(0, lw)], sem("left"))

    for peer in range(ncol):
        @pl.when(far_off(peer))
        def _():
            settle(lo.at[pl.ds(0, lw)], sem("leftfar"))

    settle(ro.at[pl.ds(0, chips * rw)], sem("right"))
    settle(ro.at[pl.ds(0, (chips - 1) * rw)], sem("pass"))
    settle(bown, sem("bmate"))
    settle(brow.at[others], sem("bchip"))
    settle(bcol.at[pl.ds(0, ncol - 1)], sem("bcol"))
    settle(wp.at[0], sem("core"))
    settle(xs.at[:, others], sem("chip"))
    settle(mbuf, sem("swap"))

    @pl.loop(1, ncol)
    def _(k):
        q = along(k)
        piece_in = wg_ref.at[core, q, chip]
        settle(piece_in, azr.at[q])
        each_chip(lambda m: chip_whole(q, m).start())

    @pl.when(core == 0)
    def _():
        q = along(ncol - 1)
        each_chip(lambda m: direct_whole(q, 2 * m + 1).start())
        direct_whole(q, mate).start()

    @pl.when(core == 1)
    def _():
        combine()

    @pl.loop(0, ncol)
    def _(k):
        q = along(k)
        settle(wg_ref.at[core, q, others], axr.at[q])

        @pl.when(jnp.logical_or(core == 1, k < ncol - 1))
        def _():
            core_whole(q).start()

    settle(rbuf.at[others], sem("rterm"))
    rg_ref[...] = total([rbuf[m] for m in range(chips)])
    settle(rbuf.at[others], sem("rterms"))
    settle(zs.at[pl.ds(0, ncol - 1)], sem("col"))
    settle(zs.at[pl.ds(0, ncol - 1)], sem("allcol"))
    settle(xs.at[:, others], sem("allchip"))
    settle(wg_ref.at[1 - core], sem("done"))

    @pl.when(core == 0)
    def _():
        settle(wg_ref.at[core, 0], sem("alldirect"))
        settle(wg_ref.at[core, pl.ds(0, ncol - 1)], sem("allcore"))

    @pl.when(core == 1)
    def _():
        settle(wg_ref.at[core], sem("allcore"))
    settle(bcol.at[pl.ds(0, ncol - 1)], sem("bcoled"))
    bg_ref[...] = total([bcol[q] for q in range(ncol)])[0:1, :] / (tile_rows * nrow)
    near_ends = [jnp.logical_and(ncol > 3, col >= 3), jnp.logical_and(ncol > 3, col <= ncol - 4)]
    absent = near_ends[0].astype(jnp.int32) + near_ends[1].astype(jnp.int32)
    for n in range(3):
        if ncol - 1 - n > 0:
            @pl.when(absent == n)
            def _():
                settle(lbuf.at[pl.ds(0, ncol - 1 - n)], sem("term"))

    lg_ref[...] = total([lbuf[q] for q in range(ncol)])
    settle(lbuf.at[pl.ds(0, ncol - 1)], sem("terms"))


def finish_kernel(
    width, pair_ref, lg_ref, rg_ref, wg_ref, bg_ref,
    pair_out, lg_out, rg_out, w_out, bg_out, sems,
):
    halves, ncol, chips, share, _ = wg_ref.shape
    copies = [
        pltpu.make_async_copy(src, dst, sems.at[k])
        for k, (src, dst) in enumerate([
            (pair_ref, pair_out), (lg_ref, lg_out), (rg_ref, rg_out), (bg_ref, bg_out),
        ])
    ]
    for s in range(halves * ncol * chips):
        d, c = divmod(s * share, width)
        q, m = divmod(s, chips)
        h, q = divmod(q, ncol)
        b, q = divmod(q, ncol // 2)
        q += h * (ncol // 2)
        pltpu.make_async_copy(wg_ref.at[b, q, m], w_out.at[pl.ds(c, share), d], sems.at[4]).start()
    for copy in copies:
        copy.start()
    for copy in copies:
        copy.wait()
    pltpu.make_async_copy(wg_ref, wg_ref, sems.at[4]).wait()


def per_device(nrow, ncol, left_factors, right_factors, weight, bias, cotangent):
    samples, li, width = left_factors.shape
    rj = right_factors.shape[1]
    tile_rows, tile_cols, pair_width = cotangent.shape
    channels = weight.shape[0]
    lw, rw = li * width, rj * width
    lefts, rights = tile_rows * width, tile_cols * width
    pairs = tile_rows * tile_cols
    chips, share = nrow // 2, channels // (nrow * ncol)
    group = max(lw, STEP * width)
    dma = pltpu.SemaphoreType.DMA

    def shape(*dims):
        return jax.ShapeDtypeStruct(dims, F32)

    def half(*dims):
        return pltpu.VMEM(dims, BF16)

    def buf(*dims):
        return pltpu.VMEM(dims, F32)

    scratch = [
        buf(lefts, samples), buf(rights, samples), buf(lefts, samples), *[buf(ncol, lw, samples)] * 2,
        buf(rights, samples), buf(rights, samples), *[buf(chips, rw, samples)] * 3,
        buf(2, ncol, chips, share, pair_width), *[buf(ncol, chips, share, pair_width)] * 3,
        *[buf(ncol, share, pair_width)] * 2,
        *[buf(8, pair_width)] * 3, buf(chips, 8, pair_width), buf(8, pair_width), buf(ncol, 8, pair_width),
        buf(channels, pair_width), buf(1, pair_width), buf(pairs, pair_width),
        buf(max(rights, channels), 128),
        *[buf(max(pairs, rights), max(group, STEP * width))] * 2, buf(pair_width, channels),
        half(pairs, 2 * pair_width), half(2 * pair_width, pairs), half(channels, 2 * pair_width),
        half(2 * pair_width, channels), half(pair_width, channels),
        half(rights, lefts), half(rights, lefts), half(rights, 2 * samples), half(2 * samples, rights),
        half(pairs, channels), half(pairs, channels),
        half(2 * samples, group), half(samples, group), half(group, 2 * samples),
        dma((5,)), dma((len(SINGLE),)), dma((ncol, 2)), dma((chips,)),
        dma((ncol,)), dma((ncol,)), dma((ncol,)), dma((ncol,)),
    ]
    pair, lg, rg, wg, bg = pl.pallas_call(
        functools.partial(tile_kernel, nrow, ncol, width),
        out_shape=(
            shape(pairs, pair_width), shape(lw, samples), shape(rw, samples),
            shape(2, ncol, chips, share, pair_width), shape(1, pair_width),
        ),
        in_specs=[HBM] * 5,
        out_specs=[VMEM] * 5,
        scratch_shapes=scratch,
        compiler_params=pltpu.CompilerParams(
            collective_id=0, has_side_effects=True, vmem_limit_bytes=40 * 2**20
        ),
        name="tile",
    )(
        in_hbm(left_factors.transpose(1, 2, 0).reshape(lw, samples)),
        in_hbm(right_factors.transpose(1, 2, 0).reshape(rw, samples)),
        in_hbm(weight),
        in_hbm(bias.reshape(1, pair_width)),
        in_hbm(cotangent.reshape(pairs, pair_width)),
    )
    pair, lg, rg, wg, bg = pl.pallas_call(
        functools.partial(finish_kernel, width),
        out_shape=(
            shape(pairs, pair_width), shape(lw, samples), shape(rw, samples),
            shape(width, channels // width, pair_width), shape(1, pair_width),
        ),
        in_specs=[VMEM] * 5,
        out_specs=[HBM] * 5,
        scratch_shapes=[dma((5,))],
        compiler_params=pltpu.CompilerParams(vmem_limit_bytes=8 * 2**20),
        name="finish",
    )(pair, lg, rg, wg, bg)
    return (
        pair.reshape(tile_rows, tile_cols, pair_width),
        lg.reshape(li, width, samples).transpose(2, 0, 1),
        rg.reshape(rj, width, samples).transpose(2, 0, 1),
        wg.reshape(channels, pair_width),
        bg.reshape(pair_width),
    )


def solution(mesh):
    nrow, ncol = mesh.shape["row"], mesh.shape["col"]
    in_specs = (
        P(None, ("row", "col"), None),
        P(None, ("col", "row"), None),
        P(),
        P(),
        P("row", "col", None),
    )
    out_specs = (
        P("row", "col", None),
        P(None, ("row", "col"), None),
        P(None, ("col", "row"), None),
        P(),
        P(),
    )
    return jax.shard_map(
        functools.partial(per_device, nrow, ncol),
        mesh=mesh, in_specs=in_specs, out_specs=out_specs, check_vma=False,
    )
```

```python
import functools

import jax
import jax.numpy as jnp
from jax import lax
from jax.experimental import pallas as pl
from jax.experimental.pallas import tpu as pltpu
from jax.sharding import PartitionSpec as P

F32 = jnp.float32
BF16 = jnp.bfloat16
MESH = pl.DeviceIdType.MESH
VMEM = pl.BlockSpec(memory_space=pltpu.VMEM)
HBM = pl.BlockSpec(memory_space=pltpu.HBM)
STEP = 8
SINGLE = (
    "left", "leftfar", "relay", "right", "pass", "mate", "passed", "terms", "term", "via", "swap", "swapped",
    "rterms", "rterm", "bmate", "bmated", "bchip", "bchiped", "bcol", "bcoled", "core", "chip", "col", "coled",
    "allcol", "allchip", "allcore", "alldirect", "done",
)


def in_hbm(x):
    return pltpu.with_memory_space_constraint(x, pltpu.HBM)


def split(x):
    high = x.astype(BF16)
    return high, (x - high.astype(F32)).astype(BF16)


def dot(a, b):
    return lax.dot_general(a, b, (((1,), (0,)), ((), ())), preferred_element_type=F32)


def dot_wide(a_high, a_low, b_both):
    half = b_both.shape[1] // 2
    wide = dot(a_high, b_both)
    return wide[:, 0:half] + (wide[:, half:] + dot(a_low, b_both[:, 0:half]))


def dot_tall(a_both, b_high, b_low):
    half = a_both.shape[0] // 2
    tall = dot(a_both, b_high)
    return tall[0:half] + (tall[half:] + dot(a_both[0:half], b_low))


def total(parts):
    return functools.reduce(lambda a, b: a + b, parts)


def swap_groups(pieces):
    lane = lax.broadcasted_iota(jnp.int32, pieces[0].shape, 1)
    low = lane < 64
    even = (lane & 32) == 0

    def far(a, b):
        moved = pltpu.roll(jnp.where(low, b, a), 64, 1)
        return jnp.where(low, a, moved), jnp.where(low, moved, b)

    def near(a, b):
        return (
            jnp.where(even, a, pltpu.roll(b, 32, 1)),
            jnp.where(even, pltpu.roll(a, 96, 1), b),
        )

    p0, p2 = far(pieces[0], pieces[2])
    p1, p3 = far(pieces[1], pieces[3])
    p0, p1 = near(p0, p1)
    p2, p3 = near(p2, p3)
    return p0, p1, p2, p3


def tile_kernel(
    nrow, ncol, width, l_ref, r_ref, w_ref, b_ref, cot_ref,
    pair_ref, lg_ref, rg_ref, wg_ref, bg_ref,
    lo, ro, lp, lbuf, vbuf, rpa, rp, mbuf, rsum, rbuf,
    wp, cbuf, xs, xbuf, zs, zbuf, bown, bmate, bsrc, brow, bmid, bcol,
    w_v, b_v, cot_v, tmp, scr_a, scr_b, acc,
    c2, ct2, w_c, wt2, wt_l, h_h, h_l, rt_c, r2, t_h, t_l, l_c, l_l, lt_c,
    loc, one, glr, grr, kr, xsr, azr, axr,
):
    row, col = lax.axis_index("row"), lax.axis_index("col")
    chip, core = row // 2, lax.rem(row, 2)
    mate = row + 1 - 2 * core
    chips = nrow // 2
    lw, samples = l_ref.shape
    rw = r_ref.shape[0]
    tile_rows, tile_cols = ncol * lw // width, nrow * rw // width
    channels, pair_width = w_ref.shape
    rights = tile_cols * width
    scale = 1.0 / samples
    per = 128 // width
    share = channels // (nrow * ncol)
    lanes_step = STEP * width
    gcols = max(1, lanes_step // lw)
    groups = ncol // gcols
    glanes = gcols * lw
    grows = glanes // width * tile_cols
    own_group = col // gcols
    piece = lw // 2
    lower, upper = col, ncol - 1 - col
    both = jnp.minimum(lower, upper)
    longer = jnp.where(lower > upper, -1, 1)
    halfway = ncol // 2
    low_half = col < halfway
    inner = jnp.logical_and(col > 0, col < ncol - 1)

    def along(k):
        paired = k <= 2 * both
        distance = jnp.where(paired, (k + 1) // 2, k - both)
        side = jnp.where(jnp.logical_and(paired, lax.rem(k, 2) == 0), -longer, longer)
        return col + side * distance

    def order(k):
        far = jnp.where(low_half, ncol - 1 - k, k)
        base = jnp.where(low_half, 0, halfway)
        near = base + lax.rem(col - base + 1 + lax.rem(k, halfway), halfway)
        return jnp.where(k < halfway, far, near)

    def group_at(k):
        return along(k) if gcols == 1 else lax.rem(own_group + k, groups)

    crossed = gcols == 1 and groups >= 4
    span = glanes // 2
    deep = grows // 2

    def units(k):
        if crossed and k >= groups - 2:
            return [2 * group_at(n) + k - (groups - 2) for n in (groups - 2, groups - 1)]
        return [2 * group_at(k) + n for n in range(2)]

    def lanes_of(ref, k):
        return jnp.concatenate([ref[:, pl.ds(pl.multiple_of(n * span, span), span)] for n in units(k)], axis=1)

    def rows_of(ref, k):
        return jnp.concatenate([ref[pl.ds(pl.multiple_of(n * span, span), span), :] for n in units(k)], axis=0)

    def via_end(source, target):
        return jnp.logical_or(
            jnp.logical_and(source == 0, target >= 3),
            jnp.logical_and(source == ncol - 1, target <= ncol - 4),
        )

    def via_here(target):
        return jnp.logical_or(
            jnp.logical_and(col == 1, target >= 3),
            jnp.logical_and(col == ncol - 2, target <= ncol - 4),
        )

    def in_row(peer):
        return {"row": peer, "col": col}

    def in_col(peer):
        return {"row": row, "col": peer}

    def block(ref, index, size):
        return ref.at[pl.ds(pl.multiple_of(index * size, size), size)]

    def each(count, here, act):
        @pl.loop(1, count)
        def _(k):
            act(lax.rem(here + k, count))

    wide = chips // 2
    steps_out = sorted(
        ((a, b) for a in range(wide) for b in range(2) if a + b), key=lambda s: -(min(s[0], wide - s[0]) + s[1])
    )

    def each_chip(act):
        for a, b in steps_out:
            act(lax.rem(chip // 2 + a, wide) * 2 + lax.rem(chip + b, 2))

    def send(src, dst, send_sem, recv_sem, device):
        return pltpu.make_async_remote_copy(
            src_ref=src, dst_ref=dst, send_sem=send_sem, recv_sem=recv_sem,
            device_id=device, device_id_type=MESH,
        )

    def part(ref, index, s):
        return ref.at[pl.ds(pl.multiple_of(index * lw + s * piece, piece), piece)]

    def sem(name):
        return one.at[SINGLE.index(name)]

    def here(act):
        pl.when(row >= 0)(act)

    def fence():
        @pl.when(row < 0)
        def _():
            tmp[0:8, :] = jnp.zeros((8, tmp.shape[1]), F32)

    def settle(ref, semaphore):
        send(ref, ref, semaphore, semaphore, in_row(mate)).wait_recv()

    def left_own(s, side):
        return send(
            part(lo, col, s), part(lo, col, s), sem("left"), glr.at[col, s], in_col(col + side)
        )

    def left_far(peer, s):
        return send(part(lo, col, s), part(lo, col, s), sem("leftfar"), glr.at[col, s], in_col(peer))

    def far_off(peer):
        return jnp.abs(peer - col) >= 3

    def left_on(q, s):
        return send(
            part(lo, q, s), part(lo, q, s), sem("relay"), glr.at[q, s], in_col(col + jnp.where(q < col, 1, -1))
        )

    def right_own(peer, recv):
        return send(block(ro, row, rw), block(ro, row, rw), sem("right"), recv, in_row(peer))

    def right_pass(slot):
        return send(block(ro, slot, rw), block(ro, slot, rw), sem("pass"), sem("passed"), in_row(mate))

    def left_term(peer):
        return send(block(lp, peer, lw), lbuf.at[col], sem("terms"), sem("term"), in_col(peer))

    def left_via(peer):
        return send(
            block(lp, peer, lw), vbuf.at[peer], sem("terms"), sem("via"), in_col(jnp.where(col == 0, 1, ncol - 2))
        )

    def right_swap(m):
        return send(block(rp, 2 * m + 1 - core, rw), mbuf.at[m], sem("swap"), sem("swapped"), in_row(mate))

    def right_term(m):
        return send(rsum.at[m], rbuf.at[chip], sem("rterms"), sem("rterm"), in_row(2 * m + core))

    def bias_mate():
        return send(bown, bmate, sem("bmate"), sem("bmated"), in_row(mate))

    def bias_chip(m):
        return send(bsrc, brow.at[chip], sem("bchip"), sem("bchiped"), in_row(2 * m + core))

    def bias_col(peer):
        return send(bmid, bcol.at[col], sem("bcol"), sem("bcoled"), in_col(peer))

    def core_term(q):
        return send(wp.at[1 - core, q], cbuf.at[q], sem("core"), kr.at[q], in_row(mate))

    def chip_term(q, m):
        return send(xs.at[q, m], xbuf.at[q, chip], sem("chip"), xsr.at[q], in_row(2 * m + core))

    def col_term(peer):
        return send(zs.at[peer], zbuf.at[col], sem("col"), sem("coled"), in_col(peer))

    def col_whole(peer):
        piece = wg_ref.at[core, col, chip]
        return send(piece, piece, sem("allcol"), azr.at[col], in_col(peer))

    def chip_whole(q, m):
        piece = wg_ref.at[core, q, chip]
        return send(piece, piece, sem("allchip"), axr.at[q], in_row(2 * m + core))

    def core_whole(q):
        piece = wg_ref.at[core, q]
        return send(piece, piece, sem("allcore"), sem("done"), in_row(mate))

    def direct_whole(q, to):
        piece = wg_ref.at[core, q, chip]
        return send(piece, piece, sem("alldirect"), sem("done"), in_row(to))

    others = pl.ds(0, chips - 1)
    own_left = pl.ds(pl.multiple_of(col * lw, lw), lw)
    own_right = pl.ds(pl.multiple_of(row * rw, rw), rw)
    loads = [
        pltpu.make_async_copy(src, dst, loc.at[k])
        for k, (src, dst) in enumerate([
            (l_ref, lo.at[own_left]), (r_ref, ro.at[own_right]), (w_ref, w_v), (cot_ref, cot_v), (b_ref, b_v),
        ])
    ]
    barrier = pltpu.get_barrier_semaphore()
    for load in loads:
        load.start()
    def hello(device):
        pl.semaphore_signal(barrier, inc=1, device_id=device, device_id_type=MESH)

    for k in range(1, ncol):
        hello(in_col(lax.rem(col + k, ncol)))
    each_chip(lambda m: hello(in_row(2 * m + core)))
    hello(in_row(mate))
    pl.semaphore_wait(barrier, ncol + chips - 1)
    loads[0].wait()
    loads[1].wait()

    for s in range(2):
        @pl.when(col < ncol - 1)
        def _():
            left_own(s, 1).start()

        @pl.when(col > 0)
        def _():
            left_own(s, -1).start()

    for peer in range(ncol):
        @pl.when(far_off(peer))
        def _():
            for s in range(2):
                left_far(peer, s).start()

    @here
    def _():
        each_chip(lambda m: right_own(2 * m + core, grr.at[chip]).start())
        right_own(mate, sem("mate")).start()


    fence()

    loads[2].wait()
    loads[3].wait()
    for d in range(width):
        tmp[d * width : (d + 1) * width, :] = w_v[pl.ds(d, width, stride=width), :]
    weight = tmp[0:channels, :]
    w_c[:, 0:pair_width], w_c[:, pair_width:] = split(weight)
    high, wt_l[...] = split(weight.T * scale)
    wt2[0:pair_width, :] = high
    wt2[pair_width:, :] = high
    cot = cot_v[...]
    c2[:, 0:pair_width], c2[:, pair_width:] = split(cot)
    ct2[0:pair_width, :], ct2[pair_width:, :] = split(cot.T)
    bown[...] = jnp.broadcast_to(jnp.sum(cot, axis=0, keepdims=True), (8, pair_width))
    bias_mate().start()

    fence()

    scrs = [scr_a, scr_b]
    steps = channels // lanes_step

    def grad_block(b):
        lanes = slice(b * lanes_step, (b + 1) * lanes_step)
        scrs[b % 2][...] = dot(c2[...], wt2[:, lanes]) + dot(c2[:, 0:pair_width], wt_l[:, lanes])

    def grad_swap(b):
        scr = scrs[b % 2]
        for u in range(STEP // per):
            for v in range(tile_rows // per):
                pieces = [
                    scr[(v * per + a) * tile_cols : (v * per + a + 1) * tile_cols, u * 128 : (u + 1) * 128]
                    for a in range(per)
                ]
                for a, piece in enumerate(swap_groups(pieces)):
                    at = (b * STEP + u * per + a) * tile_cols
                    high, low = split(piece)
                    h_h[at : at + tile_cols, v * 128 : (v + 1) * 128] = high
                    h_l[at : at + tile_cols, v * 128 : (v + 1) * 128] = low

    def relay(k, s):
        @pl.when(inner)
        def _():
            q = along(k)
            left_on(q, s).wait_recv()
            left_on(q, s).start()

    def arrive(k, pieces=(0, 1)):
        @pl.when(jnp.logical_or(k > 2, jnp.logical_not(inner)))
        def _():
            q = along(k)
            for s in pieces:
                settle(part(lo, q, s), glr.at[q, s])

    def ready(k):
        if crossed and k >= groups - 2:
            for n in (groups - 2, groups - 1):
                arrive(n, (k - (groups - 2),))
        elif gcols == 1 and k > 0:
            arrive(k)

    near = range(1, min(ncol, 3))
    grad_block(0)
    for b in range(steps):
        if b + 1 < steps:
            grad_block(b + 1)
        else:
            @pl.when(core == 1)
            def _():
                for k in near:
                    relay(k, 0)

        grad_swap(b)
    fence()

    @pl.when(core == 0)
    def _():
        for k in near:
            relay(k, 0)


    def right_grad(k):
        lt_c[:, 0:samples], lt_c[:, samples:] = split(rows_of(lo, k))
        term = dot_wide(lanes_of(h_h, k), lanes_of(h_l, k), lt_c[...])
        if k == 0:
            rpa[...] = term
        else:
            rpa[...] += term

    early = 1 if gcols == 1 and groups > 1 else 0
    fence()

    if early:
        right_grad(0)
    for k in near:
        relay(k, 1)
    fence()

    settle(bmate, sem("bmated"))
    bsrc[...] = bown[...] + bmate[...]
    brow[chip] = bsrc[...]
    each_chip(lambda m: bias_chip(m).start())

    def hand_over(m):
        settle(block(ro, 0, rw), grr.at[m])

        @here
        def _():
            right_pass(2 * m + core).start()

    for a, b in reversed(steps_out):
        hand_over(lax.rem(chip // 2 + a, wide) * 2 + lax.rem(chip + b, 2))
    settle(block(ro, 0, rw), sem("mate"))
    settle(block(ro, 0, (chips - 1) * rw), sem("passed"))
    fence()

    for d in range(width):
        tmp[d * tile_cols : (d + 1) * tile_cols, :] = ro[pl.ds(d, tile_cols, stride=width), :]
    right = tmp[0:rights, :]
    rt_c[:, 0:samples], rt_c[:, samples:] = split(right)
    r2[0:samples, :], r2[samples:, :] = split(right.T)


    def left_grad(k):
        g = group_at(groups - 1 - k)
        lanes = pl.ds(pl.multiple_of(g * glanes, glanes), glanes)
        lp[lanes, :] = dot_tall(r2[...], h_h[:, lanes], h_l[:, lanes]).T

    def send_term(k):
        peer = along(ncol - 1 - k)

        @pl.when(via_end(col, peer))
        def _():
            left_via(peer).start()

        @pl.when(jnp.logical_not(jnp.logical_or(via_end(col, peer), via_here(peer))))
        def _():
            left_term(peer).start()

        @pl.when(via_end(peer, col))
        def _():
            lbuf[peer] = jnp.zeros(lbuf.shape[1:], F32)

    if gcols > 1:
        @pl.loop(1, ncol)
        def _(k):
            arrive(k)

    middle = channels // 2

    def outer(k, halves, beside, then):
        high, l_l[...] = split(rows_of(lo, k).T * scale)
        l_c[0:samples, :] = high
        l_c[samples:, :] = high
        half = rights // 2
        units = width // per // 2
        for scr, h in zip(scrs, halves):
            at = pl.ds(pl.multiple_of(h * half, half), half)
            scr[0:half, 0:glanes] = dot(rt_c[at, :], l_c[...]) + dot(rt_c[at, 0:samples], l_l[...])
        beside()
        for scr, h in zip(scrs, halves):
            for u in range(units):
                for v in range(glanes // 128):
                    pieces = [
                        scr[(u * per + a) * tile_cols : (u * per + a + 1) * tile_cols, v * 128 : (v + 1) * 128]
                        for a in range(per)
                    ]
                    lanes = pl.ds(pl.multiple_of(h * middle + u * 128, 128), 128)
                    for a, piece in enumerate(swap_groups(pieces)):
                        at = k * grows + (v * per + a) * tile_cols
                        high, low = split(piece)
                        t_h[at : at + tile_cols, lanes] = high
                        t_l[at : at + tile_cols, lanes] = low
            then(h)

    def weight_grad(k, lanes):
        at = slice(k * grows, (k + 1) * grows)
        both = jnp.concatenate([ct2[:, pl.ds(pl.multiple_of(n * deep, deep), deep)] for n in units(k)], axis=1)
        term = dot_tall(both, t_h[at, lanes], t_l[at, lanes])
        if k == 0:
            acc[:, lanes] = term
        else:
            acc[:, lanes] += term

    def beside(k):
        if k < groups - 1 or gcols > 1:
            left_grad(k)
        if k > 0:
            weight_grad(k - 1, slice(0, channels))

    for k in range(groups - 1):
        ready(k)
        outer(k, (0, 1), functools.partial(beside, k), lambda h: None)
        if gcols == 1:
            @pl.when(jnp.logical_not(inner))
            def _():
                send_term(k)

    if gcols == 1:
        @pl.when(inner)
        def _():
            for k in range(groups - 1):
                send_term(k)

    ready(groups - 1)
    turned = jnp.where(low_half, 1, 0)

    def last_half(h):
        start = pl.multiple_of(h * middle, middle)
        weight_grad(groups - 1, pl.ds(start, middle))
        for i in range(middle // 128):
            terms = acc[:, pl.ds(pl.multiple_of(start + i * 128, 128), 128)].T
            for n in range(128 // share):
                b, q = divmod((i * 128) // share + n, halfway * chips)
                q, m = divmod(q, chips)
                wp[b, h * halfway + q, m] = terms[n * share : (n + 1) * share, :]

        @here
        def _():
            for q in range(halfway):
                core_term(h * halfway + q).start()

    outer(groups - 1, (turned, 1 - turned), functools.partial(beside, groups - 1), last_half)

    def chip_terms(first):
        for k in range(first, first + halfway):
            q = order(k)
            core_term(q).wait_recv()
            xs[q] = wp[core, q] + cbuf[q]
            xbuf[q, chip] = xs[q, chip]

            @here
            def _():
                each_chip(lambda m: chip_term(q, m).start())

    if gcols > 1:
        for k in range(ncol - 1):
            send_term(k)
    chip_terms(0)
    chip_terms(halfway)
    for k in range(early, groups - 1):
        right_grad(k)
    loads[4].wait()
    if gcols == 1:
        left_grad(groups - 1)
    lbuf[col] = lp[own_left, :]
    right_grad(groups - 1)
    settle(brow.at[others], sem("bchiped"))
    bmid[...] = total([brow[m] for m in range(chips)])
    bcol[col] = bmid[...]
    each(ncol, col, lambda p: bias_col(p).start())

    for d in range(width):
        rp[pl.ds(d, tile_cols, stride=width), :] = rpa[d * tile_cols : (d + 1) * tile_cols, :]

    @here
    def _():
        for m in range(chips):
            right_swap(m).start()

    for k in range(ncol - 1):
        q = order(k)
        settle(xbuf.at[q, others], xsr.at[q])
        zs[q] = total([xbuf[q, m] for m in range(chips)])

        @here
        def _():
            col_term(q).start()

    settle(mbuf, sem("swapped"))
    for m in range(chips):
        rsum[m] = rp[pl.ds(pl.multiple_of((2 * m + core) * rw, rw), rw), :] + mbuf[m]

    @here
    def _():
        each_chip(lambda m: right_term(m).start())

    rbuf[chip] = rsum[chip]
    settle(xbuf.at[col, others], xsr.at[col])
    zbuf[col] = total([xbuf[col, m] for m in range(chips)])
    pair = dot_wide(t_h[...], t_l[...], w_c[...]) + b_v[...]
    for k in range(groups):
        for n, unit in enumerate(units(k)):
            at = k * grows + n * deep
            pair_ref[pl.ds(pl.multiple_of(unit * deep, deep), deep), :] = pair[at : at + deep, :]
    settle(zbuf.at[pl.ds(0, ncol - 1)], sem("coled"))
    wg_ref[core, col, chip] = total([zbuf[q] for q in range(ncol)]) / (tile_rows * nrow)

    @pl.loop(1, ncol)
    def _(k):
        col_whole(along(ncol - k)).start()

    @here
    def _():
        each_chip(lambda m: chip_whole(col, m).start())

    def combine():
        if ncol > 3:
            @pl.when(jnp.logical_or(col == 1, col == ncol - 2))
            def _():
                settle(vbuf.at[pl.ds(0, ncol - 3)], sem("via"))

        for p in range(ncol):
            @pl.when(via_here(p))
            def _():
                lp[p * lw : (p + 1) * lw, :] += vbuf[p]
                left_term(p).start()

    @pl.when(core == 0)
    def _():
        combine()

    ends = jnp.logical_not(inner)

    @pl.when(inner)
    def _():
        settle(lo.at[pl.ds(0, 2 * lw)], sem("left"))
        settle(lo.at[pl.ds(0, 2 * lw)], sem("relay"))

    @pl.when(ends)
    def _():
        settle(lo.at[pl.ds(0, lw)], sem("left"))

    for peer in range(ncol):
        @pl.when(far_off(peer))
        def _():
            settle(lo.at[pl.ds(0, lw)], sem("leftfar"))

    settle(ro.at[pl.ds(0, chips * rw)], sem("right"))
    settle(ro.at[pl.ds(0, (chips - 1) * rw)], sem("pass"))
    settle(bown, sem("bmate"))
    settle(brow.at[others], sem("bchip"))
    settle(bcol.at[pl.ds(0, ncol - 1)], sem("bcol"))
    settle(wp.at[0], sem("core"))
    settle(xs.at[:, others], sem("chip"))
    settle(mbuf, sem("swap"))

    @pl.loop(1, ncol)
    def _(k):
        q = along(k)
        piece_in = wg_ref.at[core, q, chip]
        settle(piece_in, azr.at[q])
        each_chip(lambda m: chip_whole(q, m).start())

    @pl.when(core == 0)
    def _():
        q = along(ncol - 1)
        each_chip(lambda m: direct_whole(q, 2 * m + 1).start())
        direct_whole(q, mate).start()

    @pl.when(core == 1)
    def _():
        combine()

    @pl.loop(0, ncol)
    def _(k):
        q = along(k)
        settle(wg_ref.at[core, q, others], axr.at[q])

        @pl.when(jnp.logical_or(core == 1, k < ncol - 1))
        def _():
            core_whole(q).start()

    settle(rbuf.at[others], sem("rterm"))
    rg_ref[...] = total([rbuf[m] for m in range(chips)])
    settle(rbuf.at[others], sem("rterms"))
    settle(zs.at[pl.ds(0, ncol - 1)], sem("col"))
    settle(zs.at[pl.ds(0, ncol - 1)], sem("allcol"))
    settle(xs.at[:, others], sem("allchip"))
    settle(wg_ref.at[1 - core], sem("done"))

    @pl.when(core == 0)
    def _():
        settle(wg_ref.at[core, 0], sem("alldirect"))
        settle(wg_ref.at[core, pl.ds(0, ncol - 1)], sem("allcore"))

    @pl.when(core == 1)
    def _():
        settle(wg_ref.at[core], sem("allcore"))
    settle(bcol.at[pl.ds(0, ncol - 1)], sem("bcoled"))
    bg_ref[...] = total([bcol[q] for q in range(ncol)])[0:1, :] / (tile_rows * nrow)
    near_ends = [jnp.logical_and(ncol > 3, col >= 3), jnp.logical_and(ncol > 3, col <= ncol - 4)]
    absent = near_ends[0].astype(jnp.int32) + near_ends[1].astype(jnp.int32)
    for n in range(3):
        if ncol - 1 - n > 0:
            @pl.when(absent == n)
            def _():
                settle(lbuf.at[pl.ds(0, ncol - 1 - n)], sem("term"))

    lg_ref[...] = total([lbuf[q] for q in range(ncol)])
    settle(lbuf.at[pl.ds(0, ncol - 1)], sem("terms"))


def finish_kernel(
    width, pair_ref, lg_ref, rg_ref, wg_ref, bg_ref,
    pair_out, lg_out, rg_out, w_out, bg_out, sems,
):
    halves, ncol, chips, share, _ = wg_ref.shape
    copies = [
        pltpu.make_async_copy(src, dst, sems.at[k])
        for k, (src, dst) in enumerate([
            (pair_ref, pair_out), (lg_ref, lg_out), (rg_ref, rg_out), (bg_ref, bg_out),
        ])
    ]
    for s in range(halves * ncol * chips):
        d, c = divmod(s * share, width)
        q, m = divmod(s, chips)
        h, q = divmod(q, ncol)
        b, q = divmod(q, ncol // 2)
        q += h * (ncol // 2)
        pltpu.make_async_copy(wg_ref.at[b, q, m], w_out.at[pl.ds(c, share), d], sems.at[4]).start()
    for copy in copies:
        copy.start()
    for copy in copies:
        copy.wait()
    pltpu.make_async_copy(wg_ref, wg_ref, sems.at[4]).wait()


def per_device(nrow, ncol, left_factors, right_factors, weight, bias, cotangent):
    samples, li, width = left_factors.shape
    rj = right_factors.shape[1]
    tile_rows, tile_cols, pair_width = cotangent.shape
    channels = weight.shape[0]
    lw, rw = li * width, rj * width
    lefts, rights = tile_rows * width, tile_cols * width
    pairs = tile_rows * tile_cols
    chips, share = nrow // 2, channels // (nrow * ncol)
    group = max(lw, STEP * width)
    dma = pltpu.SemaphoreType.DMA

    def shape(*dims):
        return jax.ShapeDtypeStruct(dims, F32)

    def half(*dims):
        return pltpu.VMEM(dims, BF16)

    def buf(*dims):
        return pltpu.VMEM(dims, F32)

    scratch = [
        buf(lefts, samples), buf(rights, samples), buf(lefts, samples), *[buf(ncol, lw, samples)] * 2,
        buf(rights, samples), buf(rights, samples), *[buf(chips, rw, samples)] * 3,
        buf(2, ncol, chips, share, pair_width), *[buf(ncol, chips, share, pair_width)] * 3,
        *[buf(ncol, share, pair_width)] * 2,
        *[buf(8, pair_width)] * 3, buf(chips, 8, pair_width), buf(8, pair_width), buf(ncol, 8, pair_width),
        buf(channels, pair_width), buf(1, pair_width), buf(pairs, pair_width),
        buf(max(rights, channels), 128),
        *[buf(max(pairs, rights), max(group, STEP * width))] * 2, buf(pair_width, channels),
        half(pairs, 2 * pair_width), half(2 * pair_width, pairs), half(channels, 2 * pair_width),
        half(2 * pair_width, channels), half(pair_width, channels),
        half(rights, lefts), half(rights, lefts), half(rights, 2 * samples), half(2 * samples, rights),
        half(pairs, channels), half(pairs, channels),
        half(2 * samples, group), half(samples, group), half(group, 2 * samples),
        dma((5,)), dma((len(SINGLE),)), dma((ncol, 2)), dma((chips,)),
        dma((ncol,)), dma((ncol,)), dma((ncol,)), dma((ncol,)),
    ]
    pair, lg, rg, wg, bg = pl.pallas_call(
        functools.partial(tile_kernel, nrow, ncol, width),
        out_shape=(
            shape(pairs, pair_width), shape(lw, samples), shape(rw, samples),
            shape(2, ncol, chips, share, pair_width), shape(1, pair_width),
        ),
        in_specs=[HBM] * 5,
        out_specs=[VMEM] * 5,
        scratch_shapes=scratch,
        compiler_params=pltpu.CompilerParams(
            collective_id=0, has_side_effects=True, vmem_limit_bytes=40 * 2**20
        ),
        name="tile",
    )(
        in_hbm(left_factors.transpose(1, 2, 0).reshape(lw, samples)),
        in_hbm(right_factors.transpose(1, 2, 0).reshape(rw, samples)),
        in_hbm(weight),
        in_hbm(bias.reshape(1, pair_width)),
        in_hbm(cotangent.reshape(pairs, pair_width)),
    )
    pair, lg, rg, wg, bg = pl.pallas_call(
        functools.partial(finish_kernel, width),
        out_shape=(
            shape(pairs, pair_width), shape(lw, samples), shape(rw, samples),
            shape(width, channels // width, pair_width), shape(1, pair_width),
        ),
        in_specs=[VMEM] * 5,
        out_specs=[HBM] * 5,
        scratch_shapes=[dma((5,))],
        compiler_params=pltpu.CompilerParams(vmem_limit_bytes=8 * 2**20),
        name="finish",
    )(pair, lg, rg, wg, bg)
    return (
        pair.reshape(tile_rows, tile_cols, pair_width),
        lg.reshape(li, width, samples).transpose(2, 0, 1),
        rg.reshape(rj, width, samples).transpose(2, 0, 1),
        wg.reshape(channels, pair_width),
        bg.reshape(pair_width),
    )


def solution(mesh):
    nrow, ncol = mesh.shape["row"], mesh.shape["col"]
    in_specs = (
        P(None, ("row", "col"), None),
        P(None, ("col", "row"), None),
        P(),
        P(),
        P("row", "col", None),
    )
    out_specs = (
        P("row", "col", None),
        P(None, ("row", "col"), None),
        P(None, ("col", "row"), None),
        P(),
        P(),
    )
    return jax.shard_map(
        functools.partial(per_device, nrow, ncol),
        mesh=mesh, in_specs=in_specs, out_specs=out_specs, check_vma=False,
    )
```
